32 devices in a mesh: seq: 4 (over y, x), fsdp: 8 (over z, core).
Axes of the slice: x: 2, y: 2, z: 4, core: 2. Of those that a mesh axis runs over, the one named last changes fastest.
Arguments:
- tokens: bfloat16 [16, 1568, 1024], P('fsdp', 'seq'), may hold values from -6 to 6
- lengths: int32 [16], P('fsdp'), may hold values from 392 to 1568, as said below
- ln1_gain: bfloat16 [1024], P('fsdp'), may hold values from 0.5 to 1.5
- ln1_bias: bfloat16 [1024], P('fsdp'), may hold values from -2 to 2
- w_qkv: bfloat16 [1024, 3072], P('fsdp'), may hold values from -0.1875 to 0.1875
- q_bias: bfloat16 [1024], P('fsdp'), may hold values from -3 to 3
- v_bias: bfloat16 [1024], P('fsdp'), may hold values from -3 to 3
- w_out: bfloat16 [1024, 1024], P('fsdp'), may hold values from -4 to 4
- b_out: bfloat16 [1024], P('fsdp'), may hold values from -2 to 2
- ln2_gain: bfloat16 [1024], P('fsdp'), may hold values from 0.5 to 1.5
- ln2_bias: bfloat16 [1024], P('fsdp'), may hold values from -2 to 2
- w_fc1: bfloat16 [1024, 4096], P('fsdp'), may hold values from -0.1875 to 0.1875
- b_fc1: bfloat16 [4096], P('fsdp'), may hold values from -2 to 2
- w_fc2: bfloat16 [4096, 1024], P('fsdp'), may hold values from -0.09375 to 0.09375
- b_fc2: bfloat16 [1024], P('fsdp'), may hold values from -2 to 2
- cotangent: bfloat16 [16, 1568, 1024], P('fsdp', 'seq'), may hold values from -6 to 6
Outputs:
- layer_out: bfloat16 [16, 1568, 1024], P('fsdp', 'seq')
- grad_tokens: float32 [16, 1568, 1024], P('fsdp', 'seq')
- grad_ln1_gain: float32 [1024], P('fsdp')
- grad_ln1_bias: float32 [1024], P('fsdp')
- grad_w_qkv: float32 [1024, 3072], P('fsdp')
- grad_q_bias: float32 [1024], P('fsdp')
- grad_v_bias: float32 [1024], P('fsdp')
- grad_w_out: float32 [1024, 1024], P('fsdp')
- grad_b_out: float32 [1024], P('fsdp')
- grad_ln2_gain: float32 [1024], P('fsdp')
- grad_ln2_bias: float32 [1024], P('fsdp')
- grad_w_fc1: float32 [1024, 4096], P('fsdp')
- grad_b_fc1: float32 [4096], P('fsdp')
- grad_w_fc2: float32 [4096, 1024], P('fsdp')
- grad_b_fc2: float32 [1024], P('fsdp')
The draws below stay inside these ranges and needn't reach their ends.
Inputs may be any that keep to these rules, and one draw needn't show every extreme that they name: `lengths`: the valid tokens of a clip are its first ones; some clip is full and some has exactly 392.
All inputs are finite; a program needn't handle non-finite values.
Results may differ from the reference program's by a relative error of at most 0.018.
Values may be sent and summed in bfloat16 or wider, within the bound.
No kernel may reach another device: no remote copies, remote signals or barrier semaphores. Data moves between devices by JAX's collectives and lax.ppermute only.
A program may use at most 192 MiB of HBM per device.

```python
import jax
import jax.numpy as jnp
from jax import lax

D = 1024
HEADS = 16
HEAD_DIM = 64
FF = 4096
LEN = 1568
CLIPS = 16


def draw_lengths(key, part):
    base_key = jax.random.fold_in(key, 11)
    key_values, key_ranking = jax.random.split(base_key)
    drawn = jax.random.randint(key_values, (CLIPS,), LEN // 4, LEN + 1)
    ranking = jax.random.permutation(key_ranking, CLIPS)
    positions = jnp.arange(CLIPS)
    drawn = jnp.where(positions == ranking[0], LEN, drawn)
    drawn = jnp.where(positions == ranking[1], LEN // 4, drawn)
    return drawn.astype(jnp.int32)


def spiked(values, key, source, target, blocks, factor):
    owner, partner = [(jnp.arange(values.shape[axis_at]) // (values.shape[axis_at] // blocks)).reshape([-1 if axis == axis_at else 1 for axis in range(values.ndim)]) for axis_at in (source, target)]
    chosen = jax.random.permutation(key, blocks)[partner]
    strong = (owner == chosen) | (owner == (partner + blocks // 2) % blocks)
    return jnp.where(strong, factor * values, values)


def block_levels(own_key, dims, shards, low, top_value):
    loudness = 1.0
    for dim, blocks in shards:
        draws = jax.random.uniform(jax.random.fold_in(jax.random.fold_in(own_key, 6), dim), (blocks,), jnp.float32, low / len(shards), top_value / len(shards))
        loudness = loudness * jnp.repeat(jnp.exp(draws), dims[dim] // blocks).reshape((-1,) + (1,) * (len(dims) - 1 - dim))
    return loudness


def scatter_about(own_key, dims, spread, limit, shards=(), held_as=jnp.bfloat16):
    factor_of = block_levels(own_key, dims, shards, -0.22, 0.18) if shards else 1.0
    array = jax.random.normal(own_key, dims, jnp.float32) * spread * factor_of
    return jnp.minimum(jnp.maximum(array, -limit), limit).astype(held_as)


def heavy_noise(stream_key, extent, width, reach, cuts, heavy, kind=jnp.bfloat16):
    values = width * jax.random.normal(stream_key, extent, jnp.float32)
    if cuts:
        values = values * block_levels(stream_key, extent, cuts, -0.22, 0.18)
    return jnp.clip(spiked(values, jax.random.fold_in(stream_key, 3), *heavy), -reach, reach).astype(kind)


def setup_inputs(seed: int = 0) -> dict:
    splits = jax.random.split(jax.random.key(seed), 17)
    tokens = scatter_about(splits[0], (CLIPS, LEN, D), 1.0, 6.0, ((0, 8), (1, 4)))
    lengths = draw_lengths(jax.random.fold_in(splits[16], 71), 0)
    ln1_gain = jnp.clip(1.0 + 0.1 * jax.random.normal(splits[2], (D,), jnp.float32), 0.5, 1.5).astype(jnp.bfloat16)
    ln1_bias = scatter_about(splits[3], (D,), 0.3, 2.0, ((0, 8),))
    w_qkv = scatter_about(splits[4], (D, 3 * D), D ** -0.5, 0.1875, ((0, 8),))
    q_bias = scatter_about(splits[5], (D,), 0.5, 3.0, ((0, 8),))
    v_bias = scatter_about(splits[6], (D,), 0.5, 3.0, ((0, 8),))
    w_out = scatter_about(splits[7], (D, D), (max(D // 512, 1)) ** -0.5, 4.0, ((0, 8),))
    b_out = scatter_about(splits[8], (D,), 0.3, 2.0, ((0, 8),))
    ln2_gain = jnp.clip(1.0 + 0.1 * jax.random.normal(splits[9], (D,), jnp.float32), 0.5, 1.5).astype(jnp.bfloat16)
    ln2_bias = scatter_about(splits[10], (D,), 0.3, 2.0, ((0, 8),))
    w_fc1 = scatter_about(splits[11], (D, FF), D ** -0.5, 0.1875, ((0, 8),))
    b_fc1 = scatter_about(splits[12], (FF,), 0.3, 2.0, ((0, 8),))
    w_fc2 = scatter_about(splits[13], (FF, D), FF ** -0.5, 0.09375, ((0, 8),))
    b_fc2 = scatter_about(splits[14], (D,), 0.3, 2.0, ((0, 8),))
    cotangent = heavy_noise(splits[15], (CLIPS, LEN, D), 1.0, 6.0, ((0, 8), (1, 4)), (0, 2, 8, 2.0))
    return {"tokens": tokens, "lengths": lengths, "ln1_gain": ln1_gain, "ln1_bias": ln1_bias, "w_qkv": w_qkv, "q_bias": q_bias, "v_bias": v_bias, "w_out": w_out, "b_out": b_out, "ln2_gain": ln2_gain, "ln2_bias": ln2_bias, "w_fc1": w_fc1, "b_fc1": b_fc1, "w_fc2": w_fc2, "b_fc2": b_fc2, "cotangent": cotangent}


EPSILON = 1e-06
HIGHEST = lax.Precision.HIGHEST

@jax.custom_vjp
def low(v):
    return lax.optimization_barrier(v.astype(jnp.bfloat16)).astype(jnp.float32)

@jax.custom_vjp
def low_back(v):
    return v

def low_keep(v):
    return (low(v), None)

def low_pass(kept, grad):
    return (grad,)

def back_keep(v):
    return (v, None)

def back_low(kept, grad):
    return (low(grad),)
low.defvjp(low_keep, low_pass)
low_back.defvjp(back_keep, back_low)

def layer_norm(values, gain, shift):
    centered = values - lax.optimization_barrier(jnp.mean(values, axis=-1, keepdims=True))
    variance = lax.optimization_barrier(jnp.mean(centered * centered, axis=-1, keepdims=True))
    return centered * lax.rsqrt(variance + EPSILON) * gain + shift

def clip_layer(params, clip_rows, length):
    ln1_gain, ln1_bias, w_qkv, q_bias, v_bias, w_out, b_out, ln2_gain, ln2_bias, w_fc1, b_fc1, w_fc2, b_fc2 = params
    seq_len = clip_rows.shape[0]
    normed = low(layer_norm(clip_rows, ln1_gain, ln1_bias))
    projected = jnp.dot(normed, w_qkv, precision=HIGHEST)
    queries = low_back(low(projected[:, :D] + q_bias))
    keys = low_back(low(projected[:, D:2 * D]))
    values = low_back(low(projected[:, 2 * D:] + v_bias))
    queries = queries.reshape(seq_len, HEADS, HEAD_DIM)
    keys = keys.reshape(seq_len, HEADS, HEAD_DIM)
    values = values.reshape(seq_len, HEADS, HEAD_DIM)
    raw = low_back(jnp.einsum('qhd,khd->hqk', queries, keys, precision=HIGHEST))
    valid = jnp.arange(seq_len, dtype=jnp.int32) < length
    scores = jnp.where(valid[None, None, :], raw * HEAD_DIM ** (-0.5), -1e+30)
    peaks = lax.optimization_barrier(jnp.max(scores, axis=-1, keepdims=True))
    weights = jnp.exp(scores - peaks)
    probs = weights / lax.optimization_barrier(jnp.sum(weights, axis=-1, keepdims=True))
    attended = jnp.einsum('hqk,khd->qhd', low(probs), values, precision=HIGHEST).reshape(seq_len, D)
    attended = low_back(low(attended))
    branch = low_back(jnp.dot(attended, w_out, precision=HIGHEST) + b_out)
    middle = clip_rows + branch
    normed_two = low(layer_norm(middle, ln2_gain, ln2_bias))
    hidden_pre = low_back(jnp.dot(normed_two, w_fc1, precision=HIGHEST) + b_fc1)
    hidden = low(jax.nn.gelu(hidden_pre, approximate=False))
    mlp_out = low_back(jnp.dot(hidden, w_fc2, precision=HIGHEST) + b_fc2)
    return middle + mlp_out

def reference(tokens, lengths, ln1_gain, ln1_bias, w_qkv, q_bias, v_bias, w_out, b_out, ln2_gain, ln2_bias, w_fc1, b_fc1, w_fc2, b_fc2, cotangent):
    params = tuple((weight.astype(jnp.float32) for weight in (ln1_gain, ln1_bias, w_qkv, q_bias, v_bias, w_out, b_out, ln2_gain, ln2_bias, w_fc1, b_fc1, w_fc2, b_fc2)))

    def forward(param_set, inputs):

        def per_clip(pair):
            return jax.checkpoint(clip_layer)(param_set, pair[0], pair[1])
        return lax.map(per_clip, (inputs, lengths))
    outputs, pullback = jax.vjp(forward, params, tokens.astype(jnp.float32))
    grad_params, grad_inputs = pullback(cotangent.astype(jnp.float32))
    return (outputs.astype(jnp.bfloat16), grad_inputs, grad_params[0], grad_params[1], grad_params[2], grad_params[3], grad_params[4], grad_params[5], grad_params[6], grad_params[7], grad_params[8], grad_params[9], grad_params[10], grad_params[11], grad_params[12])
```

```python
import functools

import jax
import jax.numpy as jnp
from jax import lax
from jax.experimental import pallas as pl
from jax.experimental.pallas import tpu as pltpu
from jax.sharding import PartitionSpec as P

HEAD_DIM = 64
PAIR = 2 * HEAD_DIM
EPSILON = 1e-06
NEGATIVE = -1e30
F32, BF16 = jnp.float32, jnp.bfloat16
SCALE = HEAD_DIM ** -0.5
SCALE2 = SCALE * 1.4426950408889634
NT = (((1,), (1,)), ((), ()))
NN = (((1,), (0,)), ((), ()))
TN = (((0,), (0,)), ((), ()))


def dot(a, b, dims=NN):
    return lax.dot_general(a, b, dims, preferred_element_type=F32)


def of_head(block, h):
    lane = lax.broadcasted_iota(jnp.int32, (1, PAIR), 1)
    return jnp.where(lane // HEAD_DIM == h, block, jnp.zeros_like(block))


def valid_rows(j, bk, length):
    return j * bk + lax.broadcasted_iota(jnp.int32, (bk, 1), 0) < length


def transposed_chunks(out_ref, in_ref, cols, bk):
    for j in range(in_ref.shape[1] // bk):
        out_ref[j] = jnp.transpose(in_ref[0, pl.ds(j * bk, bk), cols])


def attend_kernel(len_ref, q_ref, k_ref, v_ref, o_ref, lse_ref, s_ref, vt_ref, ot_ref, *, bk):
    length = len_ref[pl.program_id(0)]
    rows_all, width = q_ref.shape[1:]
    chunks = pl.cdiv(length, bk)
    for pair in range(width // PAIR):
        cols = pl.ds(PAIR * pair, PAIR)
        transposed_chunks(vt_ref, v_ref, cols, bk)
        queries = [of_head(q_ref[0, :, cols], h) for h in range(2)]

        def score(j, tops):
            keys = k_ref[0, pl.ds(pl.multiple_of(j * bk, bk), bk), cols]
            ok = valid_rows(j, bk, length)
            out = []
            for h in range(2):
                s = jnp.where(ok, dot(keys, queries[h], NT), NEGATIVE)
                s_ref[h, j] = s
                top = tops[h]
                for i in range(bk // 8):
                    top = jnp.maximum(top, s[8 * i : 8 * i + 8])
                out.append(top)
            return tuple(out)

        low = jnp.full((8, rows_all), NEGATIVE, F32)
        tops = lax.fori_loop(0, chunks, score, (low, low))
        peaks = [jnp.max(top, axis=0, keepdims=True) * SCALE2 for top in tops]
        ot_ref[...] = jnp.zeros_like(ot_ref)

        def mix(j, sums):
            out = []
            for h in range(2):
                p = jnp.exp2(s_ref[h, j] * SCALE2 - peaks[h])
                total = sums[h]
                for i in range(bk // 8):
                    total = total + p[8 * i : 8 * i + 8]
                out.append(total)
                half = pl.ds(HEAD_DIM * h, HEAD_DIM)
                ot_ref[half] += dot(vt_ref[j, half], p.astype(BF16))
            return tuple(out)

        zero = jnp.zeros((8, rows_all), F32)
        sums = lax.fori_loop(0, chunks, mix, (zero, zero))
        for h in range(2):
            total = jnp.sum(sums[h], axis=0, keepdims=True)
            half = pl.ds(HEAD_DIM * h, HEAD_DIM)
            lse_ref[0, pl.ds(2 * pair + h, 1)] = peaks[h] + jnp.log2(total)
            ot_ref[half] = ot_ref[half] / total
        o_ref[0, :, cols] = jnp.transpose(ot_ref[...]).astype(BF16)


def attend_back_kernel(
    len_ref, q_ref, k_ref, v_ref, do_ref, o_ref, lse_ref, d_ref, kt_ref, dqt_ref, *, bk
):
    length = len_ref[pl.program_id(0)]
    width = q_ref.shape[2]
    chunks = pl.cdiv(length, bk)
    d_ref[...] = jnp.zeros_like(d_ref)
    for pair in range(width // PAIR):
        cols = pl.ds(PAIR * pair, PAIR)
        outs = do_ref[0, :, cols]
        both = jnp.transpose(outs.astype(F32) * o_ref[0, :, cols].astype(F32))
        inner = [
            jnp.sum(both[HEAD_DIM * h : HEAD_DIM * (h + 1)], axis=0, keepdims=True)
            for h in range(2)
        ]
        queries = [of_head(q_ref[0, :, cols], h) for h in range(2)]
        grads = [of_head(outs, h) for h in range(2)]
        logs = [lse_ref[0, pl.ds(2 * pair + h, 1)] for h in range(2)]
        transposed_chunks(kt_ref, k_ref, cols, bk)
        dqt_ref[...] = jnp.zeros_like(dqt_ref)

        def step(j, carry):
            rows = pl.ds(pl.multiple_of(j * bk, bk), bk)
            keys = k_ref[0, rows, cols]
            values = v_ref[0, rows, cols]
            ok = valid_rows(j, bk, length)
            dk = jnp.zeros((bk, PAIR), F32)
            dv = jnp.zeros((bk, PAIR), F32)
            for h in range(2):
                p = jnp.exp2(dot(keys, queries[h], NT) * SCALE2 - logs[h])
                p = jnp.where(ok, p, 0.0)
                g = (p * (dot(values, grads[h], NT) - inner[h])).astype(BF16)
                dv = dv + dot(p.astype(BF16), grads[h])
                dk = dk + dot(g, queries[h])
                half = pl.ds(HEAD_DIM * h, HEAD_DIM)
                dqt_ref[half] += dot(kt_ref[j, half], g)
            d_ref[0, rows, pl.ds(width + PAIR * pair, PAIR)] = (dk * SCALE).astype(BF16)
            d_ref[0, rows, pl.ds(2 * width + PAIR * pair, PAIR)] = dv.astype(BF16)
            return carry

        lax.fori_loop(0, chunks, step, 0)
        d_ref[0, :, cols] = jnp.transpose(dqt_ref[...] * SCALE).astype(BF16)


def chunk_rows(rows):
    return max(b for b in range(8, 225, 8) if rows % b == 0)


def block(rows, width, at):
    return pl.BlockSpec((1, rows, width), lambda c, n: (c, 0, at))


def attend(qkv, lengths):
    clips, rows, triple = qkv.shape
    width = triple // 3
    heads, bk = width // HEAD_DIM, chunk_rows(rows)
    cost = clips * heads * rows * rows
    return pl.pallas_call(
        functools.partial(attend_kernel, bk=bk),
        grid_spec=pltpu.PrefetchScalarGridSpec(
            num_scalar_prefetch=1,
            grid=(clips,),
            in_specs=[block(rows, width, i) for i in range(3)],
            out_specs=[block(rows, width, 0), block(heads, rows, 0)],
            scratch_shapes=[
                pltpu.VMEM((2, rows // bk, bk, rows), F32),
                pltpu.VMEM((rows // bk, PAIR, bk), BF16),
                pltpu.VMEM((PAIR, rows), F32),
            ],
        ),
        out_shape=[
            jax.ShapeDtypeStruct((clips, rows, width), BF16),
            jax.ShapeDtypeStruct((clips, heads, rows), F32),
        ],
        compiler_params=pltpu.CompilerParams(vmem_limit_bytes=40 << 20),
        cost_estimate=pl.CostEstimate(
            flops=cost * 1024, bytes_accessed=clips * rows * width * 8, transcendentals=cost
        ),
        name="attend",
    )(lengths, qkv, qkv, qkv)


def attend_back(qkv, grads, outs, logs, lengths):
    clips, rows, triple = qkv.shape
    width = triple // 3
    heads, bk = width // HEAD_DIM, chunk_rows(rows)
    cost = clips * heads * rows * rows
    return pl.pallas_call(
        functools.partial(attend_back_kernel, bk=bk),
        grid_spec=pltpu.PrefetchScalarGridSpec(
            num_scalar_prefetch=1,
            grid=(clips,),
            in_specs=[block(rows, width, i) for i in (0, 1, 2, 0, 0)] + [block(heads, rows, 0)],
            out_specs=block(rows, triple, 0),
            scratch_shapes=[
                pltpu.VMEM((rows // bk, PAIR, bk), BF16),
                pltpu.VMEM((PAIR, rows), F32),
            ],
        ),
        out_shape=jax.ShapeDtypeStruct((clips, rows, triple), BF16),
        compiler_params=pltpu.CompilerParams(vmem_limit_bytes=40 << 20),
        cost_estimate=pl.CostEstimate(
            flops=cost * 2560, bytes_accessed=clips * rows * width * 16, transcendentals=cost
        ),
        name="attend_back",
    )(lengths, qkv, qkv, qkv, grads, outs, logs)


def swap(value, ring, r):
    return lax.ppermute(value, "seq", [(i, i ^ r) for i in range(ring)])


def gather_seq(value, ring, me):
    out = jnp.zeros((ring,) + value.shape, value.dtype)
    out = lax.dynamic_update_index_in_dim(out, value, me, 0)
    for r in range(1, ring):
        out = lax.dynamic_update_index_in_dim(out, swap(value, ring, r), me ^ r, 0)
    return out


def sum_seq(terms, ring, me):
    total = lax.dynamic_index_in_dim(terms, me, 0, keepdims=False).astype(F32)
    for r in range(1, ring):
        term = lax.dynamic_index_in_dim(terms, me ^ r, 0, keepdims=False)
        total = total + swap(term, ring, r).astype(F32)
    return total


def sum_owned(grad, ring, me):
    owned = lax.psum_scatter(grad.astype(BF16), "fsdp", scatter_dimension=0, tiled=True)
    rows, width = owned.shape
    part = sum_seq(owned.reshape(ring, rows // ring, width), ring, me).astype(BF16)
    return gather_seq(part, ring, me).reshape(rows, width).astype(F32)


def normalize(values):
    centered = values - jnp.mean(values, axis=-1, keepdims=True)
    variance = jnp.mean(centered * centered, axis=-1, keepdims=True)
    rstd = lax.rsqrt(variance + EPSILON)
    return centered * rstd, rstd


def normalize_back(grad, normed, rstd, gain):
    e = grad * gain
    mean = jnp.mean(e, axis=-1, keepdims=True)
    along = jnp.mean(e * normed, axis=-1, keepdims=True)
    return rstd * (e - mean - normed * along)


def shards(
    ring,
    tokens,
    lengths,
    ln1_gain,
    ln1_bias,
    w_qkv,
    q_bias,
    v_bias,
    w_out,
    b_out,
    ln2_gain,
    ln2_bias,
    w_fc1,
    b_fc1,
    w_fc2,
    b_fc2,
    cotangent,
):
    clips, rows, width = tokens.shape
    total_rows = clips * rows
    clip_rows = rows * ring
    local = width // ring
    me = lax.axis_index("seq")

    whole = [gather_seq(tokens[c], ring, me).reshape(clip_rows, width) for c in range(clips)]

    own = ln1_gain.shape[0]
    packed = jnp.concatenate(
        [
            jnp.stack([ln1_gain, ln1_bias, q_bias, v_bias, b_out, ln2_gain, ln2_bias, b_fc2]),
            b_fc1.reshape(-1, own),
        ]
    )
    vectors = lax.all_gather(packed, "fsdp", axis=0, tiled=False)
    c1 = vectors[:, 8:].reshape(-1).astype(F32)
    vectors = vectors[:, :8].transpose(1, 0, 2).reshape(8, width).astype(F32)
    g1, b1, qb, vb, bo, g2, b2, c2 = (vectors[i] for i in range(8))
    qb_mine = lax.dynamic_slice_in_dim(qb, me * local, local)
    vb_mine = lax.dynamic_slice_in_dim(vb, me * local, local)
    bias_mine = jnp.concatenate([qb_mine, jnp.zeros_like(qb_mine), vb_mine])

    mine = lax.dynamic_index_in_dim(w_qkv.reshape(own, 3, ring, local), me, 2, keepdims=False)
    wqkv = lax.all_gather(mine.reshape(own, 3 * local), "fsdp", axis=0, tiled=True)
    wo = lax.all_gather(w_out, "fsdp", axis=0, tiled=True)
    w1 = lax.all_gather(w_fc1, "fsdp", axis=0, tiled=True)
    w2 = lax.all_gather(w_fc2, "fsdp", axis=0, tiled=True)

    normed, qkv, heads_out, logs, attended = [], [], [], [], []
    for c in range(clips):
        n1 = normalize(whole[c].astype(F32))[0]
        h1 = (n1 * g1 + b1).astype(BF16)
        part = (dot(h1, wqkv) + bias_mine).astype(BF16)[None]
        out, log = attend(part, lax.dynamic_slice_in_dim(lengths, c, 1))
        moved = lax.all_to_all(
            out.reshape(ring, rows, local), "seq", split_axis=0, concat_axis=0, tiled=True
        )
        normed.append(h1)
        qkv.append(part)
        heads_out.append(out)
        logs.append(log)
        attended.append(moved.transpose(1, 0, 2).reshape(rows, width))
    attended = jnp.concatenate(attended, axis=0)

    inputs = tokens.astype(F32).reshape(total_rows, width)
    middle = inputs + (dot(attended, wo) + bo)
    n2, r2 = normalize(middle)
    h2 = (n2 * g2 + b2).astype(BF16)
    z = dot(h2, w1) + c1
    phi = 0.5 * (1.0 + lax.erf(z * (2.0 ** -0.5)))
    hidden = (z * phi).astype(BF16)
    slope = phi + z * (jnp.exp(-0.5 * z * z) * 0.3989422804014327)
    layer_out = (middle + (dot(hidden, w2) + c2)).astype(BF16).reshape(clips, rows, width)

    dy = cotangent.reshape(total_rows, width)
    dy_f = dy.astype(F32)
    grad_w2 = sum_owned(dot(hidden, dy, TN), ring, me)
    dz = (dot(dy, w2, NT) * slope).astype(BF16)
    grad_w1 = sum_owned(dot(h2, dz, TN), ring, me)
    dh2 = dot(dz, w1, NT)
    grad_middle = dy_f + normalize_back(dh2, n2, r2, g2)
    da = grad_middle.astype(BF16)
    grad_wo = sum_owned(dot(attended, da, TN), ring, me)
    do = dot(da, wo, NT).astype(BF16)

    dqkv, own_terms, gain_sum, shift_sum = [], [], 0.0, 0.0
    for c in range(clips):
        sent = do[c * rows : (c + 1) * rows].reshape(rows, ring, local).transpose(1, 0, 2)
        moved = lax.all_to_all(sent, "seq", split_axis=0, concat_axis=0, tiled=True)
        moved = moved.reshape(1, clip_rows, local)
        d = attend_back(
            qkv[c], moved, heads_out[c], logs[c], lax.dynamic_slice_in_dim(lengths, c, 1)
        )[0]
        dh1 = dot(d, wqkv, NT)
        n1 = normalize(whole[c].astype(F32))[0]
        gain_sum = gain_sum + jnp.sum(dh1 * n1, axis=0)
        shift_sum = shift_sum + jnp.sum(dh1, axis=0)
        own_terms.append(sum_seq(dh1.astype(BF16).reshape(ring, rows, width), ring, me))
        dqkv.append(d)
    dqkv = jnp.concatenate(dqkv, axis=0)
    grad_mine = dot(jnp.concatenate(normed, axis=0), dqkv, TN)
    owned = lax.psum_scatter(grad_mine.astype(BF16), "fsdp", scatter_dimension=0, tiled=True)
    grad_qkv = gather_seq(owned.reshape(own, 3, local), ring, me)
    grad_qkv = grad_qkv.transpose(1, 2, 0, 3).reshape(own, 3 * width).astype(F32)

    bias_sum = jnp.sum(dqkv.astype(F32), axis=0)
    zeros = jnp.zeros((width,), F32)
    first = jnp.stack(
        [
            gain_sum,
            shift_sum,
            lax.dynamic_update_slice_in_dim(zeros, bias_sum[:local], me * local, 0),
            lax.dynamic_update_slice_in_dim(zeros, bias_sum[2 * local :], me * local, 0),
        ]
    )
    second = jnp.stack(
        [
            jnp.sum(dh2 * n2, axis=0),
            jnp.sum(dh2, axis=0),
            jnp.sum(dy_f, axis=0),
            jnp.sum(da.astype(F32), axis=0),
        ]
    )
    second = jnp.concatenate([second, jnp.sum(dz.astype(F32), axis=0).reshape(-1, width)])
    at = lax.axis_index("fsdp") * own
    small = lax.psum(second.astype(BF16), ("seq", "fsdp")).astype(F32)
    four = lax.dynamic_slice_in_dim(small[:4], at, own, axis=1)
    grad_c1 = lax.dynamic_slice_in_dim(
        small[4:].reshape(-1), lax.axis_index("fsdp") * b_fc1.shape[0], b_fc1.shape[0]
    )
    late = lax.psum(first.astype(BF16), ("seq", "fsdp")).astype(F32)
    late = lax.dynamic_slice_in_dim(late, at, own, axis=1)

    terms = jnp.concatenate(own_terms, axis=0)
    n1, r1 = normalize(inputs)
    grad_inputs = (grad_middle + normalize_back(terms, n1, r1, g1)).reshape(clips, rows, width)
    return (
        layer_out,
        grad_inputs,
        late[0],
        late[1],
        grad_qkv,
        late[2],
        late[3],
        grad_wo,
        four[3],
        four[0],
        four[1],
        grad_w1,
        grad_c1,
        grad_w2,
        four[2],
    )


def solution(mesh):
    act, vec, mat = P("fsdp", "seq", None), P("fsdp"), P("fsdp", None)
    in_specs = (act, vec, vec, vec, mat, vec, vec, mat, vec, vec, vec, mat, vec, mat, vec, act)
    out_specs = (act, act, vec, vec, mat, vec, vec, mat, vec, vec, vec, mat, vec, mat, vec)
    return jax.shard_map(
        functools.partial(shards, mesh.shape["seq"]),
        mesh=mesh,
        in_specs=in_specs,
        out_specs=out_specs,
        check_vma=False,
    )
```

```python
import functools

import jax
import jax.numpy as jnp
from jax import lax
from jax.experimental import pallas as pl
from jax.experimental.pallas import tpu as pltpu
from jax.sharding import PartitionSpec as P

HEAD_DIM = 64
PAIR = 2 * HEAD_DIM
EPSILON = 1e-06
NEGATIVE = -1e30
F32, BF16 = jnp.float32, jnp.bfloat16
SCALE = HEAD_DIM ** -0.5
SCALE2 = SCALE * 1.4426950408889634
NT = (((1,), (1,)), ((), ()))
NN = (((1,), (0,)), ((), ()))
TN = (((0,), (0,)), ((), ()))


def dot(a, b, dims=NN):
    return lax.dot_general(a, b, dims, preferred_element_type=F32)


def of_head(block, h):
    lane = lax.broadcasted_iota(jnp.int32, (1, PAIR), 1)
    return jnp.where(lane // HEAD_DIM == h, block, jnp.zeros_like(block))


def valid_rows(j, bk, length):
    return j * bk + lax.broadcasted_iota(jnp.int32, (bk, 1), 0) < length


def transposed_chunks(out_ref, in_ref, cols, bk):
    for j in range(in_ref.shape[1] // bk):
        out_ref[j] = jnp.transpose(in_ref[0, pl.ds(j * bk, bk), cols])


def attend_kernel(len_ref, q_ref, k_ref, v_ref, o_ref, lse_ref, s_ref, vt_ref, ot_ref, *, bk):
    length = len_ref[pl.program_id(0)]
    rows_all, width = q_ref.shape[1:]
    chunks = pl.cdiv(length, bk)
    for pair in range(width // PAIR):
        cols = pl.ds(PAIR * pair, PAIR)
        transposed_chunks(vt_ref, v_ref, cols, bk)
        queries = [of_head(q_ref[0, :, cols], h) for h in range(2)]

        def score(j, tops):
            keys = k_ref[0, pl.ds(pl.multiple_of(j * bk, bk), bk), cols]
            ok = valid_rows(j, bk, length)
            out = []
            for h in range(2):
                s = jnp.where(ok, dot(keys, queries[h], NT), NEGATIVE)
                s_ref[h, j] = s
                top = tops[h]
                for i in range(bk // 8):
                    top = jnp.maximum(top, s[8 * i : 8 * i + 8])
                out.append(top)
            return tuple(out)

        low = jnp.full((8, rows_all), NEGATIVE, F32)
        tops = lax.fori_loop(0, chunks, score, (low, low))
        peaks = [jnp.max(top, axis=0, keepdims=True) * SCALE2 for top in tops]
        ot_ref[...] = jnp.zeros_like(ot_ref)

        def mix(j, sums):
            out = []
            for h in range(2):
                p = jnp.exp2(s_ref[h, j] * SCALE2 - peaks[h])
                total = sums[h]
                for i in range(bk // 8):
                    total = total + p[8 * i : 8 * i + 8]
                out.append(total)
                half = pl.ds(HEAD_DIM * h, HEAD_DIM)
                ot_ref[half] += dot(vt_ref[j, half], p.astype(BF16))
            return tuple(out)

        zero = jnp.zeros((8, rows_all), F32)
        sums = lax.fori_loop(0, chunks, mix, (zero, zero))
        for h in range(2):
            total = jnp.sum(sums[h], axis=0, keepdims=True)
            half = pl.ds(HEAD_DIM * h, HEAD_DIM)
            lse_ref[0, pl.ds(2 * pair + h, 1)] = peaks[h] + jnp.log2(total)
            ot_ref[half] = ot_ref[half] / total
        o_ref[0, :, cols] = jnp.transpose(ot_ref[...]).astype(BF16)


def attend_back_kernel(
    len_ref, q_ref, k_ref, v_ref, do_ref, o_ref, lse_ref, d_ref, kt_ref, dqt_ref, *, bk
):
    length = len_ref[pl.program_id(0)]
    width = q_ref.shape[2]
    chunks = pl.cdiv(length, bk)
    d_ref[...] = jnp.zeros_like(d_ref)
    for pair in range(width // PAIR):
        cols = pl.ds(PAIR * pair, PAIR)
        outs = do_ref[0, :, cols]
        both = jnp.transpose(outs.astype(F32) * o_ref[0, :, cols].astype(F32))
        inner = [
            jnp.sum(both[HEAD_DIM * h : HEAD_DIM * (h + 1)], axis=0, keepdims=True)
            for h in range(2)
        ]
        queries = [of_head(q_ref[0, :, cols], h) for h in range(2)]
        grads = [of_head(outs, h) for h in range(2)]
        logs = [lse_ref[0, pl.ds(2 * pair + h, 1)] for h in range(2)]
        transposed_chunks(kt_ref, k_ref, cols, bk)
        dqt_ref[...] = jnp.zeros_like(dqt_ref)

        def step(j, carry):
            rows = pl.ds(pl.multiple_of(j * bk, bk), bk)
            keys = k_ref[0, rows, cols]
            values = v_ref[0, rows, cols]
            ok = valid_rows(j, bk, length)
            dk = jnp.zeros((bk, PAIR), F32)
            dv = jnp.zeros((bk, PAIR), F32)
            for h in range(2):
                p = jnp.exp2(dot(keys, queries[h], NT) * SCALE2 - logs[h])
                p = jnp.where(ok, p, 0.0)
                g = (p * (dot(values, grads[h], NT) - inner[h])).astype(BF16)
                dv = dv + dot(p.astype(BF16), grads[h])
                dk = dk + dot(g, queries[h])
                half = pl.ds(HEAD_DIM * h, HEAD_DIM)
                dqt_ref[half] += dot(kt_ref[j, half], g)
            d_ref[0, rows, pl.ds(width + PAIR * pair, PAIR)] = (dk * SCALE).astype(BF16)
            d_ref[0, rows, pl.ds(2 * width + PAIR * pair, PAIR)] = dv.astype(BF16)
            return carry

        lax.fori_loop(0, chunks, step, 0)
        d_ref[0, :, cols] = jnp.transpose(dqt_ref[...] * SCALE).astype(BF16)


def chunk_rows(rows):
    return max(b for b in range(8, 225, 8) if rows % b == 0)


def block(rows, width, at):
    return pl.BlockSpec((1, rows, width), lambda c, n: (c, 0, at))


def attend(qkv, lengths):
    clips, rows, triple = qkv.shape
    width = triple // 3
    heads, bk = width // HEAD_DIM, chunk_rows(rows)
    cost = clips * heads * rows * rows
    return pl.pallas_call(
        functools.partial(attend_kernel, bk=bk),
        grid_spec=pltpu.PrefetchScalarGridSpec(
            num_scalar_prefetch=1,
            grid=(clips,),
            in_specs=[block(rows, width, i) for i in range(3)],
            out_specs=[block(rows, width, 0), block(heads, rows, 0)],
            scratch_shapes=[
                pltpu.VMEM((2, rows // bk, bk, rows), F32),
                pltpu.VMEM((rows // bk, PAIR, bk), BF16),
                pltpu.VMEM((PAIR, rows), F32),
            ],
        ),
        out_shape=[
            jax.ShapeDtypeStruct((clips, rows, width), BF16),
            jax.ShapeDtypeStruct((clips, heads, rows), F32),
        ],
        compiler_params=pltpu.CompilerParams(vmem_limit_bytes=40 << 20),
        cost_estimate=pl.CostEstimate(
            flops=cost * 1024, bytes_accessed=clips * rows * width * 8, transcendentals=cost
        ),
        name="attend",
    )(lengths, qkv, qkv, qkv)


def attend_back(qkv, grads, outs, logs, lengths):
    clips, rows, triple = qkv.shape
    width = triple // 3
    heads, bk = width // HEAD_DIM, chunk_rows(rows)
    cost = clips * heads * rows * rows
    return pl.pallas_call(
        functools.partial(attend_back_kernel, bk=bk),
        grid_spec=pltpu.PrefetchScalarGridSpec(
            num_scalar_prefetch=1,
            grid=(clips,),
            in_specs=[block(rows, width, i) for i in (0, 1, 2, 0, 0)] + [block(heads, rows, 0)],
            out_specs=block(rows, triple, 0),
            scratch_shapes=[
                pltpu.VMEM((rows // bk, PAIR, bk), BF16),
                pltpu.VMEM((PAIR, rows), F32),
            ],
        ),
        out_shape=jax.ShapeDtypeStruct((clips, rows, triple), BF16),
        compiler_params=pltpu.CompilerParams(vmem_limit_bytes=40 << 20),
        cost_estimate=pl.CostEstimate(
            flops=cost * 2560, bytes_accessed=clips * rows * width * 16, transcendentals=cost
        ),
        name="attend_back",
    )(lengths, qkv, qkv, qkv, grads, outs, logs)


def swap(value, ring, r):
    return lax.ppermute(value, "seq", [(i, i ^ r) for i in range(ring)])


def gather_seq(value, ring, me):
    out = jnp.zeros((ring,) + value.shape, value.dtype)
    out = lax.dynamic_update_index_in_dim(out, value, me, 0)
    for r in range(1, ring):
        out = lax.dynamic_update_index_in_dim(out, swap(value, ring, r), me ^ r, 0)
    return out


def sum_seq(terms, ring, me):
    total = lax.dynamic_index_in_dim(terms, me, 0, keepdims=False).astype(F32)
    for r in range(1, ring):
        term = lax.dynamic_index_in_dim(terms, me ^ r, 0, keepdims=False)
        total = total + swap(term, ring, r).astype(F32)
    return total


def to_owners(grad):
    return lax.psum_scatter(grad, "fsdp", scatter_dimension=0, tiled=True)


def sum_owned(owned, ring, me):
    rows, width = owned.shape
    part = sum_seq(owned.reshape(ring, rows // ring, width), ring, me).astype(BF16)
    return gather_seq(part, ring, me).reshape(rows, width).astype(F32)


def sum_vectors(rows, devices, ring):
    count, width = rows.shape
    sent = rows.reshape(count, devices, width // devices).transpose(1, 0, 2)
    total = jnp.sum(lax.all_to_all(sent, "fsdp", split_axis=0, concat_axis=0, tiled=True), axis=0)
    return total + sum(swap(total, ring, r) for r in range(1, ring))


def normalize(values):
    centered = values - jnp.mean(values, axis=-1, keepdims=True)
    variance = jnp.mean(centered * centered, axis=-1, keepdims=True)
    rstd = lax.rsqrt(variance + EPSILON)
    return centered * rstd, rstd


def normalize_back(grad, normed, rstd, gain):
    e = grad * gain
    mean = jnp.mean(e, axis=-1, keepdims=True)
    along = jnp.mean(e * normed, axis=-1, keepdims=True)
    return rstd * (e - mean - normed * along)


def shards(
    ring,
    devices,
    tokens,
    lengths,
    ln1_gain,
    ln1_bias,
    w_qkv,
    q_bias,
    v_bias,
    w_out,
    b_out,
    ln2_gain,
    ln2_bias,
    w_fc1,
    b_fc1,
    w_fc2,
    b_fc2,
    cotangent,
):
    clips, rows, width = tokens.shape
    total_rows = clips * rows
    clip_rows = rows * ring
    local = width // ring
    me = lax.axis_index("seq")

    whole = [gather_seq(tokens[c], ring, me).reshape(clip_rows, width) for c in range(clips)]

    own = ln1_gain.shape[0]
    packed = jnp.concatenate(
        [
            jnp.stack([ln1_gain, ln1_bias, q_bias, v_bias, b_out, ln2_gain, ln2_bias, b_fc2]),
            b_fc1.reshape(-1, own),
        ]
    )
    vectors = lax.all_gather(packed, "fsdp", axis=0, tiled=False)
    c1 = vectors[:, 8:].reshape(-1).astype(F32)
    vectors = vectors[:, :8].transpose(1, 0, 2).reshape(8, width).astype(F32)
    g1, b1, qb, vb, bo, g2, b2, c2 = (vectors[i] for i in range(8))
    qb_mine = lax.dynamic_slice_in_dim(qb, me * local, local)
    vb_mine = lax.dynamic_slice_in_dim(vb, me * local, local)
    bias_mine = jnp.concatenate([qb_mine, jnp.zeros_like(qb_mine), vb_mine])

    mine = lax.dynamic_index_in_dim(w_qkv.reshape(own, 3, ring, local), me, 2, keepdims=False)
    wqkv = lax.all_gather(mine.reshape(own, 3 * local), "fsdp", axis=0, tiled=True)
    wo = lax.all_gather(w_out, "fsdp", axis=0, tiled=True)
    w1 = lax.all_gather(w_fc1, "fsdp", axis=0, tiled=True)
    w2 = lax.all_gather(w_fc2, "fsdp", axis=0, tiled=True)

    normed, qkv, heads_out, logs, attended = [], [], [], [], []
    for c in range(clips):
        n1 = normalize(whole[c].astype(F32))[0]
        h1 = (n1 * g1 + b1).astype(BF16)
        part = (dot(h1, wqkv) + bias_mine).astype(BF16)[None]
        out, log = attend(part, lax.dynamic_slice_in_dim(lengths, c, 1))
        moved = lax.all_to_all(
            out.reshape(ring, rows, local), "seq", split_axis=0, concat_axis=0, tiled=True
        )
        normed.append(h1)
        qkv.append(part)
        heads_out.append(out)
        logs.append(log)
        attended.append(moved.transpose(1, 0, 2).reshape(rows, width))
    attended = jnp.concatenate(attended, axis=0)

    inputs = tokens.astype(F32).reshape(total_rows, width)
    middle = inputs + (dot(attended, wo) + bo)
    n2, r2 = normalize(middle)
    h2 = (n2 * g2 + b2).astype(BF16)
    z = dot(h2, w1) + c1
    phi = 0.5 * (1.0 + lax.erf(z * (2.0 ** -0.5)))
    hidden = (z * phi).astype(BF16)
    slope = phi + z * (jnp.exp(-0.5 * z * z) * 0.3989422804014327)
    layer_out = (middle + (dot(hidden, w2) + c2)).astype(BF16).reshape(clips, rows, width)

    dy = cotangent.reshape(total_rows, width)
    dy_f = dy.astype(F32)
    term_w2 = dot(hidden, dy, TN).astype(BF16)
    dz = (dot(dy, w2, NT) * slope).astype(BF16)
    term_w1 = dot(h2, dz, TN).astype(BF16)
    dh2 = dot(dz, w1, NT)
    grad_middle = dy_f + normalize_back(dh2, n2, r2, g2)
    da = grad_middle.astype(BF16)
    term_wo = dot(attended, da, TN).astype(BF16)
    do = dot(da, wo, NT).astype(BF16)
    do, term_w2, term_w1, term_wo = lax.optimization_barrier((do, term_w2, term_w1, term_wo))
    owned_w2, owned_w1, owned_wo = (to_owners(t) for t in (term_w2, term_w1, term_wo))

    dqkv, own_terms, gain_sum, shift_sum = [], [], 0.0, 0.0
    for c in range(clips):
        sent = do[c * rows : (c + 1) * rows].reshape(rows, ring, local).transpose(1, 0, 2)
        moved = lax.all_to_all(sent, "seq", split_axis=0, concat_axis=0, tiled=True)
        moved = moved.reshape(1, clip_rows, local)
        d = attend_back(
            qkv[c], moved, heads_out[c], logs[c], lax.dynamic_slice_in_dim(lengths, c, 1)
        )[0]
        dh1 = dot(d, wqkv, NT)
        n1 = normalize(whole[c].astype(F32))[0]
        gain_sum = gain_sum + jnp.sum(dh1 * n1, axis=0)
        shift_sum = shift_sum + jnp.sum(dh1, axis=0)
        own_terms.append(sum_seq(dh1.astype(BF16).reshape(ring, rows, width), ring, me))
        dqkv.append(d)
    dqkv = jnp.concatenate(dqkv, axis=0)
    grad_mine = dot(jnp.concatenate(normed, axis=0), dqkv, TN).astype(BF16)
    grad_mine, owned_w2, owned_w1, owned_wo = lax.optimization_barrier(
        (grad_mine, owned_w2, owned_w1, owned_wo)
    )
    owned = to_owners(grad_mine)
    grad_w2, grad_w1, grad_wo = (sum_owned(o, ring, me) for o in (owned_w2, owned_w1, owned_wo))
    grad_qkv = gather_seq(owned, ring, me).astype(F32)
    grad_qkv = jnp.concatenate(
        [grad_qkv[r, :, i * local : (i + 1) * local] for i in range(3) for r in range(ring)], axis=1
    )

    bias_sum = jnp.sum(dqkv.astype(F32), axis=0)
    zeros = jnp.zeros((width,), F32)
    first = jnp.stack(
        [
            gain_sum,
            shift_sum,
            lax.dynamic_update_slice_in_dim(zeros, bias_sum[:local], me * local, 0),
            lax.dynamic_update_slice_in_dim(zeros, bias_sum[2 * local :], me * local, 0),
        ]
    )
    second = jnp.stack(
        [
            jnp.sum(dh2 * n2, axis=0),
            jnp.sum(dh2, axis=0),
            jnp.sum(dy_f, axis=0),
            jnp.sum(da.astype(F32), axis=0),
        ]
    )
    c1_sum = jnp.sum(dz.astype(F32), axis=0).reshape(devices, -1, own).transpose(1, 0, 2)
    second = jnp.concatenate([second, c1_sum.reshape(-1, width)])
    four = sum_vectors(second, devices, ring)
    grad_c1 = four[4:].reshape(-1)
    late = sum_vectors(first, devices, ring)

    terms = jnp.concatenate(own_terms, axis=0)
    n1, r1 = normalize(inputs)
    grad_inputs = (grad_middle + normalize_back(terms, n1, r1, g1)).reshape(clips, rows, width)
    return (
        layer_out,
        grad_inputs,
        late[0],
        late[1],
        grad_qkv,
        late[2],
        late[3],
        grad_wo,
        four[3],
        four[0],
        four[1],
        grad_w1,
        grad_c1,
        grad_w2,
        four[2],
    )


def solution(mesh):
    act, vec, mat = P("fsdp", "seq", None), P("fsdp"), P("fsdp", None)
    in_specs = (act, vec, vec, vec, mat, vec, vec, mat, vec, vec, vec, mat, vec, mat, vec, act)
    out_specs = (act, act, vec, vec, mat, vec, vec, mat, vec, vec, vec, mat, vec, mat, vec)
    return jax.shard_map(
        functools.partial(shards, mesh.shape["seq"], mesh.shape["fsdp"]),
        mesh=mesh,
        in_specs=in_specs,
        out_specs=out_specs,
        check_vma=False,
    )
```

```python
import functools

import jax
import jax.numpy as jnp
from jax import lax
from jax.experimental import pallas as pl
from jax.experimental.pallas import tpu as pltpu
from jax.sharding import PartitionSpec as P

HEAD_DIM = 64
PAIR = 2 * HEAD_DIM
EPSILON = 1e-06
NEGATIVE = -1e30
F32, BF16 = jnp.float32, jnp.bfloat16
SCALE = HEAD_DIM ** -0.5
SCALE2 = SCALE * 1.4426950408889634
NT = (((1,), (1,)), ((), ()))
NN = (((1,), (0,)), ((), ()))
TN = (((0,), (0,)), ((), ()))


def dot(a, b, dims=NN):
    return lax.dot_general(a, b, dims, preferred_element_type=F32)


def of_head(block, h):
    lane = lax.broadcasted_iota(jnp.int32, (1, PAIR), 1)
    return jnp.where(lane // HEAD_DIM == h, block, jnp.zeros_like(block))


def valid_rows(j, bk, length):
    return j * bk + lax.broadcasted_iota(jnp.int32, (bk, 1), 0) < length


def transposed_chunks(out_ref, in_ref, cols, bk):
    for j in range(in_ref.shape[1] // bk):
        out_ref[j] = jnp.transpose(in_ref[0, pl.ds(j * bk, bk), cols])


def attend_kernel(len_ref, q_ref, k_ref, v_ref, o_ref, lse_ref, s_ref, vt_ref, ot_ref, *, bk):
    length = len_ref[pl.program_id(0)]
    rows_all, width = q_ref.shape[1:]
    chunks = pl.cdiv(length, bk)
    for pair in range(width // PAIR):
        cols = pl.ds(PAIR * pair, PAIR)
        transposed_chunks(vt_ref, v_ref, cols, bk)
        queries = [of_head(q_ref[0, :, cols], h) for h in range(2)]

        def score(j, tops):
            keys = k_ref[0, pl.ds(pl.multiple_of(j * bk, bk), bk), cols]
            ok = valid_rows(j, bk, length)
            out = []
            for h in range(2):
                s = jnp.where(ok, dot(keys, queries[h], NT), NEGATIVE)
                s_ref[h, j] = s
                top = tops[h]
                for i in range(bk // 8):
                    top = jnp.maximum(top, s[8 * i : 8 * i + 8])
                out.append(top)
            return tuple(out)

        low = jnp.full((8, rows_all), NEGATIVE, F32)
        tops = lax.fori_loop(0, chunks, score, (low, low))
        peaks = [jnp.max(top, axis=0, keepdims=True) * SCALE2 for top in tops]
        ot_ref[...] = jnp.zeros_like(ot_ref)

        def mix(j, sums):
            out = []
            for h in range(2):
                p = jnp.exp2(s_ref[h, j] * SCALE2 - peaks[h])
                total = sums[h]
                for i in range(bk // 8):
                    total = total + p[8 * i : 8 * i + 8]
                out.append(total)
                half = pl.ds(HEAD_DIM * h, HEAD_DIM)
                ot_ref[half] += dot(vt_ref[j, half], p.astype(BF16))
            return tuple(out)

        zero = jnp.zeros((8, rows_all), F32)
        sums = lax.fori_loop(0, chunks, mix, (zero, zero))
        for h in range(2):
            total = jnp.sum(sums[h], axis=0, keepdims=True)
            half = pl.ds(HEAD_DIM * h, HEAD_DIM)
            lse_ref[0, pl.ds(2 * pair + h, 1)] = peaks[h] + jnp.log2(total)
            ot_ref[half] = ot_ref[half] / total
        o_ref[0, :, cols] = jnp.transpose(ot_ref[...]).astype(BF16)


def attend_back_kernel(
    len_ref, q_ref, k_ref, v_ref, do_ref, o_ref, lse_ref, d_ref, kt_ref, dqt_ref, *, bk
):
    length = len_ref[pl.program_id(0)]
    width = q_ref.shape[2]
    chunks = pl.cdiv(length, bk)
    d_ref[...] = jnp.zeros_like(d_ref)
    for pair in range(width // PAIR):
        cols = pl.ds(PAIR * pair, PAIR)
        outs = do_ref[0, :, cols]
        both = jnp.transpose(outs.astype(F32) * o_ref[0, :, cols].astype(F32))
        inner = [
            jnp.sum(both[HEAD_DIM * h : HEAD_DIM * (h + 1)], axis=0, keepdims=True)
            for h in range(2)
        ]
        queries = [of_head(q_ref[0, :, cols], h) for h in range(2)]
        grads = [of_head(outs, h) for h in range(2)]
        logs = [lse_ref[0, pl.ds(2 * pair + h, 1)] for h in range(2)]
        transposed_chunks(kt_ref, k_ref, cols, bk)
        dqt_ref[...] = jnp.zeros_like(dqt_ref)

        def step(j, carry):
            rows = pl.ds(pl.multiple_of(j * bk, bk), bk)
            keys = k_ref[0, rows, cols]
            values = v_ref[0, rows, cols]
            ok = valid_rows(j, bk, length)
            dk = jnp.zeros((bk, PAIR), F32)
            dv = jnp.zeros((bk, PAIR), F32)
            for h in range(2):
                p = jnp.exp2(dot(keys, queries[h], NT) * SCALE2 - logs[h])
                p = jnp.where(ok, p, 0.0)
                g = (p * (dot(values, grads[h], NT) - inner[h])).astype(BF16)
                dv = dv + dot(p.astype(BF16), grads[h])
                dk = dk + dot(g, queries[h])
                half = pl.ds(HEAD_DIM * h, HEAD_DIM)
                dqt_ref[half] += dot(kt_ref[j, half], g)
            d_ref[0, rows, pl.ds(width + PAIR * pair, PAIR)] = (dk * SCALE).astype(BF16)
            d_ref[0, rows, pl.ds(2 * width + PAIR * pair, PAIR)] = dv.astype(BF16)
            return carry

        lax.fori_loop(0, chunks, step, 0)
        d_ref[0, :, cols] = jnp.transpose(dqt_ref[...] * SCALE).astype(BF16)


def chunk_rows(rows):
    return max(b for b in range(8, 225, 8) if rows % b == 0)


def block(rows, width, at):
    return pl.BlockSpec((1, rows, width), lambda c, n: (c, 0, at))


def attend(qkv, lengths):
    clips, rows, triple = qkv.shape
    width = triple // 3
    heads, bk = width // HEAD_DIM, chunk_rows(rows)
    cost = clips * heads * rows * rows
    return pl.pallas_call(
        functools.partial(attend_kernel, bk=bk),
        grid_spec=pltpu.PrefetchScalarGridSpec(
            num_scalar_prefetch=1,
            grid=(clips,),
            in_specs=[block(rows, width, i) for i in range(3)],
            out_specs=[block(rows, width, 0), block(heads, rows, 0)],
            scratch_shapes=[
                pltpu.VMEM((2, rows // bk, bk, rows), F32),
                pltpu.VMEM((rows // bk, PAIR, bk), BF16),
                pltpu.VMEM((PAIR, rows), F32),
            ],
        ),
        out_shape=[
            jax.ShapeDtypeStruct((clips, rows, width), BF16),
            jax.ShapeDtypeStruct((clips, heads, rows), F32),
        ],
        compiler_params=pltpu.CompilerParams(vmem_limit_bytes=40 << 20),
        cost_estimate=pl.CostEstimate(
            flops=cost * 1024, bytes_accessed=clips * rows * width * 8, transcendentals=cost
        ),
        name="attend",
    )(lengths, qkv, qkv, qkv)


def attend_back(qkv, grads, outs, logs, lengths):
    clips, rows, triple = qkv.shape
    width = triple // 3
    heads, bk = width // HEAD_DIM, chunk_rows(rows)
    cost = clips * heads * rows * rows
    return pl.pallas_call(
        functools.partial(attend_back_kernel, bk=bk),
        grid_spec=pltpu.PrefetchScalarGridSpec(
            num_scalar_prefetch=1,
            grid=(clips,),
            in_specs=[block(rows, width, i) for i in (0, 1, 2, 0, 0)] + [block(heads, rows, 0)],
            out_specs=block(rows, triple, 0),
            scratch_shapes=[
                pltpu.VMEM((rows // bk, PAIR, bk), BF16),
                pltpu.VMEM((PAIR, rows), F32),
            ],
        ),
        out_shape=jax.ShapeDtypeStruct((clips, rows, triple), BF16),
        compiler_params=pltpu.CompilerParams(vmem_limit_bytes=40 << 20),
        cost_estimate=pl.CostEstimate(
            flops=cost * 2560, bytes_accessed=clips * rows * width * 16, transcendentals=cost
        ),
        name="attend_back",
    )(lengths, qkv, qkv, qkv, grads, outs, logs)


def mlp_piece_kernel(
    core_ref, h_ref, ht_ref, dy_ref, mine_ref, other_ref, c1_ref, *rest, first, nz
):
    if first:
        y_ref, dh_ref, keep_ref, send_ref, sums_ref, hm_ref, hmt_ref, w1_ref, w2_ref, u_ref, dz_ref = rest
        yin_ref = dhin_ref = None
    else:
        yin_ref, dhin_ref, y_ref, dh_ref, keep_ref, send_ref, sums_ref, hm_ref, hmt_ref, w1_ref, w2_ref, u_ref, dz_ref = rest
    core = core_ref[0]
    width = h_ref.shape[1]
    rows = mine_ref.shape[2]
    half = nz * rows
    def at(i, p):
        block = 2 * i + (core if p == 0 else 1 - core)
        return pl.ds(pl.multiple_of(block * rows, rows), rows)
    def put(i, p):
        return pl.ds(p * half + i * rows, rows)
    for i in range(nz):
        for p in range(2):
            hm_ref[:, put(i, p)] = h_ref[:, at(i, p)]
            hmt_ref[put(i, p), :] = ht_ref[at(i, p), :]
            src = (mine_ref, other_ref)[p]
            w2_ref[pl.ds((2 * i + p) * rows, rows), :] = src[i, 1]
            for j in range(nz):
                for r in range(2):
                    w1_ref[put(i, p), pl.ds((2 * j + r) * rows, rows)] = src[i, 0, :, at(j, r)]
    for i in range(nz):
        cols = pl.ds(2 * i * rows, 2 * rows)
        bias = jnp.concatenate([c1_ref[:, at(i, p)] for p in range(2)], axis=1)
        z = dot(hm_ref[...], w1_ref[:, cols]) + bias
        phi = 0.5 * (1.0 + lax.erf(z * (2.0 ** -0.5)))
        u_ref[:, cols] = (z * phi).astype(BF16)
        slope = phi + z * (jnp.exp(z * z * -0.5) * 0.3989422804014327)
        dz = (dot(dy_ref[...], w2_ref[cols, :], NT) * slope).astype(BF16)
        dz_ref[:, cols] = dz
        s = jnp.sum(dz.astype(F32), axis=0, keepdims=True)
        for p in range(2):
            sums_ref[:, at(i, p)] = s[:, p * rows:(p + 1) * rows]
        g2 = dot(u_ref[:, cols], dy_ref[...], TN).astype(BF16)
        keep_ref[i, 1] = g2[:rows]
        send_ref[i, 1] = g2[rows:]
        g1 = dot(hmt_ref[...], dz_ref[:, cols]).astype(BF16)
        for p in range(2):
            part = g1[:, p * rows:(p + 1) * rows]
            keep_ref[:, 0, :, at(i, p)] = part[:half].reshape(nz, rows, rows)
            send_ref[:, 0, :, at(i, p)] = part[half:].reshape(nz, rows, rows)
    for n in range(width // 256):
        cols = pl.ds(256 * n, 256)
        y = dot(u_ref[...], w2_ref[:, cols])
        y_ref[:, cols] = y if first else y + yin_ref[:, cols]
    for n in range(width // 256):
        d = dot(dz_ref[...], w1_ref[pl.ds(256 * n, 256), :], NT)
        for q in range(256 // rows):
            p, i = divmod((256 // rows) * n + q, nz)
            v = d[:, q * rows:(q + 1) * rows]
            dh_ref[:, at(i, p)] = v if first else v + dhin_ref[:, at(i, p)]


def mlp_piece(core, h2, h2t, dy, mine, other, c1, acc):
    nz = mine.shape[0]
    t, width = h2.shape
    first = acc is None
    vm = pl.BlockSpec(memory_space=pltpu.VMEM)
    ins = [core, h2, h2t, dy, mine, other, c1] + ([] if first else list(acc))
    specs = [pl.BlockSpec(memory_space=pltpu.SMEM)] + [vm] * (len(ins) - 1)
    wide = jax.ShapeDtypeStruct((t, width), F32)
    return pl.pallas_call(
        functools.partial(mlp_piece_kernel, first=first, nz=nz),
        in_specs=specs,
        out_specs=[vm] * 5,
        out_shape=[wide, wide, jax.ShapeDtypeStruct(mine.shape, BF16), jax.ShapeDtypeStruct(mine.shape, BF16), jax.ShapeDtypeStruct(c1.shape, F32)],
        scratch_shapes=[pltpu.VMEM((t, width), BF16), pltpu.VMEM((width, t), BF16)] + [pltpu.VMEM((width, width), BF16)] * 2 + [pltpu.VMEM((t, width), BF16)] * 2,
        input_output_aliases={} if first else {7: 0, 8: 1},
        compiler_params=pltpu.CompilerParams(vmem_limit_bytes=40 << 20),
        cost_estimate=pl.CostEstimate(flops=12 * t * width * width, bytes_accessed=20 << 20, transcendentals=2 * t * width),
        name="mlp_piece",
    )(*ins)


def swap(value, ring, r):
    return lax.ppermute(value, "seq", [(i, i ^ r) for i in range(ring)])


def gather_seq(value, ring, me):
    out = jnp.zeros((ring,) + value.shape, value.dtype)
    cut = value.shape[0] // 16 * 8
    for r, part in enumerate(partners(value, ring, cut)):
        out = lax.dynamic_update_index_in_dim(out, part, me ^ r, 0)
    return out


def twin(value, devices):
    return lax.ppermute(value, "fsdp", [(i, i ^ 1) for i in range(devices)])


def partners(value, ring, cut):
    if ring != 4:
        return [value] + [swap(value, ring, r) for r in range(1, ring)]
    one, two = swap(value, ring, 1), swap(value, ring, 2)
    far = [swap(two[:cut], ring, 1), swap(one[cut:], ring, 2)]
    return [value, one, two, jnp.concatenate(far, axis=0)]


def sum_seq(terms, ring, me):
    total = lax.dynamic_index_in_dim(terms, me, 0, keepdims=False).astype(F32)
    for r in range(1, ring):
        term = lax.dynamic_index_in_dim(terms, me ^ r, 0, keepdims=False)
        total = total + swap(term, ring, r).astype(F32)
    return total


def to_owners(grad):
    return lax.psum_scatter(grad, "fsdp", scatter_dimension=0, tiled=True)


def sum_owned(owned, ring, me):
    rows, width = owned.shape
    part = sum_seq(owned.reshape(ring, rows // ring, width), ring, me).astype(BF16)
    return gather_seq(part, ring, me).reshape(rows, width).astype(F32)


def sum_vectors(rows, devices, ring):
    count, width = rows.shape
    sent = rows.reshape(count, devices, width // devices).transpose(1, 0, 2)
    total = jnp.sum(lax.all_to_all(sent, "fsdp", split_axis=0, concat_axis=0, tiled=True), axis=0)
    return total + sum(swap(total, ring, r) for r in range(1, ring))


def normalize(values):
    centered = values - jnp.mean(values, axis=-1, keepdims=True)
    variance = jnp.mean(centered * centered, axis=-1, keepdims=True)
    rstd = lax.rsqrt(variance + EPSILON)
    return centered * rstd, rstd


def normalize_back(grad, normed, rstd, gain):
    e = grad * gain
    mean = jnp.mean(e, axis=-1, keepdims=True)
    along = jnp.mean(e * normed, axis=-1, keepdims=True)
    return rstd * (e - mean - normed * along)


def shards(
    ring,
    devices,
    tokens,
    lengths,
    ln1_gain,
    ln1_bias,
    w_qkv,
    q_bias,
    v_bias,
    w_out,
    b_out,
    ln2_gain,
    ln2_bias,
    w_fc1,
    b_fc1,
    w_fc2,
    b_fc2,
    cotangent,
):
    clips, rows, width = tokens.shape
    total_rows = clips * rows
    clip_rows = rows * ring
    local = width // ring
    me = lax.axis_index("seq")

    whole = [gather_seq(tokens[c], ring, me).reshape(clip_rows, width) for c in range(clips)]

    own = ln1_gain.shape[0]
    packed = jnp.concatenate(
        [
            jnp.stack([ln1_gain, ln1_bias, q_bias, v_bias, b_out, ln2_gain, ln2_bias, b_fc2]),
            b_fc1.reshape(-1, own),
        ]
    )
    vectors = lax.all_gather(packed, "fsdp", axis=0, tiled=False)
    c1 = vectors[:, 8:].reshape(-1).astype(F32)
    vectors = vectors[:, :8].transpose(1, 0, 2).reshape(8, width).astype(F32)
    g1, b1, qb, vb, bo, g2, b2, c2 = (vectors[i] for i in range(8))
    qb_mine = lax.dynamic_slice_in_dim(qb, me * local, local)
    vb_mine = lax.dynamic_slice_in_dim(vb, me * local, local)
    bias_mine = jnp.concatenate([qb_mine, jnp.zeros_like(qb_mine), vb_mine])

    mine = lax.dynamic_index_in_dim(w_qkv.reshape(own, 3, ring, local), me, 2, keepdims=False)
    wqkv = lax.all_gather(mine.reshape(own, 3 * local), "fsdp", axis=0, tiled=True)
    wo = lax.all_gather(w_out, "fsdp", axis=0, tiled=True)
    quarters = ring == 4 and w_fc1.shape[1] == ring * width and devices % 2 == 0
    if quarters:
        core = lax.axis_index("fsdp") % 2
        same_core = [list(range(p, devices, 2)) for p in range(2)]
        part1 = lax.dynamic_index_in_dim(w_fc1.reshape(own, devices, ring, own), me, 2)
        part2 = lax.dynamic_index_in_dim(w_fc2.reshape(ring, own, width), me, 0)
        part = jnp.concatenate([part1.reshape(1, own, width), part2], axis=0)
        part = lax.all_gather(part, "fsdp", axis=0, axis_index_groups=same_core)
        pieces = [(p, twin(p, devices)) for p in partners(part, ring, devices // 4)]
    else:
        w1 = lax.all_gather(w_fc1, "fsdp", axis=0, tiled=True)
        w2 = lax.all_gather(w_fc2, "fsdp", axis=0, tiled=True)

    normed, qkv, heads_out, logs, attended = [], [], [], [], []
    for c in range(clips):
        n1 = normalize(whole[c].astype(F32))[0]
        h1 = (n1 * g1 + b1).astype(BF16)
        part = (dot(h1, wqkv) + bias_mine).astype(BF16)[None]
        out, log = attend(part, lax.dynamic_slice_in_dim(lengths, c, 1))
        moved = lax.all_to_all(
            out.reshape(ring, rows, local), "seq", split_axis=0, concat_axis=0, tiled=True
        )
        normed.append(h1)
        qkv.append(part)
        heads_out.append(out)
        logs.append(log)
        attended.append(moved.transpose(1, 0, 2).reshape(rows, width))
    attended = jnp.concatenate(attended, axis=0)

    inputs = tokens.astype(F32).reshape(total_rows, width)
    middle = inputs + (dot(attended, wo) + bo)
    n2, r2 = normalize(middle)
    h2 = (n2 * g2 + b2).astype(BF16)
    dy = cotangent.reshape(total_rows, width)
    dy_f = dy.astype(F32)
    if quarters:
        h2t, acc = h2.T, None
        terms, c1_sum = [None] * ring, jnp.zeros((ring, width), F32)
        for r in (1, 2, 3, 0):
            shift = lax.dynamic_index_in_dim(c1.reshape(devices, ring, own), me ^ r, 1)
            y, dh2, keep, send, sums = mlp_piece(
                core[None], h2, h2t, dy, *pieces[r], shift.reshape(1, width), acc
            )
            acc = (y, dh2)
            terms[r] = keep.astype(F32) + twin(send, devices).astype(F32)
            c1_sum = lax.dynamic_update_slice_in_dim(c1_sum, sums, me ^ r, 0)
        total = terms[0]
        for r in range(1, ring):
            total = total + swap(terms[r].astype(BF16), ring, r).astype(F32)
        mlp_terms = (total.astype(BF16),)
    else:
        z = dot(h2, w1) + c1
        phi = 0.5 * (1.0 + lax.erf(z * (2.0 ** -0.5)))
        hidden = (z * phi).astype(BF16)
        slope = phi + z * (jnp.exp(-0.5 * z * z) * 0.3989422804014327)
        y = dot(hidden, w2)
        dz = (dot(dy, w2, NT) * slope).astype(BF16)
        dh2 = dot(dz, w1, NT)
        mlp_terms = (dot(hidden, dy, TN).astype(BF16), dot(h2, dz, TN).astype(BF16))
        c1_sum = jnp.sum(dz.astype(F32), axis=0).reshape(devices, -1, own).transpose(1, 0, 2)
    layer_out = (middle + (y + c2)).astype(BF16).reshape(clips, rows, width)

    grad_middle = dy_f + normalize_back(dh2, n2, r2, g2)
    da = grad_middle.astype(BF16)
    term_wo = dot(attended, da, TN).astype(BF16)
    do = dot(da, wo, NT).astype(BF16)
    owned_wo = to_owners(term_wo)
    if quarters:
        owned_mlp = (
            lax.psum_scatter(
                mlp_terms[0], "fsdp", scatter_dimension=0, tiled=True, axis_index_groups=same_core
            ),
        )
    else:
        owned_mlp = tuple(to_owners(t) for t in mlp_terms)

    dqkv, own_terms, gain_sum, shift_sum = [], [], 0.0, 0.0
    for c in range(clips):
        sent = do[c * rows : (c + 1) * rows].reshape(rows, ring, local).transpose(1, 0, 2)
        moved = lax.all_to_all(sent, "seq", split_axis=0, concat_axis=0, tiled=True)
        moved = moved.reshape(1, clip_rows, local)
        d = attend_back(
            qkv[c], moved, heads_out[c], logs[c], lax.dynamic_slice_in_dim(lengths, c, 1)
        )[0]
        dh1 = dot(d, wqkv, NT)
        n1 = normalize(whole[c].astype(F32))[0]
        gain_sum = gain_sum + jnp.sum(dh1 * n1, axis=0)
        shift_sum = shift_sum + jnp.sum(dh1, axis=0)
        own_terms.append(sum_seq(dh1.astype(BF16).reshape(ring, rows, width), ring, me))
        dqkv.append(d)
    dqkv = jnp.concatenate(dqkv, axis=0)
    grad_mine = dot(jnp.concatenate(normed, axis=0), dqkv, TN).astype(BF16)
    grad_mine, owned_mlp, owned_wo = lax.optimization_barrier((grad_mine, owned_mlp, owned_wo))
    owned = to_owners(grad_mine)
    grad_wo = sum_owned(owned_wo, ring, me)
    if quarters:
        both = gather_seq(owned_mlp[0][0], ring, me).astype(F32)
        grad_w1 = both[:, 0].reshape(ring, own, devices, own).transpose(1, 2, 0, 3)
        grad_w1 = grad_w1.reshape(own, ring * width)
        grad_w2 = both[:, 1].reshape(ring * own, width)
    else:
        grad_w2, grad_w1 = (sum_owned(o, ring, me) for o in owned_mlp)
    grad_qkv = gather_seq(owned, ring, me).astype(F32)
    grad_qkv = jnp.concatenate(
        [grad_qkv[r, :, i * local : (i + 1) * local] for i in range(3) for r in range(ring)], axis=1
    )

    bias_sum = jnp.sum(dqkv.astype(F32), axis=0)
    zeros = jnp.zeros((width,), F32)
    first = jnp.stack(
        [
            gain_sum,
            shift_sum,
            lax.dynamic_update_slice_in_dim(zeros, bias_sum[:local], me * local, 0),
            lax.dynamic_update_slice_in_dim(zeros, bias_sum[2 * local :], me * local, 0),
        ]
    )
    second = jnp.stack(
        [
            jnp.sum(dh2 * n2, axis=0),
            jnp.sum(dh2, axis=0),
            jnp.sum(dy_f, axis=0),
            jnp.sum(da.astype(F32), axis=0),
        ]
    )
    second = jnp.concatenate([second, c1_sum.reshape(-1, width)])
    four = sum_vectors(second, devices, ring)
    grad_c1 = four[4:].reshape(-1)
    late = sum_vectors(first, devices, ring)

    terms = jnp.concatenate(own_terms, axis=0)
    n1, r1 = normalize(inputs)
    grad_inputs = (grad_middle + normalize_back(terms, n1, r1, g1)).reshape(clips, rows, width)
    return (
        layer_out,
        grad_inputs,
        late[0],
        late[1],
        grad_qkv,
        late[2],
        late[3],
        grad_wo,
        four[3],
        four[0],
        four[1],
        grad_w1,
        grad_c1,
        grad_w2,
        four[2],
    )


def solution(mesh):
    act, vec, mat = P("fsdp", "seq", None), P("fsdp"), P("fsdp", None)
    in_specs = (act, vec, vec, vec, mat, vec, vec, mat, vec, vec, vec, mat, vec, mat, vec, act)
    out_specs = (act, act, vec, vec, mat, vec, vec, mat, vec, vec, vec, mat, vec, mat, vec)
    return jax.shard_map(
        functools.partial(shards, mesh.shape["seq"], mesh.shape["fsdp"]),
        mesh=mesh,
        in_specs=in_specs,
        out_specs=out_specs,
        check_vma=False,
    )
```

```python
import functools

import jax
import jax.numpy as jnp
from jax import lax
from jax.experimental import pallas as pl
from jax.experimental.pallas import tpu as pltpu
from jax.sharding import PartitionSpec as P

HEAD_DIM = 64
PAIR = 2 * HEAD_DIM
EPSILON = 1e-06
NEGATIVE = -1e30
F32, BF16 = jnp.float32, jnp.bfloat16
SCALE = HEAD_DIM ** -0.5
SCALE2 = SCALE * 1.4426950408889634
NT = (((1,), (1,)), ((), ()))
NN = (((1,), (0,)), ((), ()))
TN = (((0,), (0,)), ((), ()))


def dot(a, b, dims=NN):
    return lax.dot_general(a, b, dims, preferred_element_type=F32)


WHOLE = pl.BlockSpec(memory_space=pltpu.VMEM)
SCALAR = pl.BlockSpec(memory_space=pltpu.SMEM)


def kernel_call(body, name, operands, outs, scratch=(), scalars=0, aliases=None, vmem=40):
    return pl.pallas_call(
        body,
        in_specs=[SCALAR] * scalars + [WHOLE] * (len(operands) - scalars),
        out_specs=[WHOLE] * len(outs),
        out_shape=[jax.ShapeDtypeStruct(*out) for out in outs],
        scratch_shapes=list(scratch),
        input_output_aliases=aliases or {},
        compiler_params=pltpu.CompilerParams(vmem_limit_bytes=vmem << 20),
        cost_estimate=pl.CostEstimate(flops=1 << 20, bytes_accessed=1 << 20, transcendentals=0),
        name=name,
    )(*operands)


def of_head(block, h):
    lane = lax.broadcasted_iota(jnp.int32, (1, PAIR), 1)
    return jnp.where(lane // HEAD_DIM == h, block, jnp.zeros_like(block))


def valid_rows(j, bk, length):
    return j * bk + lax.broadcasted_iota(jnp.int32, (bk, 1), 0) < length


def transposed_chunks(out_ref, in_ref, cols, bk):
    for j in range(in_ref.shape[1] // bk):
        out_ref[j] = jnp.transpose(in_ref[0, pl.ds(j * bk, bk), cols])


def attend_kernel(len_ref, q_ref, k_ref, v_ref, o_ref, lse_ref, s_ref, vt_ref, ot_ref, *, bk):
    length = len_ref[pl.program_id(0)]
    rows_all, width = q_ref.shape[1:]
    chunks = pl.cdiv(length, bk)
    for pair in range(width // PAIR):
        cols = pl.ds(PAIR * pair, PAIR)
        transposed_chunks(vt_ref, v_ref, cols, bk)
        queries = [of_head(q_ref[0, :, cols], h) for h in range(2)]

        def score(j, tops):
            keys = k_ref[0, pl.ds(pl.multiple_of(j * bk, bk), bk), cols]
            ok = valid_rows(j, bk, length)
            out = []
            for h in range(2):
                s = jnp.where(ok, dot(keys, queries[h], NT), NEGATIVE)
                s_ref[h, j] = s
                top = tops[h]
                for i in range(bk // 8):
                    top = jnp.maximum(top, s[8 * i : 8 * i + 8])
                out.append(top)
            return tuple(out)

        low = jnp.full((8, rows_all), NEGATIVE, F32)
        tops = lax.fori_loop(0, chunks, score, (low, low))
        peaks = [jnp.max(top, axis=0, keepdims=True) * SCALE2 for top in tops]
        ot_ref[...] = jnp.zeros_like(ot_ref)

        def mix(j, sums):
            out = []
            for h in range(2):
                p = jnp.exp2(s_ref[h, j] * SCALE2 - peaks[h])
                total = sums[h]
                for i in range(bk // 8):
                    total = total + p[8 * i : 8 * i + 8]
                out.append(total)
                half = pl.ds(HEAD_DIM * h, HEAD_DIM)
                ot_ref[half] += dot(vt_ref[j, half], p.astype(BF16))
            return tuple(out)

        zero = jnp.zeros((8, rows_all), F32)
        sums = lax.fori_loop(0, chunks, mix, (zero, zero))
        for h in range(2):
            total = jnp.sum(sums[h], axis=0, keepdims=True)
            half = pl.ds(HEAD_DIM * h, HEAD_DIM)
            lse_ref[0, pl.ds(2 * pair + h, 1)] = peaks[h] + jnp.log2(total)
            ot_ref[half] = ot_ref[half] / total
        o_ref[0, :, cols] = jnp.transpose(ot_ref[...]).astype(BF16)


def attend_back_kernel(
    len_ref, q_ref, k_ref, v_ref, do_ref, o_ref, lse_ref, d_ref, kt_ref, dqt_ref, *, bk
):
    length = len_ref[pl.program_id(0)]
    width = q_ref.shape[2]
    chunks = pl.cdiv(length, bk)
    d_ref[...] = jnp.zeros_like(d_ref)
    for pair in range(width // PAIR):
        cols = pl.ds(PAIR * pair, PAIR)
        outs = do_ref[0, :, cols]
        both = jnp.transpose(outs.astype(F32) * o_ref[0, :, cols].astype(F32))
        inner = [
            jnp.sum(both[HEAD_DIM * h : HEAD_DIM * (h + 1)], axis=0, keepdims=True)
            for h in range(2)
        ]
        queries = [of_head(q_ref[0, :, cols], h) for h in range(2)]
        grads = [of_head(outs, h) for h in range(2)]
        logs = [lse_ref[0, pl.ds(2 * pair + h, 1)] for h in range(2)]
        transposed_chunks(kt_ref, k_ref, cols, bk)
        dqt_ref[...] = jnp.zeros_like(dqt_ref)

        def step(j, carry):
            rows = pl.ds(pl.multiple_of(j * bk, bk), bk)
            keys = k_ref[0, rows, cols]
            values = v_ref[0, rows, cols]
            ok = valid_rows(j, bk, length)
            dk = jnp.zeros((bk, PAIR), F32)
            dv = jnp.zeros((bk, PAIR), F32)
            for h in range(2):
                p = jnp.exp2(dot(keys, queries[h], NT) * SCALE2 - logs[h])
                p = jnp.where(ok, p, 0.0)
                g = (p * (dot(values, grads[h], NT) - inner[h])).astype(BF16)
                dv = dv + dot(p.astype(BF16), grads[h])
                dk = dk + dot(g, queries[h])
                half = pl.ds(HEAD_DIM * h, HEAD_DIM)
                dqt_ref[half] += dot(kt_ref[j, half], g)
            d_ref[0, rows, pl.ds(width + PAIR * pair, PAIR)] = (dk * SCALE).astype(BF16)
            d_ref[0, rows, pl.ds(2 * width + PAIR * pair, PAIR)] = dv.astype(BF16)
            return carry

        lax.fori_loop(0, chunks, step, 0)
        d_ref[0, :, cols] = jnp.transpose(dqt_ref[...] * SCALE).astype(BF16)


def chunk_rows(rows):
    return max(b for b in range(8, 225, 8) if rows % b == 0)


def block(rows, width, at):
    return pl.BlockSpec((1, rows, width), lambda c, n: (c, 0, at))


def attend(qkv, lengths):
    clips, rows, triple = qkv.shape
    width = triple // 3
    heads, bk = width // HEAD_DIM, chunk_rows(rows)
    cost = clips * heads * rows * rows
    return pl.pallas_call(
        functools.partial(attend_kernel, bk=bk),
        grid_spec=pltpu.PrefetchScalarGridSpec(
            num_scalar_prefetch=1,
            grid=(clips,),
            in_specs=[block(rows, width, i) for i in range(3)],
            out_specs=[block(rows, width, 0), block(heads, rows, 0)],
            scratch_shapes=[
                pltpu.VMEM((2, rows // bk, bk, rows), F32),
                pltpu.VMEM((rows // bk, PAIR, bk), BF16),
                pltpu.VMEM((PAIR, rows), F32),
            ],
        ),
        out_shape=[
            jax.ShapeDtypeStruct((clips, rows, width), BF16),
            jax.ShapeDtypeStruct((clips, heads, rows), F32),
        ],
        compiler_params=pltpu.CompilerParams(vmem_limit_bytes=40 << 20),
        cost_estimate=pl.CostEstimate(
            flops=1 << 20, bytes_accessed=1 << 20, transcendentals=0
        ),
        name="attend",
    )(lengths, qkv, qkv, qkv)


def attend_back(qkv, grads, outs, logs, lengths):
    clips, rows, triple = qkv.shape
    width = triple // 3
    heads, bk = width // HEAD_DIM, chunk_rows(rows)
    cost = clips * heads * rows * rows
    return pl.pallas_call(
        functools.partial(attend_back_kernel, bk=bk),
        grid_spec=pltpu.PrefetchScalarGridSpec(
            num_scalar_prefetch=1,
            grid=(clips,),
            in_specs=[block(rows, width, i) for i in (0, 1, 2, 0, 0)] + [block(heads, rows, 0)],
            out_specs=block(rows, triple, 0),
            scratch_shapes=[
                pltpu.VMEM((rows // bk, PAIR, bk), BF16),
                pltpu.VMEM((PAIR, rows), F32),
            ],
        ),
        out_shape=jax.ShapeDtypeStruct((clips, rows, triple), BF16),
        compiler_params=pltpu.CompilerParams(vmem_limit_bytes=40 << 20),
        cost_estimate=pl.CostEstimate(
            flops=1 << 20, bytes_accessed=1 << 20, transcendentals=0
        ),
        name="attend_back",
    )(lengths, qkv, qkv, qkv, grads, outs, logs)


def norm_kernel(me_ref, *refs, places):
    parts, rest = refs[: len(places)], refs[len(places) :]
    g_ref, b_ref, w_ref, bias_ref, n_ref, h_ref, qkv_ref, x_ref = rest
    for r, place in enumerate(places):

        @pl.when(pl.program_id(0) == r)
        def _():
            x_ref[...] = parts[r][place]

    normed, _ = normalize(x_ref[...].astype(F32))
    h = (normed * g_ref[...] + b_ref[...]).astype(BF16)
    n_ref[0] = normed.astype(BF16)
    h_ref[0] = h
    qkv_ref[0] = (dot(h, w_ref[...]) + bias_ref[...]).astype(BF16)


def norm_project(me, parts, places, gain, shift, weight, bias):
    _, rows, width = parts[0].shape
    triple, ring = bias.shape[-1], len(parts)
    once = pl.BlockSpec(memory_space=pltpu.VMEM)

    def out(cols):
        return pl.BlockSpec((1, rows, cols), lambda r, m: (m[0] ^ r, 0, 0))

    normed, h, qkv = pl.pallas_call(
        functools.partial(norm_kernel, places=places),
        grid_spec=pltpu.PrefetchScalarGridSpec(
            num_scalar_prefetch=1,
            grid=(ring,),
            in_specs=[once] * (len(parts) + 2)
            + [pl.BlockSpec((width, triple), lambda r, m: (0, 0)), once],
            out_specs=[out(width), out(width), out(triple)],
            scratch_shapes=[pltpu.VMEM((rows, width), BF16)],
        ),
        out_shape=[jax.ShapeDtypeStruct((ring, rows, c), BF16) for c in (width, width, triple)],
        compiler_params=pltpu.CompilerParams(vmem_limit_bytes=32 << 20),
        cost_estimate=pl.CostEstimate(flops=1 << 20, bytes_accessed=1 << 20, transcendentals=0),
        name="norm_project",
    )(me[None], *parts, gain[None], shift[None], weight, bias[None])
    return (
        normed.reshape(ring * rows, width),
        h.reshape(ring * rows, width),
        qkv.reshape(1, ring * rows, triple),
    )


def mlp_piece_kernel(core_ref, h_ref, ht_ref, dy_ref, *refs, first, nz, counts):
    mines, others, refs = refs[: counts[0]], refs[counts[0] : sum(counts)], refs[sum(counts) :]
    c1_ref, *refs = refs
    yin_ref, dhin_ref = (None, None) if first else (refs.pop(0), refs.pop(0))
    y_ref, dh_ref, keep_ref, send_ref, sums_ref, hm_ref, hmt_ref, w1_ref, w2_ref, u_ref, dz_ref = refs
    core = core_ref[0]
    width = h_ref.shape[1]
    clips, _, share = ht_ref.shape
    rows = mines[0].shape[2]
    half = nz * rows

    def at(i, p):
        block = 2 * i + (core if p == 0 else 1 - core)
        return pl.ds(pl.multiple_of(block * rows, rows), rows)

    def put(i, p):
        return pl.ds(p * half + i * rows, rows)

    def source(i, p):
        parts = (mines, others)[p]
        size = nz // len(parts)
        return parts[i // size], i % size

    for i in range(nz):
        for p in range(2):
            hm_ref[:, put(i, p)] = h_ref[:, at(i, p)]
            for c in range(clips):
                hmt_ref[c, put(i, p), :] = ht_ref[c, at(i, p), :]
            src, z = source(i, p)
            w2_ref[pl.ds((2 * i + p) * rows, rows), :] = src[z, 1]
            for j in range(nz):
                for r in range(2):
                    w1_ref[put(i, p), pl.ds((2 * j + r) * rows, rows)] = src[z, 0, :, at(j, r)]
    for i in range(nz):
        cols = pl.ds(2 * i * rows, 2 * rows)
        bias = jnp.concatenate([c1_ref[:, at(i, p)] for p in range(2)], axis=1)
        z = dot(hm_ref[...], w1_ref[:, cols]) + bias
        phi = 0.5 * (1.0 + lax.erf(z * (2.0 ** -0.5)))
        u_ref[:, cols] = (z * phi).astype(BF16)
        slope = phi + z * (jnp.exp(z * z * -0.5) * 0.3989422804014327)
        dz = (dot(dy_ref[...], w2_ref[cols, :], NT) * slope).astype(BF16)
        dz_ref[:, cols] = dz
        total = jnp.sum(dz.astype(F32), axis=0, keepdims=True)
        for p in range(2):
            sums_ref[:, at(i, p)] = total[:, p * rows : (p + 1) * rows]
        g2 = dot(u_ref[:, cols], dy_ref[...], TN).astype(BF16)
        keep_ref[i, 1] = g2[:rows]
        send_ref[i, 1] = g2[rows:]
        g1 = sum(dot(hmt_ref[c], dz_ref[pl.ds(c * share, share), cols]) for c in range(clips))
        g1 = g1.astype(BF16)
        for p in range(2):
            part = g1[:, p * rows : (p + 1) * rows]
            keep_ref[:, 0, :, at(i, p)] = part[:half].reshape(nz, rows, rows)
            send_ref[:, 0, :, at(i, p)] = part[half:].reshape(nz, rows, rows)
    for n in range(width // 256):
        cols = pl.ds(256 * n, 256)
        y = dot(u_ref[...], w2_ref[:, cols])
        y_ref[:, cols] = y if first else y + yin_ref[:, cols]
    for n in range(width // 256):
        d = dot(dz_ref[...], w1_ref[pl.ds(256 * n, 256), :], NT)
        for q in range(256 // rows):
            p, i = divmod((256 // rows) * n + q, nz)
            v = d[:, q * rows : (q + 1) * rows]
            dh_ref[:, at(i, p)] = v if first else v + dhin_ref[:, at(i, p)]


def mlp_piece(core, h2, h2t, dy, mine, other, c1, acc):
    rows = mine[0].shape[2]
    t, width = h2.shape
    nz = width // (2 * rows)
    first = acc is None
    ins = [core, h2, h2t, dy, *mine, *other, c1] + ([] if first else list(acc))
    gradient = ((nz, 2, rows, width), BF16)
    return kernel_call(
        functools.partial(
            mlp_piece_kernel, first=first, nz=nz, counts=(len(mine), len(other))
        ),
        "mlp_piece",
        ins,
        [((t, width), F32), ((t, width), F32), gradient, gradient, (c1.shape, F32)],
        scratch=[pltpu.VMEM((t, width), BF16), pltpu.VMEM(h2t.shape, BF16)]
        + [pltpu.VMEM((width, width), BF16)] * 2
        + [pltpu.VMEM((t, width), BF16)] * 2,
        scalars=1,
        aliases={} if first else {len(ins) - 2: 0, len(ins) - 1: 1},
    )


def project_kernel(*refs, clips):
    moved, rest = refs[:clips], refs[clips:]
    x_ref, wo_ref, bo_ref, g_ref, b_ref, att_ref, mid_ref, h_ref, ht_ref = rest
    ring, rows, local = moved[0].shape
    for c in range(clips):
        at = pl.ds(c * rows, rows)
        for s in range(ring):
            att_ref[at, pl.ds(s * local, local)] = moved[c][s]
        middle = x_ref[c].astype(F32) + (dot(att_ref[at, :], wo_ref[...]) + bo_ref[...])
        mid_ref[at, :] = middle
        h = (normalize(middle)[0] * g_ref[...] + b_ref[...]).astype(BF16)
        h_ref[at, :] = h
        ht_ref[c] = jnp.transpose(h)


def project_norm(moved, tokens, wo, bo, gain, shift):
    clips, rows, width = tokens.shape
    flat = (clips * rows, width)
    return kernel_call(
        functools.partial(project_kernel, clips=clips),
        "project_norm",
        [*moved, tokens, wo, bo[None], gain[None], shift[None]],
        [(flat, BF16), (flat, F32), (flat, BF16), ((clips, width, rows), BF16)],
    )


def project_back_kernel(*refs, clips, count):
    y_ref, dh_ref, mid_ref, dy_ref, att_ref, wo_ref, g_ref, c2_ref = refs[:8]
    more, rest = refs[8 : 8 + count], refs[8 + count :]
    out_ref, gm_ref, gw_ref = rest[:3]
    do_refs, acc_ref, sum_ref = rest[3 : 3 + clips], rest[3 + clips], rest[4 + clips]
    ring, rows, local = do_refs[0].shape
    width = mid_ref.shape[1]
    sum_ref[...] = jnp.zeros_like(sum_ref)
    for c in range(clips):
        at = pl.ds(c * rows, rows)
        middle = mid_ref[at, :]
        out_ref[c] = (middle + (y_ref[at, :] + c2_ref[...])).astype(BF16)
        normed, rstd = normalize(middle)
        dh = dh_ref[at, :]
        dy = dy_ref[at, :].astype(F32)
        grad = dy + normalize_back(dh, normed, rstd, g_ref[...])
        gm_ref[c] = grad
        da = grad.astype(BF16)
        for i, terms in enumerate((dh * normed, dh, dy, da.astype(F32))):
            sum_ref[pl.ds(i, 1), :] += jnp.sum(terms, axis=0, keepdims=True)
        do = dot(da, wo_ref[...], NT).astype(BF16)
        for s in range(ring):
            do_refs[c][s] = do[:, s * local : (s + 1) * local]
        term = dot(att_ref[at, :], da, TN)
        acc_ref[...] = term if c == 0 else acc_ref[...] + term
    sum_ref[pl.ds(4, more[0].shape[0]), :] = more[0][...]
    gw_ref[:, pl.ds(0, width)] = acc_ref[...].astype(BF16)
    gw_ref[:, pl.ds(width, 128)] = jnp.transpose(sum_ref[...]).astype(BF16)


def project_back(y, dh, middle, dy, attended, wo, gain, c2, sums, shape, ring):
    clips, rows, width = shape
    local = width // ring
    outs = kernel_call(
        functools.partial(project_back_kernel, clips=clips, count=len(sums)),
        "project_back",
        [y, dh, middle, dy, attended, wo, gain[None], c2[None], *sums],
        [(shape, BF16), (shape, F32), ((width, width + 128), BF16)]
        + [((ring, rows, local), BF16)] * clips,
        scratch=[pltpu.VMEM((width, width), F32), pltpu.VMEM((128, width), F32)],
        vmem=56,
    )
    return outs[0], outs[1], outs[2], outs[3:]


def qkv_back_kernel(me_ref, d_ref, w_ref, n_ref, h_ref, *rest, ring, first, last):
    me = me_ref[0]
    rest = list(rest)
    acc_in, sum_in = (None, None) if first else (rest.pop(0), rest.pop(0))
    parts, (gw_ref, sum_ref) = rest[:ring], rest[ring:]
    triple = d_ref.shape[1]
    local = triple // 3
    rows = parts[0].shape[0]
    sum_ref[...] = jnp.zeros_like(sum_ref) if first else sum_in[...]
    for r in range(ring):
        at = pl.ds(pl.multiple_of((me ^ r) * rows, 8), rows)
        d = d_ref[at, :]
        dh = dot(d, w_ref[:, pl.ds(0, triple)], NT)
        parts[r][...] = dh.astype(parts[r].dtype)
        sum_ref[pl.ds(0, 1), :] += jnp.sum(dh * n_ref[at, :].astype(F32), axis=0, keepdims=True)
        sum_ref[pl.ds(1, 1), :] += jnp.sum(dh, axis=0, keepdims=True)
        bias = jnp.sum(d.astype(F32), axis=0, keepdims=True)
        at_me = pl.ds(pl.multiple_of(me * local, local), local)
        sum_ref[pl.ds(2, 1), at_me] += bias[:, :local]
        sum_ref[pl.ds(3, 1), at_me] += bias[:, 2 * local :]
    term = dot(h_ref[...], d_ref[...], TN)
    if not first:
        term = term + acc_in[...]
    if last:
        gw_ref[:, pl.ds(0, triple)] = term.astype(BF16)
        gw_ref[:, pl.ds(triple, 128)] = jnp.transpose(sum_ref[...]).astype(BF16)
    else:
        gw_ref[...] = term


def qkv_back(me, d, weight, normed, h, acc, ring, last):
    whole, triple = d.shape
    width = normed.shape[1]
    rows = whole // ring
    first = acc is None
    outs = [((rows, width), F32 if r == 0 else BF16) for r in range(ring)]
    outs.append(((width, triple + 128), BF16) if last else ((width, triple), F32))
    outs.append(((128, width), F32))
    results = kernel_call(
        functools.partial(qkv_back_kernel, ring=ring, first=first, last=last),
        "qkv_back",
        [me[None], d, weight, normed, h] + ([] if first else list(acc)),
        outs,
        scalars=1,
        vmem=56,
    )
    return results[:ring], (results[ring], results[ring + 1])


def tokens_back_kernel(*refs, count):
    terms, (x_ref, gm_ref, g_ref) = refs[:count], refs[count : count + 3]
    out_ref = refs[-1]
    grad = terms[0][...]
    for term in terms[1:]:
        grad = grad + term[...].astype(F32)
    normed, rstd = normalize(x_ref[0].astype(F32))
    out_ref[0] = gm_ref[0] + normalize_back(grad, normed, rstd, g_ref[...])


def tokens_back(c, terms, tokens, grad_middle, gain, out):
    clips, rows, width = tokens.shape
    at_c = pl.BlockSpec((1, rows, width), lambda i: (c, 0, 0))
    specs = [WHOLE] * len(terms) + [at_c, at_c, WHOLE]
    operands = [*terms, tokens, grad_middle, gain[None]]
    if out is not None:
        specs.append(pl.BlockSpec(memory_space=pl.ANY))
        operands.append(out)
    return pl.pallas_call(
        functools.partial(tokens_back_kernel, count=len(terms)),
        grid=(1,),
        in_specs=specs,
        out_specs=at_c,
        out_shape=jax.ShapeDtypeStruct((clips, rows, width), F32),
        input_output_aliases={} if out is None else {len(operands) - 1: 0},
        compiler_params=pltpu.CompilerParams(vmem_limit_bytes=32 << 20),
        cost_estimate=pl.CostEstimate(flops=1 << 20, bytes_accessed=1 << 20, transcendentals=0),
        name="tokens_back",
    )(*operands)


def swap(value, ring, r):
    return lax.ppermute(value, "seq", [(i, i ^ r) for i in range(ring)])


def gather_seq(value, ring, me):
    out = jnp.zeros((ring,) + value.shape, value.dtype)
    out = lax.dynamic_update_index_in_dim(out, value, me, 0)
    for r in range(1, ring):
        out = lax.dynamic_update_index_in_dim(out, swap(value, ring, r), me ^ r, 0)
    return out


def sum_seq(terms, ring, me):
    total = lax.dynamic_index_in_dim(terms, me, 0, keepdims=False).astype(F32)
    for r in range(1, ring):
        term = lax.dynamic_index_in_dim(terms, me ^ r, 0, keepdims=False)
        total = total + swap(term, ring, r).astype(F32)
    return total


def to_owners(grad):
    return lax.psum_scatter(grad, "fsdp", scatter_dimension=0, tiled=True)


def sum_owned(owned, ring, me):
    rows, width = owned.shape
    part = sum_seq(owned.reshape(ring, rows // ring, width), ring, me).astype(BF16)
    return gather_seq(part, ring, me).reshape(rows, width).astype(F32)


def sum_vectors(rows, devices, ring):
    count, width = rows.shape
    sent = rows.reshape(count, devices, width // devices).transpose(1, 0, 2)
    total = jnp.sum(lax.all_to_all(sent, "fsdp", split_axis=0, concat_axis=0, tiled=True), axis=0)
    return total + sum(swap(total, ring, r) for r in range(1, ring))


def normalize(values):
    centered = values - jnp.mean(values, axis=-1, keepdims=True)
    variance = jnp.mean(centered * centered, axis=-1, keepdims=True)
    rstd = lax.rsqrt(variance + EPSILON)
    return centered * rstd, rstd


def normalize_back(grad, normed, rstd, gain):
    e = grad * gain
    mean = jnp.mean(e, axis=-1, keepdims=True)
    along = jnp.mean(e * normed, axis=-1, keepdims=True)
    return rstd * (e - mean - normed * along)


def shards_any(
    ring,
    devices,
    tokens,
    lengths,
    ln1_gain,
    ln1_bias,
    w_qkv,
    q_bias,
    v_bias,
    w_out,
    b_out,
    ln2_gain,
    ln2_bias,
    w_fc1,
    b_fc1,
    w_fc2,
    b_fc2,
    cotangent,
):
    clips, rows, width = tokens.shape
    total_rows = clips * rows
    clip_rows = rows * ring
    local = width // ring
    me = lax.axis_index("seq")

    whole = [gather_seq(tokens[c], ring, me).reshape(clip_rows, width) for c in range(clips)]

    own = ln1_gain.shape[0]
    packed = jnp.concatenate(
        [
            jnp.stack([ln1_gain, ln1_bias, q_bias, v_bias, b_out, ln2_gain, ln2_bias, b_fc2]),
            b_fc1.reshape(-1, own),
        ]
    )
    vectors = lax.all_gather(packed, "fsdp", axis=0, tiled=False)
    c1 = vectors[:, 8:].reshape(-1).astype(F32)
    vectors = vectors[:, :8].transpose(1, 0, 2).reshape(8, width).astype(F32)
    g1, b1, qb, vb, bo, g2, b2, c2 = (vectors[i] for i in range(8))
    qb_mine = lax.dynamic_slice_in_dim(qb, me * local, local)
    vb_mine = lax.dynamic_slice_in_dim(vb, me * local, local)
    bias_mine = jnp.concatenate([qb_mine, jnp.zeros_like(qb_mine), vb_mine])

    mine = lax.dynamic_index_in_dim(w_qkv.reshape(own, 3, ring, local), me, 2, keepdims=False)
    wqkv = lax.all_gather(mine.reshape(own, 3 * local), "fsdp", axis=0, tiled=True)
    wo = lax.all_gather(w_out, "fsdp", axis=0, tiled=True)
    w1 = lax.all_gather(w_fc1, "fsdp", axis=0, tiled=True)
    w2 = lax.all_gather(w_fc2, "fsdp", axis=0, tiled=True)

    normed, qkv, heads_out, logs, attended = [], [], [], [], []
    for c in range(clips):
        n1 = normalize(whole[c].astype(F32))[0]
        h1 = (n1 * g1 + b1).astype(BF16)
        part = (dot(h1, wqkv) + bias_mine).astype(BF16)[None]
        out, log = attend(part, lax.dynamic_slice_in_dim(lengths, c, 1))
        moved = lax.all_to_all(
            out.reshape(ring, rows, local), "seq", split_axis=0, concat_axis=0, tiled=True
        )
        normed.append(h1)
        qkv.append(part)
        heads_out.append(out)
        logs.append(log)
        attended.append(moved.transpose(1, 0, 2).reshape(rows, width))
    attended = jnp.concatenate(attended, axis=0)

    inputs = tokens.astype(F32).reshape(total_rows, width)
    middle = inputs + (dot(attended, wo) + bo)
    n2, r2 = normalize(middle)
    h2 = (n2 * g2 + b2).astype(BF16)
    z = dot(h2, w1) + c1
    phi = 0.5 * (1.0 + lax.erf(z * (2.0 ** -0.5)))
    hidden = (z * phi).astype(BF16)
    slope = phi + z * (jnp.exp(-0.5 * z * z) * 0.3989422804014327)
    layer_out = (middle + (dot(hidden, w2) + c2)).astype(BF16).reshape(clips, rows, width)

    dy = cotangent.reshape(total_rows, width)
    dy_f = dy.astype(F32)
    term_w2 = dot(hidden, dy, TN).astype(BF16)
    dz = (dot(dy, w2, NT) * slope).astype(BF16)
    term_w1 = dot(h2, dz, TN).astype(BF16)
    dh2 = dot(dz, w1, NT)
    grad_middle = dy_f + normalize_back(dh2, n2, r2, g2)
    da = grad_middle.astype(BF16)
    term_wo = dot(attended, da, TN).astype(BF16)
    do = dot(da, wo, NT).astype(BF16)
    do, term_w2, term_w1, term_wo = lax.optimization_barrier((do, term_w2, term_w1, term_wo))
    owned_w2, owned_w1, owned_wo = (to_owners(t) for t in (term_w2, term_w1, term_wo))

    dqkv, own_terms, gain_sum, shift_sum = [], [], 0.0, 0.0
    for c in range(clips):
        sent = do[c * rows : (c + 1) * rows].reshape(rows, ring, local).transpose(1, 0, 2)
        moved = lax.all_to_all(sent, "seq", split_axis=0, concat_axis=0, tiled=True)
        moved = moved.reshape(1, clip_rows, local)
        d = attend_back(
            qkv[c], moved, heads_out[c], logs[c], lax.dynamic_slice_in_dim(lengths, c, 1)
        )[0]
        dh1 = dot(d, wqkv, NT)
        n1 = normalize(whole[c].astype(F32))[0]
        gain_sum = gain_sum + jnp.sum(dh1 * n1, axis=0)
        shift_sum = shift_sum + jnp.sum(dh1, axis=0)
        own_terms.append(sum_seq(dh1.astype(BF16).reshape(ring, rows, width), ring, me))
        dqkv.append(d)
    dqkv = jnp.concatenate(dqkv, axis=0)
    grad_mine = dot(jnp.concatenate(normed, axis=0), dqkv, TN).astype(BF16)
    grad_mine, owned_w2, owned_w1, owned_wo = lax.optimization_barrier(
        (grad_mine, owned_w2, owned_w1, owned_wo)
    )
    owned = to_owners(grad_mine)
    grad_w2, grad_w1, grad_wo = (sum_owned(o, ring, me) for o in (owned_w2, owned_w1, owned_wo))
    grad_qkv = gather_seq(owned, ring, me).astype(F32)
    grad_qkv = jnp.concatenate(
        [grad_qkv[r, :, i * local : (i + 1) * local] for i in range(3) for r in range(ring)], axis=1
    )

    bias_sum = jnp.sum(dqkv.astype(F32), axis=0)
    zeros = jnp.zeros((width,), F32)
    first = jnp.stack(
        [
            gain_sum,
            shift_sum,
            lax.dynamic_update_slice_in_dim(zeros, bias_sum[:local], me * local, 0),
            lax.dynamic_update_slice_in_dim(zeros, bias_sum[2 * local :], me * local, 0),
        ]
    )
    second = jnp.stack(
        [
            jnp.sum(dh2 * n2, axis=0),
            jnp.sum(dh2, axis=0),
            jnp.sum(dy_f, axis=0),
            jnp.sum(da.astype(F32), axis=0),
        ]
    )
    c1_sum = jnp.sum(dz.astype(F32), axis=0).reshape(devices, -1, own).transpose(1, 0, 2)
    second = jnp.concatenate([second, c1_sum.reshape(-1, width)])
    four = sum_vectors(second, devices, ring)
    grad_c1 = four[4:].reshape(-1)
    late = sum_vectors(first, devices, ring)

    terms = jnp.concatenate(own_terms, axis=0)
    n1, r1 = normalize(inputs)
    grad_inputs = (grad_middle + normalize_back(terms, n1, r1, g1)).reshape(clips, rows, width)
    return (
        layer_out,
        grad_inputs,
        late[0],
        late[1],
        grad_qkv,
        late[2],
        late[3],
        grad_wo,
        four[3],
        four[0],
        four[1],
        grad_w1,
        grad_c1,
        grad_w2,
        four[2],
    )


def twin(value, devices):
    return lax.ppermute(value, "fsdp", [(i, i ^ 1) for i in range(devices)])


def columns(vectors):
    vectors = jnp.pad(vectors.astype(BF16), ((0, -vectors.shape[0] % 128), (0, 0)))
    return dot(jnp.eye(vectors.shape[1], dtype=BF16), vectors, NT).astype(BF16)


def as_rows(block, count):
    return dot(block, jnp.eye(block.shape[0], dtype=BF16), TN)[:count]


def plus(a, b):
    return (a.astype(F32) + b.astype(F32)).astype(BF16)


def stage(*values):
    return lax.optimization_barrier(values)


def placed(parts, me):
    out = jnp.zeros((len(parts),) + parts[0].shape, parts[0].dtype)
    for r, part in enumerate(parts):
        out = lax.dynamic_update_index_in_dim(out, part, me ^ r, 0)
    return out


def shards(
    ring,
    devices,
    tokens,
    lengths,
    ln1_gain,
    ln1_bias,
    w_qkv,
    q_bias,
    v_bias,
    w_out,
    b_out,
    ln2_gain,
    ln2_bias,
    w_fc1,
    b_fc1,
    w_fc2,
    b_fc2,
    cotangent,
):
    clips, rows, width = tokens.shape
    total_rows, clip_rows, local = clips * rows, rows * ring, width // ring
    own, half, cut = ln1_gain.shape[0], clips // 2, devices // 4
    me, core = lax.axis_index("seq"), lax.axis_index("fsdp") % 2
    same_core = [list(range(p, devices, 2)) for p in range(2)]

    def over(value, r):
        return swap(value, ring, r)

    vectors = jnp.concatenate(
        [
            jnp.stack([ln1_gain, ln1_bias, q_bias, v_bias, b_out, ln2_gain, ln2_bias, b_fc2]),
            b_fc1.reshape(-1, own),
        ]
    )
    count = vectors.shape[0]
    mine = lax.dynamic_index_in_dim(w_qkv.reshape(own, 3, ring, local), me, 2, keepdims=False)
    mine = jnp.concatenate([mine.reshape(own, 3 * local), columns(vectors)], axis=1)
    mine = lax.all_gather(mine, "fsdp", axis=0, tiled=True)
    part1 = lax.dynamic_index_in_dim(w_fc1.reshape(own, devices, ring, own), me, 2)
    part2 = lax.dynamic_index_in_dim(w_fc2.reshape(ring, own, width), me, 0)
    quarter = jnp.concatenate([part1.reshape(1, own, width), part2], axis=0)
    quarter = lax.all_gather(quarter, "fsdp", axis=0, axis_index_groups=same_core)
    wo = lax.all_gather(w_out, "fsdp", axis=0, tiled=True)

    one, two = stage(over(tokens, 1), over(tokens, 2))
    far = [over(two[:half], 1), over(one[half:], 2)]
    mine, *far = stage(mine, *far)
    vectors = as_rows(mine[:, 3 * local :], count)
    g1, b1, qb, vb, bo, g2, b2, c2 = (vectors[i] for i in range(8))
    c1_rows = vectors[8:]
    qb_mine = lax.dynamic_slice_in_dim(qb, me * local, local)
    vb_mine = lax.dynamic_slice_in_dim(vb, me * local, local)
    bias_mine = jnp.concatenate([qb_mine, jnp.zeros_like(qb_mine), vb_mine])

    norms, normed, qkv, outs, logs = ([None] * clips for _ in range(5))

    def project(c):
        parts = [tokens, one, two, far[int(c >= half)]]
        places = [c, c, c, c % half]
        norms[c], normed[c], qkv[c] = norm_project(me, parts, places, g1, b1, mine, bias_mine)

    def to_rows(out):
        return lax.all_to_all(
            out.reshape(ring, rows, local), "seq", split_axis=0, concat_axis=0, tiled=True
        )

    def length(c):
        return lax.dynamic_slice_in_dim(lengths, c, 1)

    project(0)
    qkv[0], quarter = stage(qkv[0], quarter)
    near = [over(quarter, 1), over(quarter, 2)]
    outs[0], logs[0] = attend(qkv[0], length(0))
    moved = []
    for c in range(1, clips):
        moved.append(to_rows(outs[c - 1]))
        project(c)
        outs[c], logs[c] = attend(qkv[c], length(c))
    moved.append(to_rows(outs[-1]))
    *moved, near1, near2 = stage(*moved, *near)
    near = [near1, near2]
    far = [over(near[1][:cut], 1), over(near[0][cut:], 2)]
    twins = [twin(quarter, devices)] + [twin(n, devices) for n in near]
    attended, middle, h2, h2t = project_norm(moved, tokens, wo, bo, g2, b2)
    dy = cotangent.reshape(total_rows, width)

    sums = [None] * ring

    def quarter_of(r, mine_r, twin_r, acc):
        shift = lax.dynamic_index_in_dim(c1_rows, me ^ r, 0)
        y, dh2, keep, send, sums[r] = mlp_piece(
            core[None], h2, h2t, dy, mine_r, twin_r, shift, acc
        )
        return (y, dh2), keep, send

    acc, keep0, send0 = quarter_of(0, [quarter], twins[:1], None)
    *acc, keep0, send0, far0, far1 = stage(*acc, keep0, send0, *far)
    far = [far0, far1]
    got0 = twin(send0, devices)
    acc, keep3, send3 = quarter_of(3, far, [twin(f, devices) for f in far], acc)
    *acc, keep3, send3, got0 = stage(*acc, keep3, send3, got0)
    got3 = twin(send3, devices)
    acc, keep1, send1 = quarter_of(1, near[:1], twins[1:2], acc)
    *acc, keep1, send1, got3 = stage(*acc, keep1, send1, got3)
    term3 = plus(keep3, got3)
    ends = [over(term3[:cut], 1), over(term3[cut:], 2)]
    got1 = twin(send1, devices)
    acc, keep2, send2 = quarter_of(2, near[1:], twins[2:], acc)
    *acc, keep2, send2, got1, end2, end1 = stage(*acc, keep2, send2, got1, *ends)
    y, dh2 = acc
    term1 = [plus(keep1[:cut], got1[:cut])]
    term1.append(plus(plus(keep1[cut:], got1[cut:]), end1))
    got2 = twin(send2, devices)
    term2 = [plus(plus(keep2[:cut], got2[:cut]), end2), plus(keep2[cut:], got2[cut:])]
    term2, term1 = stage(term2, term1)
    first = [over(term1[0], 1), over(term2[1], 2)]

    c1_sum = placed([v[0] for v in sums], me)
    layer_out, grad_middle, term_wo, heads = project_back(
        y, dh2, middle, dy, attended, wo, g2, c2, [c1_sum], tokens.shape, ring
    )
    *heads, term_wo, first1, first2 = stage(*heads, term_wo, *first)
    owned_wo = to_owners(term_wo)

    def to_heads(c):
        part = lax.all_to_all(heads[c], "seq", split_axis=0, concat_axis=0, tiled=True)
        return part.reshape(1, clip_rows, local)

    (moved,) = stage(to_heads(0))
    second = [over(term1[1], 1), over(term2[0], 2)]
    acc, flying, token_terms = None, [], [None] * clips
    for c in range(clips):
        later = [to_heads(c + 1)] if c + 1 < clips else []
        if c == clips - 1:
            owned_wo = owned_wo.reshape(ring, own // ring, width + 128)
            wo_terms = [lax.dynamic_index_in_dim(owned_wo, me ^ r, 0, False) for r in range(ring)]
            flying = flying + [over(t, r) for r, t in enumerate(wo_terms) if r]
        d = attend_back(qkv[c], moved, outs[c], logs[c], length(c))
        d, later, flying, second = lax.optimization_barrier((d, later, flying, second))
        moved = later[0] if later else None
        if c == clips - 1:
            wo_term = wo_terms[0].astype(F32) + sum(t.astype(F32) for t in flying[1 - ring :])
            wo_term = wo_term.astype(BF16)
        if c:
            token_terms[c - 1] = [kept, *flying[: ring - 1]]
        else:
            total = plus(keep0, got0).astype(F32)
            total = total + jnp.concatenate([first1, second[0]], axis=0).astype(F32)
            total = total + jnp.concatenate([second[1], first2], axis=0).astype(F32)
            owned_mlp = lax.psum_scatter(
                total.astype(BF16),
                "fsdp",
                scatter_dimension=0,
                tiled=True,
                axis_index_groups=same_core,
            )
            second = []
        (kept, *parts), acc = qkv_back(
            me, d[0], mine, norms[c], normed[c], acc, ring, c == clips - 1
        )
        flying = [over(p, r + 1) for r, p in enumerate(parts)]
    grad_mine, owned_mlp = stage(acc[0], owned_mlp)
    owned = to_owners(grad_mine)

    grad_inputs = None
    token_terms[-1] = [kept, *flying]
    for c in range(clips):
        grad_inputs = tokens_back(c, token_terms[c], tokens, grad_middle, g1, grad_inputs)

    grad_wo = gather_seq(wo_term, ring, me).reshape(own, width + 128).astype(F32)
    middle_sums = grad_wo[:, width:].T
    grad_wo = grad_wo[:, :width]
    both = gather_seq(owned_mlp[0], ring, me).astype(F32)
    grad_w1 = both[:, 0].reshape(ring, own, devices, own).transpose(1, 2, 0, 3)
    grad_w1 = grad_w1.reshape(own, ring * width)
    grad_w2 = both[:, 1].reshape(ring * own, width)
    grad_qkv = gather_seq(owned, ring, me).astype(F32)
    last_sums = jnp.sum(grad_qkv[:, :, 3 * local :], axis=0).T
    grad_qkv = jnp.concatenate(
        [grad_qkv[r, :, i * local : (i + 1) * local] for i in range(3) for r in range(ring)], axis=1
    )

    return (
        layer_out,
        grad_inputs,
        last_sums[0],
        last_sums[1],
        grad_qkv,
        last_sums[2],
        last_sums[3],
        grad_wo,
        middle_sums[3],
        middle_sums[0],
        middle_sums[1],
        grad_w1,
        middle_sums[4 : count - 4].reshape(-1),
        grad_w2,
        middle_sums[2],
    )


def solution(mesh):
    act, vec, mat = P("fsdp", "seq", None), P("fsdp"), P("fsdp", None)
    in_specs = (act, vec, vec, vec, mat, vec, vec, mat, vec, vec, vec, mat, vec, mat, vec, act)
    out_specs = (act, act, vec, vec, mat, vec, vec, mat, vec, vec, vec, mat, vec, mat, vec)
    ring, devices = mesh.shape["seq"], mesh.shape["fsdp"]

    def layer(*args):
        clips, rows, width = args[0].shape
        square = ring == 4 and args[11].shape[1] == ring * width and devices % 4 == 0
        square = square and clips % (2 * devices) == 0 and width % (128 * devices) == 0
        return jax.shard_map(
            functools.partial(shards if square else shards_any, ring, devices),
            mesh=mesh,
            in_specs=in_specs,
            out_specs=out_specs,
            check_vma=False,
        )(*args)

    return layer
```

```python
import functools

import jax
import jax.numpy as jnp
from jax import lax
from jax.experimental import pallas as pl
from jax.experimental.pallas import tpu as pltpu
from jax.sharding import PartitionSpec as P

HEAD_DIM = 64
PAIR = 2 * HEAD_DIM
EPSILON = 1e-06
NEGATIVE = -1e30
F32, BF16 = jnp.float32, jnp.bfloat16
SCALE = HEAD_DIM ** -0.5
SCALE2 = SCALE * 1.4426950408889634
NT = (((1,), (1,)), ((), ()))
NN = (((1,), (0,)), ((), ()))
TN = (((0,), (0,)), ((), ()))


def dot(a, b, dims=NN):
    return lax.dot_general(a, b, dims, preferred_element_type=F32)


LARGE = 56 << 20
WHOLE = pl.BlockSpec(memory_space=pltpu.VMEM)
SCALAR = pl.BlockSpec(memory_space=pltpu.SMEM)


def kernel_call(body, name, operands, outs, scratch=(), scalars=0, aliases=None, vmem=40):
    return pl.pallas_call(
        body,
        in_specs=[SCALAR] * scalars + [WHOLE] * (len(operands) - scalars),
        out_specs=[WHOLE] * len(outs),
        out_shape=[jax.ShapeDtypeStruct(*out) for out in outs],
        scratch_shapes=list(scratch),
        input_output_aliases=aliases or {},
        compiler_params=pltpu.CompilerParams(vmem_limit_bytes=vmem << 20),
        cost_estimate=pl.CostEstimate(flops=1 << 20, bytes_accessed=1 << 20, transcendentals=0),
        name=name,
    )(*operands)


def of_head(block, h):
    lane = lax.broadcasted_iota(jnp.int32, (1, PAIR), 1)
    return jnp.where(lane // HEAD_DIM == h, block, jnp.zeros_like(block))


def valid_rows(j, bk, length):
    return j * bk + lax.broadcasted_iota(jnp.int32, (bk, 1), 0) < length


def transposed_chunks(out_ref, in_ref, cols, bk):
    for j in range(in_ref.shape[1] // bk):
        out_ref[j] = jnp.transpose(in_ref[0, pl.ds(j * bk, bk), cols])


def attend_kernel(len_ref, q_ref, k_ref, v_ref, o_ref, lse_ref, s_ref, vt_ref, ot_ref, *, bk):
    length = len_ref[pl.program_id(0)]
    rows_all, width = q_ref.shape[1:]
    chunks = pl.cdiv(length, bk)
    for pair in range(width // PAIR):
        cols = pl.ds(PAIR * pair, PAIR)
        transposed_chunks(vt_ref, v_ref, cols, bk)
        queries = [of_head(q_ref[0, :, cols], h) for h in range(2)]

        def score(j, tops):
            keys = k_ref[0, pl.ds(pl.multiple_of(j * bk, bk), bk), cols]
            ok = valid_rows(j, bk, length)
            out = []
            for h in range(2):
                s = jnp.where(ok, dot(keys, queries[h], NT), NEGATIVE)
                s_ref[h, j] = s
                top = tops[h]
                for i in range(bk // 8):
                    top = jnp.maximum(top, s[8 * i : 8 * i + 8])
                out.append(top)
            return tuple(out)

        low = jnp.full((8, rows_all), NEGATIVE, F32)
        tops = lax.fori_loop(0, chunks, score, (low, low))
        peaks = [jnp.max(top, axis=0, keepdims=True) * SCALE2 for top in tops]
        ot_ref[...] = jnp.zeros_like(ot_ref)

        def mix(j, sums):
            out = []
            for h in range(2):
                p = jnp.exp2(s_ref[h, j] * SCALE2 - peaks[h])
                total = sums[h]
                for i in range(bk // 8):
                    total = total + p[8 * i : 8 * i + 8]
                out.append(total)
                half = pl.ds(HEAD_DIM * h, HEAD_DIM)
                ot_ref[half] += dot(vt_ref[j, half], p.astype(BF16))
            return tuple(out)

        zero = jnp.zeros((8, rows_all), F32)
        sums = lax.fori_loop(0, chunks, mix, (zero, zero))
        for h in range(2):
            total = jnp.sum(sums[h], axis=0, keepdims=True)
            half = pl.ds(HEAD_DIM * h, HEAD_DIM)
            lse_ref[0, pl.ds(2 * pair + h, 1)] = peaks[h] + jnp.log2(total)
            ot_ref[half] = ot_ref[half] / total
        o_ref[0, :, cols] = jnp.transpose(ot_ref[...]).astype(BF16)


def attend_back_kernel(
    len_ref, q_ref, k_ref, v_ref, do_ref, o_ref, lse_ref, d_ref, kt_ref, dqt_ref, *, bk
):
    length = len_ref[pl.program_id(0)]
    width = q_ref.shape[2]
    chunks = pl.cdiv(length, bk)
    d_ref[...] = jnp.zeros_like(d_ref)
    for pair in range(width // PAIR):
        cols = pl.ds(PAIR * pair, PAIR)
        outs = do_ref[0, :, cols]
        both = jnp.transpose(outs.astype(F32) * o_ref[0, :, cols].astype(F32))
        inner = [
            jnp.sum(both[HEAD_DIM * h : HEAD_DIM * (h + 1)], axis=0, keepdims=True)
            for h in range(2)
        ]
        queries = [of_head(q_ref[0, :, cols], h) for h in range(2)]
        grads = [of_head(outs, h) for h in range(2)]
        logs = [lse_ref[0, pl.ds(2 * pair + h, 1)] for h in range(2)]
        transposed_chunks(kt_ref, k_ref, cols, bk)
        dqt_ref[...] = jnp.zeros_like(dqt_ref)

        def step(j, carry):
            rows = pl.ds(pl.multiple_of(j * bk, bk), bk)
            keys = k_ref[0, rows, cols]
            values = v_ref[0, rows, cols]
            ok = valid_rows(j, bk, length)
            dk = jnp.zeros((bk, PAIR), F32)
            dv = jnp.zeros((bk, PAIR), F32)
            for h in range(2):
                p = jnp.exp2(dot(keys, queries[h], NT) * SCALE2 - logs[h])
                p = jnp.where(ok, p, 0.0)
                g = (p * (dot(values, grads[h], NT) - inner[h])).astype(BF16)
                dv = dv + dot(p.astype(BF16), grads[h])
                dk = dk + dot(g, queries[h])
                half = pl.ds(HEAD_DIM * h, HEAD_DIM)
                dqt_ref[half] += dot(kt_ref[j, half], g)
            d_ref[0, rows, pl.ds(width + PAIR * pair, PAIR)] = (dk * SCALE).astype(BF16)
            d_ref[0, rows, pl.ds(2 * width + PAIR * pair, PAIR)] = dv.astype(BF16)
            return carry

        lax.fori_loop(0, chunks, step, 0)
        d_ref[0, :, cols] = jnp.transpose(dqt_ref[...] * SCALE).astype(BF16)


def chunk_rows(rows):
    return max(b for b in range(8, 225, 8) if rows % b == 0)


def block(rows, width, at):
    return pl.BlockSpec((1, rows, width), lambda c, n: (c, 0, at))


def attend(qkv, lengths):
    clips, rows, triple = qkv.shape
    width = triple // 3
    heads, bk = width // HEAD_DIM, chunk_rows(rows)
    cost = clips * heads * rows * rows
    return pl.pallas_call(
        functools.partial(attend_kernel, bk=bk),
        grid_spec=pltpu.PrefetchScalarGridSpec(
            num_scalar_prefetch=1,
            grid=(clips,),
            in_specs=[block(rows, width, i) for i in range(3)],
            out_specs=[block(rows, width, 0), block(heads, rows, 0)],
            scratch_shapes=[
                pltpu.VMEM((2, rows // bk, bk, rows), F32),
                pltpu.VMEM((rows // bk, PAIR, bk), BF16),
                pltpu.VMEM((PAIR, rows), F32),
            ],
        ),
        out_shape=[
            jax.ShapeDtypeStruct((clips, rows, width), BF16),
            jax.ShapeDtypeStruct((clips, heads, rows), F32),
        ],
        compiler_params=pltpu.CompilerParams(vmem_limit_bytes=LARGE),
        cost_estimate=pl.CostEstimate(
            flops=1 << 20, bytes_accessed=1 << 20, transcendentals=0
        ),
        name="attend",
    )(lengths, qkv, qkv, qkv)


def attend_back(qkv, grads, outs, logs, lengths):
    clips, rows, triple = qkv.shape
    width = triple // 3
    heads, bk = width // HEAD_DIM, chunk_rows(rows)
    cost = clips * heads * rows * rows
    return pl.pallas_call(
        functools.partial(attend_back_kernel, bk=bk),
        grid_spec=pltpu.PrefetchScalarGridSpec(
            num_scalar_prefetch=1,
            grid=(clips,),
            in_specs=[block(rows, width, i) for i in (0, 1, 2, 0, 0)] + [block(heads, rows, 0)],
            out_specs=block(rows, triple, 0),
            scratch_shapes=[
                pltpu.VMEM((rows // bk, PAIR, bk), BF16),
                pltpu.VMEM((PAIR, rows), F32),
            ],
        ),
        out_shape=jax.ShapeDtypeStruct((clips, rows, triple), BF16),
        compiler_params=pltpu.CompilerParams(vmem_limit_bytes=LARGE),
        cost_estimate=pl.CostEstimate(
            flops=1 << 20, bytes_accessed=1 << 20, transcendentals=0
        ),
        name="attend_back",
    )(lengths, qkv, qkv, qkv, grads, outs, logs)


def norm_kernel(me_ref, *refs, counts):
    parts, rest = refs[: sum(counts)], refs[sum(counts) :]
    g_ref, b_ref, w_ref, bias_ref, n_ref, h_ref, qkv_ref, x_ref = rest
    taken = 0
    for r, count in enumerate(counts):
        group = parts[taken : taken + count]
        taken += count

        @pl.when(pl.program_id(0) == r)
        def _():
            row = 0
            for ref in group:
                x_ref[pl.ds(row, ref.shape[0])] = ref[...]
                row += ref.shape[0]

    normed, _ = normalize(x_ref[...].astype(F32))
    h = (normed * g_ref[...] + b_ref[...]).astype(BF16)
    n_ref[0] = normed.astype(BF16)
    h_ref[0] = h
    qkv_ref[0] = (dot(h, w_ref[...]) + bias_ref[...]).astype(BF16)


def norm_project(me, groups, gain, shift, weight, bias):
    flat = [part if isinstance(part, tuple) else (part, None) for g in groups for part in g]
    triple, ring = bias.shape[-1], len(groups)
    rows, width = flat[0][0].shape[-2:]

    def part_spec(array, clip):
        if clip is None:
            return pl.BlockSpec(array.shape, lambda r, m: (0, 0))
        return pl.BlockSpec((None, rows, width), lambda r, m: (clip, 0, 0))

    def out(cols):
        return pl.BlockSpec((1, rows, cols), lambda r, m: (m[0] ^ r, 0, 0))

    normed, h, qkv = pl.pallas_call(
        functools.partial(norm_kernel, counts=[len(g) for g in groups]),
        grid_spec=pltpu.PrefetchScalarGridSpec(
            num_scalar_prefetch=1,
            grid=(ring,),
            in_specs=[part_spec(*part) for part in flat]
            + [WHOLE] * 2
            + [pl.BlockSpec((width, triple), lambda r, m: (0, 0)), WHOLE],
            out_specs=[out(width), out(width), out(triple)],
            scratch_shapes=[pltpu.VMEM((rows, width), BF16)],
        ),
        out_shape=[jax.ShapeDtypeStruct((ring, rows, c), BF16) for c in (width, width, triple)],
        compiler_params=pltpu.CompilerParams(vmem_limit_bytes=LARGE),
        cost_estimate=pl.CostEstimate(flops=1 << 20, bytes_accessed=1 << 20, transcendentals=0),
        name="norm_project",
    )(me[None], *[part[0] for part in flat], gain[None], shift[None], weight, bias[None])
    return (
        normed.reshape(ring * rows, width),
        h.reshape(ring * rows, width),
        qkv.reshape(1, ring * rows, triple),
    )


def mlp_piece_kernel(core_ref, h_ref, ht_ref, dy_ref, *refs, first, nz, counts):
    mines, others, refs = refs[: counts[0]], refs[counts[0] : sum(counts)], refs[sum(counts) :]
    c1_ref, *refs = refs
    yin_ref, dhin_ref = (None, None) if first else (refs.pop(0), refs.pop(0))
    y_ref, dh_ref, keep_ref, send_ref, sums_ref, hm_ref, hmt_ref, w1_ref, w2_ref, u_ref, dz_ref = refs
    core = core_ref[0]
    width = h_ref.shape[1]
    clips, _, share = ht_ref.shape
    rows = mines[0].shape[2]
    half = nz * rows

    def at(i, p):
        block = 2 * i + (core if p == 0 else 1 - core)
        return pl.ds(pl.multiple_of(block * rows, rows), rows)

    def put(i, p):
        return pl.ds(p * half + i * rows, rows)

    def source(i, p):
        parts = (mines, others)[p]
        size = nz // len(parts)
        return parts[i // size], i % size

    for i in range(nz):
        for p in range(2):
            hm_ref[:, put(i, p)] = h_ref[:, at(i, p)]
            for c in range(clips):
                hmt_ref[c, put(i, p), :] = ht_ref[c, at(i, p), :]
            src, z = source(i, p)
            w2_ref[pl.ds((2 * i + p) * rows, rows), :] = src[z, 1]
            for j in range(nz):
                for r in range(2):
                    w1_ref[put(i, p), pl.ds((2 * j + r) * rows, rows)] = src[z, 0, :, at(j, r)]
    for i in range(nz):
        cols = pl.ds(2 * i * rows, 2 * rows)
        bias = jnp.concatenate([c1_ref[:, at(i, p)] for p in range(2)], axis=1)
        z = dot(hm_ref[...], w1_ref[:, cols]) + bias
        phi = 0.5 * (1.0 + lax.erf(z * (2.0 ** -0.5)))
        u_ref[:, cols] = (z * phi).astype(BF16)
        slope = phi + z * (jnp.exp(z * z * -0.5) * 0.3989422804014327)
        dz = (dot(dy_ref[...], w2_ref[cols, :], NT) * slope).astype(BF16)
        dz_ref[:, cols] = dz
        total = jnp.sum(dz.astype(F32), axis=0, keepdims=True)
        for p in range(2):
            sums_ref[:, at(i, p)] = total[:, p * rows : (p + 1) * rows]
        g2 = dot(u_ref[:, cols], dy_ref[...], TN).astype(BF16)
        keep_ref[i, 1] = g2[:rows]
        send_ref[i, 1] = g2[rows:]
        g1 = sum(dot(hmt_ref[c], dz_ref[pl.ds(c * share, share), cols]) for c in range(clips))
        g1 = g1.astype(BF16)
        for p in range(2):
            part = g1[:, p * rows : (p + 1) * rows]
            keep_ref[:, 0, :, at(i, p)] = part[:half].reshape(nz, rows, rows)
            send_ref[:, 0, :, at(i, p)] = part[half:].reshape(nz, rows, rows)
    for n in range(width // 256):
        cols = pl.ds(256 * n, 256)
        y = dot(u_ref[...], w2_ref[:, cols])
        y_ref[:, cols] = y if first else y + yin_ref[:, cols]
    for n in range(width // 256):
        d = dot(dz_ref[...], w1_ref[pl.ds(256 * n, 256), :], NT)
        for q in range(256 // rows):
            p, i = divmod((256 // rows) * n + q, nz)
            v = d[:, q * rows : (q + 1) * rows]
            dh_ref[:, at(i, p)] = v if first else v + dhin_ref[:, at(i, p)]


def mlp_piece(core, h2, h2t, dy, mine, other, c1, acc):
    rows = mine[0].shape[2]
    t, width = h2.shape
    nz = width // (2 * rows)
    first = acc is None
    ins = [core, h2, h2t, dy, *mine, *other, c1] + ([] if first else list(acc))
    gradient = ((nz, 2, rows, width), BF16)
    return kernel_call(
        functools.partial(
            mlp_piece_kernel, first=first, nz=nz, counts=(len(mine), len(other))
        ),
        "mlp_piece",
        ins,
        [((t, width), F32), ((t, width), F32), gradient, gradient, (c1.shape, F32)],
        scratch=[pltpu.VMEM((t, width), BF16), pltpu.VMEM(h2t.shape, BF16)]
        + [pltpu.VMEM((width, width), BF16)] * 2
        + [pltpu.VMEM((t, width), BF16)] * 2,
        scalars=1,
        aliases={} if first else {len(ins) - 2: 0, len(ins) - 1: 1},
        vmem=24,
    )


def project_kernel(*refs, clips):
    moved, rest = refs[:clips], refs[clips:]
    x_ref, wo_ref, bo_ref, g_ref, b_ref, att_ref, mid_ref, h_ref, ht_ref = rest
    ring, rows, local = moved[0].shape
    for c in range(clips):
        at = pl.ds(c * rows, rows)
        for s in range(ring):
            att_ref[at, pl.ds(s * local, local)] = moved[c][s]
        middle = x_ref[c].astype(F32) + (dot(att_ref[at, :], wo_ref[...]) + bo_ref[...])
        mid_ref[at, :] = middle
        h = (normalize(middle)[0] * g_ref[...] + b_ref[...]).astype(BF16)
        h_ref[at, :] = h
        ht_ref[c] = jnp.transpose(h)


def project_norm(moved, tokens, wo, bo, gain, shift):
    clips, rows, width = tokens.shape
    flat = (clips * rows, width)
    return kernel_call(
        functools.partial(project_kernel, clips=clips),
        "project_norm",
        [*moved, tokens, wo, bo[None], gain[None], shift[None]],
        [(flat, BF16), (flat, F32), (flat, BF16), ((clips, width, rows), BF16)],
    )


def project_back_kernel(*refs, clip, first):
    y_ref, dh_ref, mid_ref, dy_ref, wo_ref, g_ref, c2_ref = refs[:7]
    out_ref, gm_ref, da_ref, do_ref, sum_ref = refs[-5:]
    ring, rows, local = do_ref.shape
    middle = mid_ref[...]
    out_ref[0] = (middle + (y_ref[...] + c2_ref[...])).astype(BF16)
    normed, rstd = normalize(middle)
    dh = dh_ref[...]
    dy = dy_ref[...].astype(F32)
    grad = dy + normalize_back(dh, normed, rstd, g_ref[...])
    gm_ref[0] = grad
    da = grad.astype(BF16)
    da_ref[...] = da
    do = dot(da, wo_ref[...], NT).astype(BF16)
    for s in range(ring):
        do_ref[s] = do[:, s * local : (s + 1) * local]
    sum_ref[...] = jnp.zeros_like(sum_ref)
    for i, terms in enumerate((dh * normed, dh, dy, da.astype(F32))):
        sum_ref[pl.ds(i, 1), :] = jnp.sum(terms, axis=0, keepdims=True)


def project_back(c, y, dh, middle, dy, wo, gain, c2, shape, ring, out, grad):
    clips, rows, width = shape
    at = pl.BlockSpec((rows, width), lambda i: (c, 0))
    at_c = pl.BlockSpec((1, rows, width), lambda i: (c, 0, 0))
    one = pl.BlockSpec((1, width), lambda i: (0, 0))
    back = [] if out is None else [out, grad]
    return pl.pallas_call(
        functools.partial(project_back_kernel, clip=c, first=out is None),
        grid=(1,),
        in_specs=[at] * 4
        + [pl.BlockSpec((width, width), lambda i: (0, 0)), one, one]
        + [pl.BlockSpec(memory_space=pl.ANY)] * len(back),
        out_specs=[
            at_c,
            at_c,
            pl.BlockSpec((rows, width), lambda i: (0, 0)),
            pl.BlockSpec((ring, rows, width // ring), lambda i: (0, 0, 0)),
            pl.BlockSpec((8, width), lambda i: (0, 0)),
        ],
        out_shape=[
            jax.ShapeDtypeStruct(shape, BF16),
            jax.ShapeDtypeStruct(shape, F32),
            jax.ShapeDtypeStruct((rows, width), BF16),
            jax.ShapeDtypeStruct((ring, rows, width // ring), BF16),
            jax.ShapeDtypeStruct((8, width), F32),
        ],
        input_output_aliases={7: 0, 8: 1} if back else {},
        compiler_params=pltpu.CompilerParams(vmem_limit_bytes=LARGE),
        cost_estimate=pl.CostEstimate(flops=1 << 20, bytes_accessed=1 << 20, transcendentals=0),
        name="project_back",
    )(y, dh, middle, dy, wo, gain[None], c2[None], *back)


def project_weight_kernel(*refs, clips):
    das, att_ref, sums = refs[:clips], refs[clips], refs[clips + 1 : 2 * clips + 1]
    c1_ref, gw_ref, sum_ref = refs[2 * clips + 1 :]
    rows, width = das[0].shape
    term = dot(att_ref[pl.ds(0, rows), :], das[0][...], TN)
    total = sums[0][...]
    for c in range(1, clips):
        term = term + dot(att_ref[pl.ds(c * rows, rows), :], das[c][...], TN)
        total = total + sums[c][...]
    sum_ref[...] = jnp.zeros_like(sum_ref)
    sum_ref[pl.ds(0, 8), :] = total
    sum_ref[pl.ds(4, c1_ref.shape[0]), :] = c1_ref[...]
    gw_ref[:, pl.ds(0, width)] = term.astype(BF16)
    gw_ref[:, pl.ds(width, 128)] = jnp.transpose(sum_ref[...]).astype(BF16)


def project_weight(das, attended, sums, c1_sum):
    width = attended.shape[1]
    return kernel_call(
        functools.partial(project_weight_kernel, clips=len(das)),
        "project_weight",
        [*das, attended, *sums, c1_sum],
        [((width, width + 128), BF16)],
        scratch=[pltpu.VMEM((128, width), F32)],
        vmem=56,
    )[0]


def qkv_back_kernel(me_ref, d_ref, w_ref, n_ref, *rest, first):
    sum_in = None if first else rest[0]
    part_ref, sum_ref = rest[-2:]
    local = d_ref.shape[1] // 3

    @pl.when(pl.program_id(0) == 0)
    def _():
        sum_ref[...] = jnp.zeros_like(sum_ref) if first else sum_in[...]

    d = d_ref[...]
    dh = dot(d, w_ref[...], NT)
    part_ref[0] = dh.astype(BF16)
    sum_ref[pl.ds(0, 1), :] += jnp.sum(dh * n_ref[...].astype(F32), axis=0, keepdims=True)
    sum_ref[pl.ds(1, 1), :] += jnp.sum(dh, axis=0, keepdims=True)
    bias = jnp.sum(d.astype(F32), axis=0, keepdims=True)
    at_me = pl.ds(pl.multiple_of(me_ref[0] * local, local), local)
    sum_ref[pl.ds(2, 1), at_me] += bias[:, :local]
    sum_ref[pl.ds(3, 1), at_me] += bias[:, 2 * local :]


def qkv_back(me, d, weight, normed, sums, ring):
    whole, triple = d.shape
    width, rows = normed.shape[1], whole // ring
    fixed = [] if sums is None else [sums]
    return pl.pallas_call(
        functools.partial(qkv_back_kernel, first=sums is None),
        grid_spec=pltpu.PrefetchScalarGridSpec(
            num_scalar_prefetch=1,
            grid=(ring,),
            in_specs=[
                pl.BlockSpec((rows, triple), lambda r, m: (r, 0)),
                pl.BlockSpec((width, triple), lambda r, m: (0, 0)),
                pl.BlockSpec((rows, width), lambda r, m: (r, 0)),
            ]
            + [pl.BlockSpec((8, width), lambda r, m: (0, 0)) for _ in fixed],
            out_specs=[
                pl.BlockSpec((1, rows, width), lambda r, m: (r, 0, 0)),
                pl.BlockSpec((8, width), lambda r, m: (0, 0)),
            ],
        ),
        out_shape=[
            jax.ShapeDtypeStruct((ring, rows, width), BF16),
            jax.ShapeDtypeStruct((8, width), F32),
        ],
        compiler_params=pltpu.CompilerParams(vmem_limit_bytes=LARGE),
        cost_estimate=pl.CostEstimate(flops=1 << 20, bytes_accessed=1 << 20, transcendentals=0),
        name="qkv_back",
    )(me[None], d, weight, normed, *fixed)


def qkv_weight_kernel(*refs, clips, ring):
    ds, hs = refs[:clips], refs[clips : 2 * clips]
    sum_ref, gw_ref, acc_ref, all_ref = refs[2 * clips :]
    step = pl.program_id(0)
    for c in range(clips):

        @pl.when(step // ring == c)
        def _():
            term = dot(hs[c][...], ds[c][...], TN)

            @pl.when(step == 0)
            def _():
                acc_ref[...] = term

            @pl.when(step > 0)
            def _():
                acc_ref[...] += term

    @pl.when(step == clips * ring - 1)
    def _():
        triple = acc_ref.shape[1]
        all_ref[...] = jnp.zeros_like(all_ref)
        all_ref[pl.ds(0, 8), :] = sum_ref[...]
        gw_ref[:, pl.ds(0, triple)] = acc_ref[...].astype(BF16)
        gw_ref[:, pl.ds(triple, 128)] = jnp.transpose(all_ref[...]).astype(BF16)


def qkv_weight(ds, hs, sums, ring):
    clips = len(ds)
    (whole, triple), width = ds[0].shape, hs[0].shape[1]
    rows = whole // ring

    def share(c, cols):
        def at(i):
            return jnp.clip(i - c * ring, 0, ring - 1), 0

        return pl.BlockSpec((rows, cols), at)

    return pl.pallas_call(
        functools.partial(qkv_weight_kernel, clips=clips, ring=ring),
        grid=(clips * ring,),
        in_specs=[share(c, triple) for c in range(clips)]
        + [share(c, width) for c in range(clips)]
        + [pl.BlockSpec((8, width), lambda i: (0, 0))],
        out_specs=pl.BlockSpec((width, triple + 128), lambda i: (0, 0)),
        out_shape=jax.ShapeDtypeStruct((width, triple + 128), BF16),
        scratch_shapes=[pltpu.VMEM((width, triple), F32), pltpu.VMEM((128, width), F32)],
        compiler_params=pltpu.CompilerParams(vmem_limit_bytes=LARGE),
        cost_estimate=pl.CostEstimate(flops=1 << 20, bytes_accessed=1 << 20, transcendentals=0),
        name="qkv_weight",
    )(*ds, *hs, sums)


def tokens_back_kernel(*refs, ring):
    term_ref, x_ref, gm_ref, g_ref = refs[:4]
    out_ref = refs[-1]
    grad = term_ref[0].astype(F32)
    for r in range(1, ring):
        grad = grad + term_ref[r].astype(F32)
    normed, rstd = normalize(x_ref[0].astype(F32))
    out_ref[0] = gm_ref[0] + normalize_back(grad, normed, rstd, g_ref[...])


def tokens_back(c, terms, tokens, grad_middle, gain, out):
    clips, rows, width = tokens.shape
    steps = max(n for n in (7, 4, 2, 1) if rows % (8 * n) == 0)
    block = rows // steps
    at_c = pl.BlockSpec((1, block, width), lambda i: (c, i, 0))
    ring = terms.shape[0]
    specs = [pl.BlockSpec((ring, block, width), lambda i: (0, i, 0)), at_c, at_c]
    specs.append(pl.BlockSpec((1, width), lambda i: (0, 0)))
    operands = [terms, tokens, grad_middle, gain[None]]
    if out is not None:
        specs.append(pl.BlockSpec(memory_space=pl.ANY))
        operands.append(out)
    return pl.pallas_call(
        functools.partial(tokens_back_kernel, ring=ring),
        grid=(steps,),
        in_specs=specs,
        out_specs=at_c,
        out_shape=jax.ShapeDtypeStruct((clips, rows, width), F32),
        input_output_aliases={} if out is None else {len(operands) - 1: 0},
        compiler_params=pltpu.CompilerParams(vmem_limit_bytes=LARGE),
        cost_estimate=pl.CostEstimate(flops=1 << 20, bytes_accessed=1 << 20, transcendentals=0),
        name="tokens_back",
    )(*operands)


def spread_mlp_kernel(part_ref, w1_ref, w2_ref, *, ring):
    own = part_ref.shape[2]
    for q in range(ring):
        part = part_ref[q, 0].astype(F32)
        for f in range(part.shape[1] // own):
            w1_ref[:, pl.ds((f * ring + q) * own, own)] = part[:, f * own : (f + 1) * own]
        w2_ref[pl.ds(q * own, own), :] = part_ref[q, 1].astype(F32)


def spread_mlp(parts):
    ring, _, own, width = parts.shape
    return kernel_call(
        functools.partial(spread_mlp_kernel, ring=ring),
        "spread_mlp",
        [parts],
        [((own, ring * width), F32), ((ring * own, width), F32)],
    )


def spread_attn_kernel(me_ref, *refs, ring):
    wo_refs, (qkv_ref, gwo_ref, gqkv_ref, vec_ref, more_ref) = refs[:ring], refs[ring:]
    own, width = gwo_ref.shape
    rows = wo_refs[0].shape[0]
    triple = qkv_ref.shape[2] - 128
    local = triple // 3
    for q in range(ring):
        at = pl.ds(pl.multiple_of((me_ref[0] ^ q) * rows, rows), rows)
        gwo_ref[at, :] = wo_refs[q][:, :width].astype(F32)
        more_ref[at, :] = wo_refs[q][:, width:].astype(F32)
        for i in range(3):
            part = qkv_ref[q, :, i * local : (i + 1) * local].astype(F32)
            gqkv_ref[:, pl.ds(i * width + q * local, local)] = part
    vec_ref[0] = jnp.transpose(more_ref[...])
    last = qkv_ref[0, :, triple:].astype(F32)
    for q in range(1, ring):
        last = last + qkv_ref[q, :, triple:].astype(F32)
    vec_ref[1] = jnp.transpose(last)


def spread_attn(me, wo_parts, qkv_parts):
    ring, own, _ = qkv_parts.shape
    width = wo_parts[0].shape[1] - 128
    return kernel_call(
        functools.partial(spread_attn_kernel, ring=ring),
        "spread_attn",
        [me[None], *wo_parts, qkv_parts],
        [((own, width), F32), ((own, 3 * width), F32), ((2, 128, own), F32)],
        scratch=[pltpu.VMEM((own, 128), F32)],
        scalars=1,
    )


def swap(value, ring, r):
    return lax.ppermute(value, "seq", [(i, i ^ r) for i in range(ring)])


def gather_seq(value, ring, me):
    out = jnp.zeros((ring,) + value.shape, value.dtype)
    out = lax.dynamic_update_index_in_dim(out, value, me, 0)
    for r in range(1, ring):
        out = lax.dynamic_update_index_in_dim(out, swap(value, ring, r), me ^ r, 0)
    return out


def sum_seq(terms, ring, me):
    total = lax.dynamic_index_in_dim(terms, me, 0, keepdims=False).astype(F32)
    for r in range(1, ring):
        term = lax.dynamic_index_in_dim(terms, me ^ r, 0, keepdims=False)
        total = total + swap(term, ring, r).astype(F32)
    return total


def to_owners(grad):
    return lax.psum_scatter(grad, "fsdp", scatter_dimension=0, tiled=True)


def sum_owned(owned, ring, me):
    rows, width = owned.shape
    part = sum_seq(owned.reshape(ring, rows // ring, width), ring, me).astype(BF16)
    return gather_seq(part, ring, me).reshape(rows, width).astype(F32)


def sum_vectors(rows, devices, ring):
    count, width = rows.shape
    sent = rows.reshape(count, devices, width // devices).transpose(1, 0, 2)
    total = jnp.sum(lax.all_to_all(sent, "fsdp", split_axis=0, concat_axis=0, tiled=True), axis=0)
    return total + sum(swap(total, ring, r) for r in range(1, ring))


def normalize(values):
    centered = values - jnp.mean(values, axis=-1, keepdims=True)
    variance = jnp.mean(centered * centered, axis=-1, keepdims=True)
    rstd = lax.rsqrt(variance + EPSILON)
    return centered * rstd, rstd


def normalize_back(grad, normed, rstd, gain):
    e = grad * gain
    mean = jnp.mean(e, axis=-1, keepdims=True)
    along = jnp.mean(e * normed, axis=-1, keepdims=True)
    return rstd * (e - mean - normed * along)


def shards_any(
    ring,
    devices,
    tokens,
    lengths,
    ln1_gain,
    ln1_bias,
    w_qkv,
    q_bias,
    v_bias,
    w_out,
    b_out,
    ln2_gain,
    ln2_bias,
    w_fc1,
    b_fc1,
    w_fc2,
    b_fc2,
    cotangent,
):
    clips, rows, width = tokens.shape
    total_rows = clips * rows
    clip_rows = rows * ring
    local = width // ring
    me = lax.axis_index("seq")

    whole = [gather_seq(tokens[c], ring, me).reshape(clip_rows, width) for c in range(clips)]

    own = ln1_gain.shape[0]
    packed = jnp.concatenate(
        [
            jnp.stack([ln1_gain, ln1_bias, q_bias, v_bias, b_out, ln2_gain, ln2_bias, b_fc2]),
            b_fc1.reshape(-1, own),
        ]
    )
    vectors = lax.all_gather(packed, "fsdp", axis=0, tiled=False)
    c1 = vectors[:, 8:].reshape(-1).astype(F32)
    vectors = vectors[:, :8].transpose(1, 0, 2).reshape(8, width).astype(F32)
    g1, b1, qb, vb, bo, g2, b2, c2 = (vectors[i] for i in range(8))
    qb_mine = lax.dynamic_slice_in_dim(qb, me * local, local)
    vb_mine = lax.dynamic_slice_in_dim(vb, me * local, local)
    bias_mine = jnp.concatenate([qb_mine, jnp.zeros_like(qb_mine), vb_mine])

    mine = lax.dynamic_index_in_dim(w_qkv.reshape(own, 3, ring, local), me, 2, keepdims=False)
    wqkv = lax.all_gather(mine.reshape(own, 3 * local), "fsdp", axis=0, tiled=True)
    wo = lax.all_gather(w_out, "fsdp", axis=0, tiled=True)
    w1 = lax.all_gather(w_fc1, "fsdp", axis=0, tiled=True)
    w2 = lax.all_gather(w_fc2, "fsdp", axis=0, tiled=True)

    normed, qkv, heads_out, logs, attended = [], [], [], [], []
    for c in range(clips):
        n1 = normalize(whole[c].astype(F32))[0]
        h1 = (n1 * g1 + b1).astype(BF16)
        part = (dot(h1, wqkv) + bias_mine).astype(BF16)[None]
        out, log = attend(part, lax.dynamic_slice_in_dim(lengths, c, 1))
        moved = lax.all_to_all(
            out.reshape(ring, rows, local), "seq", split_axis=0, concat_axis=0, tiled=True
        )
        normed.append(h1)
        qkv.append(part)
        heads_out.append(out)
        logs.append(log)
        attended.append(moved.transpose(1, 0, 2).reshape(rows, width))
    attended = jnp.concatenate(attended, axis=0)

    inputs = tokens.astype(F32).reshape(total_rows, width)
    middle = inputs + (dot(attended, wo) + bo)
    n2, r2 = normalize(middle)
    h2 = (n2 * g2 + b2).astype(BF16)
    z = dot(h2, w1) + c1
    phi = 0.5 * (1.0 + lax.erf(z * (2.0 ** -0.5)))
    hidden = (z * phi).astype(BF16)
    slope = phi + z * (jnp.exp(-0.5 * z * z) * 0.3989422804014327)
    layer_out = (middle + (dot(hidden, w2) + c2)).astype(BF16).reshape(clips, rows, width)

    dy = cotangent.reshape(total_rows, width)
    dy_f = dy.astype(F32)
    term_w2 = dot(hidden, dy, TN).astype(BF16)
    dz = (dot(dy, w2, NT) * slope).astype(BF16)
    term_w1 = dot(h2, dz, TN).astype(BF16)
    dh2 = dot(dz, w1, NT)
    grad_middle = dy_f + normalize_back(dh2, n2, r2, g2)
    da = grad_middle.astype(BF16)
    term_wo = dot(attended, da, TN).astype(BF16)
    do = dot(da, wo, NT).astype(BF16)
    do, term_w2, term_w1, term_wo = lax.optimization_barrier((do, term_w2, term_w1, term_wo))
    owned_w2, owned_w1, owned_wo = (to_owners(t) for t in (term_w2, term_w1, term_wo))

    dqkv, own_terms, gain_sum, shift_sum = [], [], 0.0, 0.0
    for c in range(clips):
        sent = do[c * rows : (c + 1) * rows].reshape(rows, ring, local).transpose(1, 0, 2)
        moved = lax.all_to_all(sent, "seq", split_axis=0, concat_axis=0, tiled=True)
        moved = moved.reshape(1, clip_rows, local)
        d = attend_back(
            qkv[c], moved, heads_out[c], logs[c], lax.dynamic_slice_in_dim(lengths, c, 1)
        )[0]
        dh1 = dot(d, wqkv, NT)
        n1 = normalize(whole[c].astype(F32))[0]
        gain_sum = gain_sum + jnp.sum(dh1 * n1, axis=0)
        shift_sum = shift_sum + jnp.sum(dh1, axis=0)
        own_terms.append(sum_seq(dh1.astype(BF16).reshape(ring, rows, width), ring, me))
        dqkv.append(d)
    dqkv = jnp.concatenate(dqkv, axis=0)
    grad_mine = dot(jnp.concatenate(normed, axis=0), dqkv, TN).astype(BF16)
    grad_mine, owned_w2, owned_w1, owned_wo = lax.optimization_barrier(
        (grad_mine, owned_w2, owned_w1, owned_wo)
    )
    owned = to_owners(grad_mine)
    grad_w2, grad_w1, grad_wo = (sum_owned(o, ring, me) for o in (owned_w2, owned_w1, owned_wo))
    grad_qkv = gather_seq(owned, ring, me).astype(F32)
    grad_qkv = jnp.concatenate(
        [grad_qkv[r, :, i * local : (i + 1) * local] for i in range(3) for r in range(ring)], axis=1
    )

    bias_sum = jnp.sum(dqkv.astype(F32), axis=0)
    zeros = jnp.zeros((width,), F32)
    first = jnp.stack(
        [
            gain_sum,
            shift_sum,
            lax.dynamic_update_slice_in_dim(zeros, bias_sum[:local], me * local, 0),
            lax.dynamic_update_slice_in_dim(zeros, bias_sum[2 * local :], me * local, 0),
        ]
    )
    second = jnp.stack(
        [
            jnp.sum(dh2 * n2, axis=0),
            jnp.sum(dh2, axis=0),
            jnp.sum(dy_f, axis=0),
            jnp.sum(da.astype(F32), axis=0),
        ]
    )
    c1_sum = jnp.sum(dz.astype(F32), axis=0).reshape(devices, -1, own).transpose(1, 0, 2)
    second = jnp.concatenate([second, c1_sum.reshape(-1, width)])
    four = sum_vectors(second, devices, ring)
    grad_c1 = four[4:].reshape(-1)
    late = sum_vectors(first, devices, ring)

    terms = jnp.concatenate(own_terms, axis=0)
    n1, r1 = normalize(inputs)
    grad_inputs = (grad_middle + normalize_back(terms, n1, r1, g1)).reshape(clips, rows, width)
    return (
        layer_out,
        grad_inputs,
        late[0],
        late[1],
        grad_qkv,
        late[2],
        late[3],
        grad_wo,
        four[3],
        four[0],
        four[1],
        grad_w1,
        grad_c1,
        grad_w2,
        four[2],
    )


def twin(value, devices):
    return lax.ppermute(value, "fsdp", [(i, i ^ 1) for i in range(devices)])


def columns(vectors):
    vectors = jnp.pad(vectors.astype(BF16), ((0, -vectors.shape[0] % 128), (0, 0)))
    return dot(jnp.eye(vectors.shape[1], dtype=BF16), vectors, NT).astype(BF16)


def as_rows(block, count):
    return dot(block, jnp.eye(block.shape[0], dtype=BF16), TN)[:count]


def plus(a, b):
    return (a.astype(F32) + b.astype(F32)).astype(BF16)


def stage(*values):
    return lax.optimization_barrier(values)


def placed(parts, me):
    out = jnp.zeros((len(parts),) + parts[0].shape, parts[0].dtype)
    for r, part in enumerate(parts):
        out = lax.dynamic_update_index_in_dim(out, part, me ^ r, 0)
    return out


def shards(
    ring,
    devices,
    tokens,
    lengths,
    ln1_gain,
    ln1_bias,
    w_qkv,
    q_bias,
    v_bias,
    w_out,
    b_out,
    ln2_gain,
    ln2_bias,
    w_fc1,
    b_fc1,
    w_fc2,
    b_fc2,
    cotangent,
):
    clips, rows, width = tokens.shape
    total_rows, clip_rows, local = clips * rows, rows * ring, width // ring
    own, half, cut = ln1_gain.shape[0], clips // 2, devices // 4
    me, core = lax.axis_index("seq"), lax.axis_index("fsdp") % 2
    same_core = [list(range(p, devices, 2)) for p in range(2)]

    def over(value, r):
        return swap(value, ring, r)

    vectors = jnp.concatenate(
        [
            jnp.stack([ln1_gain, ln1_bias, q_bias, v_bias, b_out, ln2_gain, ln2_bias, b_fc2]),
            b_fc1.reshape(-1, own),
        ]
    )
    count = vectors.shape[0]
    mine = lax.dynamic_index_in_dim(w_qkv.reshape(own, 3, ring, local), me, 2, keepdims=False)
    mine = jnp.concatenate([mine.reshape(own, 3 * local), columns(vectors)], axis=1)
    mine = lax.all_gather(mine, "fsdp", axis=0, tiled=True)
    part1 = lax.dynamic_index_in_dim(w_fc1.reshape(own, devices, ring, own), me, 2)
    part2 = lax.dynamic_index_in_dim(w_fc2.reshape(ring, own, width), me, 0)
    quarter = jnp.concatenate([part1.reshape(1, own, width), part2], axis=0)
    quarter = lax.all_gather(quarter, "fsdp", axis=0, axis_index_groups=same_core)
    wo = lax.all_gather(w_out, "fsdp", axis=0, tiled=True)

    middle_row = rows // 16 * 8
    one, two = stage(over(tokens[0], 1), over(tokens[0], 2))
    far = [over(two[:middle_row], 1), over(one[middle_row:], 2)]
    mine, *far = stage(mine, *far)
    vectors = as_rows(mine[:, 3 * local :], count)
    g1, b1, qb, vb, bo, g2, b2, c2 = (vectors[i] for i in range(8))
    c1_rows = vectors[8:]
    qb_mine = lax.dynamic_slice_in_dim(qb, me * local, local)
    vb_mine = lax.dynamic_slice_in_dim(vb, me * local, local)
    bias_mine = jnp.concatenate([qb_mine, jnp.zeros_like(qb_mine), vb_mine])

    norms, normed, qkv, outs, logs = ([None] * clips for _ in range(5))

    def project(c, groups):
        norms[c], normed[c], qkv[c] = norm_project(me, groups, g1, b1, mine, bias_mine)

    def to_rows(out):
        return lax.all_to_all(
            out.reshape(ring, rows, local), "seq", split_axis=0, concat_axis=0, tiled=True
        )

    def length(c):
        return lax.dynamic_slice_in_dim(lengths, c, 1)

    project(0, [[(tokens, 0)], [one], [two], far])
    outs[0], logs[0] = attend(qkv[0], length(0))
    others = [over(tokens[1:], r) for r in range(1, ring)]
    outs[0], *others = stage(outs[0], *others)
    moved = []
    for c in range(1, clips):
        moved.append(to_rows(outs[c - 1]))
        project(c, [[(tokens, c)]] + [[(t, c - 1)] for t in others])
        if c == 1:
            qkv[c], quarter, moved[0] = stage(qkv[c], quarter, moved[0])
            near = [over(quarter, 1), over(quarter, 2)]
        outs[c], logs[c] = attend(qkv[c], length(c))
        if c == 1:
            outs[c], *near = stage(outs[c], *near)
    moved.append(to_rows(outs[-1]))
    moved, near = lax.optimization_barrier((moved, near))
    far = [over(near[1][:cut], 1), over(near[0][cut:], 2)]
    twins = [twin(quarter, devices)] + [twin(n, devices) for n in near]
    attended, middle, h2, h2t = project_norm(moved, tokens, wo, bo, g2, b2)
    dy = cotangent.reshape(total_rows, width)

    sums = [None] * ring

    def quarter_of(r, mine_r, twin_r, acc):
        shift = lax.dynamic_index_in_dim(c1_rows, me ^ r, 0)
        y, dh2, keep, send, sums[r] = mlp_piece(
            core[None], h2, h2t, dy, mine_r, twin_r, shift, acc
        )
        return (y, dh2), keep, send

    acc, keep0, send0 = quarter_of(0, [quarter], twins[:1], None)
    *acc, keep0, send0, far0, far1 = stage(*acc, keep0, send0, *far)
    far = [far0, far1]
    got0, twin_far = twin(send0, devices), [twin(f, devices) for f in far]
    acc, keep1, send1 = quarter_of(1, near[:1], twins[1:2], acc)
    *acc, keep1, send1, got0, twin1, twin2 = stage(*acc, keep1, send1, got0, *twin_far)
    got1 = twin(send1, devices)
    acc, keep3, send3 = quarter_of(3, far, [twin1, twin2], acc)
    *acc, keep3, send3, got1 = stage(*acc, keep3, send3, got1)
    (got3,) = stage(twin(send3, devices))
    term3 = plus(keep3, got3)
    ends = [over(term3[:cut], 1), over(term3[cut:], 2)]
    acc, keep2, send2 = quarter_of(2, near[1:], twins[2:], acc)
    *acc, keep2, send2, end2, end1 = stage(*acc, keep2, send2, *ends)
    y, dh2 = acc
    term1 = [plus(keep1[:cut], got1[:cut])]
    term1.append(plus(plus(keep1[cut:], got1[cut:]), end1))
    got2 = twin(send2, devices)
    term2 = [plus(plus(keep2[:cut], got2[:cut]), end2), plus(keep2[cut:], got2[cut:])]
    term2, term1 = stage(term2, term1)
    first = [over(term1[0], 1), over(term2[1], 2)]

    c1_sum = placed([v[0] for v in sums], me)
    def to_heads(part):
        part = lax.all_to_all(part, "seq", split_axis=0, concat_axis=0, tiled=True)
        return part.reshape(1, clip_rows, local)

    layer_out = grad_middle = None
    das, heads, column_sums = ([None] * clips for _ in range(3))
    for c in range(clips):
        layer_out, grad_middle, das[c], heads[c], column_sums[c] = project_back(
            c, y, dh2, middle, dy, wo, g2, c2, tokens.shape, ring, layer_out, grad_middle
        )
        if c == 0:
            moved = to_heads(heads[0])
    term_wo = project_weight(das, attended, column_sums, c1_sum)
    moved, term_wo, first1, first2 = stage(moved, term_wo, *first)
    owned_wo = to_owners(term_wo)

    second = [over(term1[1], 1), over(term2[0], 2)]
    last_sums, flying, token_terms, ds = None, [], [None] * clips, []

    def exchange(parts):
        return lax.all_to_all(parts, "seq", 0, 0, tiled=True)

    def to_all(part):
        return exchange(jnp.broadcast_to(part[None], (ring,) + part.shape))

    for c in range(clips):
        later = [to_heads(heads[c + 1])] if c + 1 < clips else []
        if c == clips - 1:
            owned_wo = owned_wo.reshape(ring, own // ring, width + 128)
            later = [lax.dynamic_index_in_dim(owned_wo, me ^ r, 0, False) for r in range(ring)]
            later = [over(t, r) if r else t for r, t in enumerate(later)]
        d = attend_back(qkv[c], moved, outs[c], logs[c], length(c))
        d, later, flying, second = lax.optimization_barrier((d, later, flying, second))
        moved, wo_terms = later[0], later
        if c:
            token_terms[c - 1] = flying[0]
        else:
            total = plus(keep0, got0).astype(F32)
            total = total + jnp.concatenate([first1, second[0]], axis=0).astype(F32)
            total = total + jnp.concatenate([second[1], first2], axis=0).astype(F32)
            owned_mlp = lax.psum_scatter(
                total.astype(BF16),
                "fsdp",
                scatter_dimension=0,
                tiled=True,
                axis_index_groups=same_core,
            )[0]
            second = []
        last = c == clips - 1
        parts, last_sums = qkv_back(me, d[0], mine, norms[c], last_sums, ring)
        flying = [exchange(parts)]
        ds.append(d[0])
    grad_mine = qkv_weight(ds, normed, last_sums, ring)
    owned = to_owners(grad_mine)
    wo_term = sum(t.astype(F32) for t in wo_terms).astype(BF16)
    wo_parts = [over(wo_term, r) if r else wo_term for r in range(ring)]

    grad_inputs = None
    for c in range(clips - 1):
        grad_inputs = tokens_back(c, token_terms[c], tokens, grad_middle, g1, grad_inputs)
    grad_inputs, flying, wo_parts, owned_mlp = lax.optimization_barrier(
        (grad_inputs, flying, wo_parts, owned_mlp)
    )
    shared = to_all(owned_mlp)
    grad_inputs = tokens_back(clips - 1, flying[0], tokens, grad_middle, g1, grad_inputs)
    grad_w1, grad_w2 = spread_mlp(shared)
    grad_wo, grad_qkv, sums = spread_attn(me, wo_parts, to_all(owned))
    middle_sums, last_sums = sums[0], sums[1]
    return (
        layer_out,
        grad_inputs,
        last_sums[0],
        last_sums[1],
        grad_qkv,
        last_sums[2],
        last_sums[3],
        grad_wo,
        middle_sums[3],
        middle_sums[0],
        middle_sums[1],
        grad_w1,
        middle_sums[4 : count - 4].reshape(-1),
        grad_w2,
        middle_sums[2],
    )


def solution(mesh):
    act, vec, mat = P("fsdp", "seq", None), P("fsdp"), P("fsdp", None)
    in_specs = (act, vec, vec, vec, mat, vec, vec, mat, vec, vec, vec, mat, vec, mat, vec, act)
    out_specs = (act, act, vec, vec, mat, vec, vec, mat, vec, vec, vec, mat, vec, mat, vec)
    ring, devices = mesh.shape["seq"], mesh.shape["fsdp"]

    def layer(*args):
        clips, rows, width = args[0].shape
        square = ring == 4 and args[11].shape[1] == ring * width and devices % 4 == 0
        square = square and clips % (2 * devices) == 0 and width % (128 * devices) == 0
        return jax.shard_map(
            functools.partial(shards if square else shards_any, ring, devices),
            mesh=mesh,
            in_specs=in_specs,
            out_specs=out_specs,
            check_vma=False,
        )(*args)

    return layer
```

```python
import functools

import jax
import jax.numpy as jnp
from jax import lax
from jax.experimental import pallas as pl
from jax.experimental.pallas import tpu as pltpu
from jax.sharding import PartitionSpec as P

HEAD_DIM = 64
PAIR = 2 * HEAD_DIM
EPSILON = 1e-06
NEGATIVE = -1e30
F32, BF16 = jnp.float32, jnp.bfloat16
SCALE = HEAD_DIM ** -0.5
SCALE2 = SCALE * 1.4426950408889634
NT = (((1,), (1,)), ((), ()))
NN = (((1,), (0,)), ((), ()))
TN = (((0,), (0,)), ((), ()))


def dot(a, b, dims=NN):
    return lax.dot_general(a, b, dims, preferred_element_type=F32)


LARGE = 56 << 20
WHOLE = pl.BlockSpec(memory_space=pltpu.VMEM)
SCALAR = pl.BlockSpec(memory_space=pltpu.SMEM)


def kernel_call(body, name, operands, outs, scratch=(), scalars=0, aliases=None, vmem=40):
    return pl.pallas_call(
        body,
        in_specs=[SCALAR] * scalars + [WHOLE] * (len(operands) - scalars),
        out_specs=[WHOLE] * len(outs),
        out_shape=[jax.ShapeDtypeStruct(*out) for out in outs],
        scratch_shapes=list(scratch),
        input_output_aliases=aliases or {},
        compiler_params=pltpu.CompilerParams(vmem_limit_bytes=vmem << 20),
        cost_estimate=pl.CostEstimate(flops=1 << 20, bytes_accessed=1 << 20, transcendentals=0),
        name=name,
    )(*operands)


def of_head(block, h):
    lane = lax.broadcasted_iota(jnp.int32, (1, PAIR), 1)
    return jnp.where(lane // HEAD_DIM == h, block, jnp.zeros_like(block))


def valid_rows(j, bk, length):
    return j * bk + lax.broadcasted_iota(jnp.int32, (bk, 1), 0) < length


def transposed_chunks(out_ref, in_ref, cols, bk):
    for j in range(in_ref.shape[1] // bk):
        out_ref[j] = jnp.transpose(in_ref[0, pl.ds(j * bk, bk), cols])


def attend_kernel(len_ref, q_ref, k_ref, v_ref, o_ref, lse_ref, s_ref, vt_ref, ot_ref, *, bk):
    length = len_ref[pl.program_id(0)]
    rows_all, width = q_ref.shape[1:]
    chunks = pl.cdiv(length, bk)
    for pair in range(width // PAIR):
        cols = pl.ds(PAIR * pair, PAIR)
        transposed_chunks(vt_ref, v_ref, cols, bk)
        queries = [of_head(q_ref[0, :, cols], h) for h in range(2)]

        def score(j, tops):
            keys = k_ref[0, pl.ds(pl.multiple_of(j * bk, bk), bk), cols]
            ok = valid_rows(j, bk, length)
            out = []
            for h in range(2):
                s = jnp.where(ok, dot(keys, queries[h], NT), NEGATIVE)
                s_ref[h, j] = s
                top = tops[h]
                for i in range(bk // 8):
                    top = jnp.maximum(top, s[8 * i : 8 * i + 8])
                out.append(top)
            return tuple(out)

        low = jnp.full((8, rows_all), NEGATIVE, F32)
        tops = lax.fori_loop(0, chunks, score, (low, low))
        peaks = [jnp.max(top, axis=0, keepdims=True) * SCALE2 for top in tops]
        ot_ref[...] = jnp.zeros_like(ot_ref)

        def mix(j, sums):
            out = []
            for h in range(2):
                p = jnp.exp2(s_ref[h, j] * SCALE2 - peaks[h])
                total = sums[h]
                for i in range(bk // 8):
                    total = total + p[8 * i : 8 * i + 8]
                out.append(total)
                half = pl.ds(HEAD_DIM * h, HEAD_DIM)
                ot_ref[half] += dot(vt_ref[j, half], p.astype(BF16))
            return tuple(out)

        zero = jnp.zeros((8, rows_all), F32)
        sums = lax.fori_loop(0, chunks, mix, (zero, zero))
        for h in range(2):
            total = jnp.sum(sums[h], axis=0, keepdims=True)
            half = pl.ds(HEAD_DIM * h, HEAD_DIM)
            lse_ref[0, pl.ds(2 * pair + h, 1)] = peaks[h] + jnp.log2(total)
            ot_ref[half] = ot_ref[half] / total
        o_ref[0, :, cols] = jnp.transpose(ot_ref[...]).astype(BF16)


def attend_back_kernel(
    len_ref, q_ref, k_ref, v_ref, do_ref, o_ref, lse_ref, d_ref, kt_ref, dqt_ref, *, bk
):
    length = len_ref[pl.program_id(0)]
    width = q_ref.shape[2]
    chunks = pl.cdiv(length, bk)
    d_ref[...] = jnp.zeros_like(d_ref)
    for pair in range(width // PAIR):
        cols = pl.ds(PAIR * pair, PAIR)
        outs = do_ref[0, :, cols]
        both = jnp.transpose(outs.astype(F32) * o_ref[0, :, cols].astype(F32))
        inner = [
            jnp.sum(both[HEAD_DIM * h : HEAD_DIM * (h + 1)], axis=0, keepdims=True)
            for h in range(2)
        ]
        queries = [of_head(q_ref[0, :, cols], h) for h in range(2)]
        grads = [of_head(outs, h) for h in range(2)]
        logs = [lse_ref[0, pl.ds(2 * pair + h, 1)] for h in range(2)]
        transposed_chunks(kt_ref, k_ref, cols, bk)
        dqt_ref[...] = jnp.zeros_like(dqt_ref)

        def step(j, carry):
            rows = pl.ds(pl.multiple_of(j * bk, bk), bk)
            keys = k_ref[0, rows, cols]
            values = v_ref[0, rows, cols]
            ok = valid_rows(j, bk, length)
            dk = jnp.zeros((bk, PAIR), F32)
            dv = jnp.zeros((bk, PAIR), F32)
            for h in range(2):
                p = jnp.exp2(dot(keys, queries[h], NT) * SCALE2 - logs[h])
                p = jnp.where(ok, p, 0.0)
                g = (p * (dot(values, grads[h], NT) - inner[h])).astype(BF16)
                dv = dv + dot(p.astype(BF16), grads[h])
                dk = dk + dot(g, queries[h])
                half = pl.ds(HEAD_DIM * h, HEAD_DIM)
                dqt_ref[half] += dot(kt_ref[j, half], g)
            d_ref[0, rows, pl.ds(width + PAIR * pair, PAIR)] = (dk * SCALE).astype(BF16)
            d_ref[0, rows, pl.ds(2 * width + PAIR * pair, PAIR)] = dv.astype(BF16)
            return carry

        lax.fori_loop(0, chunks, step, 0)
        d_ref[0, :, cols] = jnp.transpose(dqt_ref[...] * SCALE).astype(BF16)


def chunk_rows(rows):
    return max(b for b in range(8, 225, 8) if rows % b == 0)


def block(rows, width, at):
    return pl.BlockSpec((1, rows, width), lambda c, n: (c, 0, at))


def attend(qkv, lengths):
    clips, rows, triple = qkv.shape
    width = triple // 3
    heads, bk = width // HEAD_DIM, chunk_rows(rows)
    cost = clips * heads * rows * rows
    return pl.pallas_call(
        functools.partial(attend_kernel, bk=bk),
        grid_spec=pltpu.PrefetchScalarGridSpec(
            num_scalar_prefetch=1,
            grid=(clips,),
            in_specs=[block(rows, width, i) for i in range(3)],
            out_specs=[block(rows, width, 0), block(heads, rows, 0)],
            scratch_shapes=[
                pltpu.VMEM((2, rows // bk, bk, rows), F32),
                pltpu.VMEM((rows // bk, PAIR, bk), BF16),
                pltpu.VMEM((PAIR, rows), F32),
            ],
        ),
        out_shape=[
            jax.ShapeDtypeStruct((clips, rows, width), BF16),
            jax.ShapeDtypeStruct((clips, heads, rows), F32),
        ],
        compiler_params=pltpu.CompilerParams(vmem_limit_bytes=LARGE),
        cost_estimate=pl.CostEstimate(
            flops=1 << 20, bytes_accessed=1 << 20, transcendentals=0
        ),
        name="attend",
    )(lengths, qkv, qkv, qkv)


def attend_back(qkv, grads, outs, logs, lengths):
    clips, rows, triple = qkv.shape
    width = triple // 3
    heads, bk = width // HEAD_DIM, chunk_rows(rows)
    cost = clips * heads * rows * rows
    return pl.pallas_call(
        functools.partial(attend_back_kernel, bk=bk),
        grid_spec=pltpu.PrefetchScalarGridSpec(
            num_scalar_prefetch=1,
            grid=(clips,),
            in_specs=[block(rows, width, i) for i in (0, 1, 2, 0, 0)] + [block(heads, rows, 0)],
            out_specs=block(rows, triple, 0),
            scratch_shapes=[
                pltpu.VMEM((rows // bk, PAIR, bk), BF16),
                pltpu.VMEM((PAIR, rows), F32),
            ],
        ),
        out_shape=jax.ShapeDtypeStruct((clips, rows, triple), BF16),
        compiler_params=pltpu.CompilerParams(vmem_limit_bytes=LARGE),
        cost_estimate=pl.CostEstimate(
            flops=1 << 20, bytes_accessed=1 << 20, transcendentals=0
        ),
        name="attend_back",
    )(lengths, qkv, qkv, qkv, grads, outs, logs)


def norm_kernel(me_ref, *refs, counts):
    parts, rest = refs[: sum(counts)], refs[sum(counts) :]
    g_ref, b_ref, w_ref, bias_ref, h_ref, qkv_ref, x_ref = rest
    taken = 0
    for r, count in enumerate(counts):
        group = parts[taken : taken + count]
        taken += count

        @pl.when(pl.program_id(0) == r)
        def _():
            row = 0
            for ref in group:
                x_ref[pl.ds(row, ref.shape[0])] = ref[...]
                row += ref.shape[0]

    normed, _ = normalize(x_ref[...].astype(F32))
    h = (normed * g_ref[...] + b_ref[...]).astype(BF16)
    h_ref[0] = h
    qkv_ref[0] = (dot(h, w_ref[...]) + bias_ref[...]).astype(BF16)


def norm_project(me, groups, gain, shift, weight, bias):
    flat = [part if isinstance(part, tuple) else (part, None) for g in groups for part in g]
    triple, ring = bias.shape[-1], len(groups)
    rows, width = flat[0][0].shape[-2:]

    def part_spec(array, clip):
        if clip is None:
            return pl.BlockSpec(array.shape, lambda r, m: (0, 0))
        return pl.BlockSpec((None, rows, width), lambda r, m: (clip, 0, 0))

    def out(cols):
        return pl.BlockSpec((1, rows, cols), lambda r, m: (m[0] ^ r, 0, 0))

    h, qkv = pl.pallas_call(
        functools.partial(norm_kernel, counts=[len(g) for g in groups]),
        grid_spec=pltpu.PrefetchScalarGridSpec(
            num_scalar_prefetch=1,
            grid=(ring,),
            in_specs=[part_spec(*part) for part in flat]
            + [WHOLE] * 2
            + [pl.BlockSpec((width, triple), lambda r, m: (0, 0)), WHOLE],
            out_specs=[out(width), out(triple)],
            scratch_shapes=[pltpu.VMEM((rows, width), BF16)],
        ),
        out_shape=[jax.ShapeDtypeStruct((ring, rows, c), BF16) for c in (width, triple)],
        compiler_params=pltpu.CompilerParams(vmem_limit_bytes=LARGE),
        cost_estimate=pl.CostEstimate(flops=1 << 20, bytes_accessed=1 << 20, transcendentals=0),
        name="norm_project",
    )(me[None], *[part[0] for part in flat], gain[None], shift[None], weight, bias[None])
    return h.reshape(ring * rows, width), qkv.reshape(1, ring * rows, triple)


def mlp_piece_kernel(core_ref, h_ref, ht_ref, dy_ref, *refs, first, nz, counts):
    mines, others, refs = refs[: counts[0]], refs[counts[0] : sum(counts)], refs[sum(counts) :]
    c1_ref, *refs = refs
    yin_ref, dhin_ref = (None, None) if first else (refs.pop(0), refs.pop(0))
    y_ref, dh_ref, keep_ref, send_ref, sums_ref, hm_ref, hmt_ref, w1_ref, w2_ref, u_ref, dz_ref = refs
    core = core_ref[0]
    width = h_ref.shape[1]
    clips, _, share = ht_ref.shape
    rows = mines[0].shape[2]
    half = nz * rows

    def at(i, p):
        block = 2 * i + (core if p == 0 else 1 - core)
        return pl.ds(pl.multiple_of(block * rows, rows), rows)

    def put(i, p):
        return pl.ds(p * half + i * rows, rows)

    def source(i, p):
        parts = (mines, others)[p]
        size = nz // len(parts)
        return parts[i // size], i % size

    for i in range(nz):
        for p in range(2):
            hm_ref[:, put(i, p)] = h_ref[:, at(i, p)]
            for c in range(clips):
                hmt_ref[c, put(i, p), :] = ht_ref[c, at(i, p), :]
            src, z = source(i, p)
            w2_ref[pl.ds((2 * i + p) * rows, rows), :] = src[z, 1]
            for j in range(nz):
                for r in range(2):
                    w1_ref[put(i, p), pl.ds((2 * j + r) * rows, rows)] = src[z, 0, :, at(j, r)]
    for i in range(nz):
        cols = pl.ds(2 * i * rows, 2 * rows)
        bias = jnp.concatenate([c1_ref[:, at(i, p)] for p in range(2)], axis=1)
        z = dot(hm_ref[...], w1_ref[:, cols]) + bias
        phi = 0.5 * (1.0 + lax.erf(z * (2.0 ** -0.5)))
        u_ref[:, cols] = (z * phi).astype(BF16)
        slope = phi + z * (jnp.exp(z * z * -0.5) * 0.3989422804014327)
        dz = (dot(dy_ref[...], w2_ref[cols, :], NT) * slope).astype(BF16)
        dz_ref[:, cols] = dz
        total = jnp.sum(dz.astype(F32), axis=0, keepdims=True)
        for p in range(2):
            sums_ref[:, at(i, p)] = total[:, p * rows : (p + 1) * rows]
        g2 = dot(u_ref[:, cols], dy_ref[...], TN).astype(BF16)
        keep_ref[i, 1] = g2[:rows]
        send_ref[i, 1] = g2[rows:]
        g1 = sum(dot(hmt_ref[c], dz_ref[pl.ds(c * share, share), cols]) for c in range(clips))
        g1 = g1.astype(BF16)
        for p in range(2):
            part = g1[:, p * rows : (p + 1) * rows]
            keep_ref[:, 0, :, at(i, p)] = part[:half].reshape(nz, rows, rows)
            send_ref[:, 0, :, at(i, p)] = part[half:].reshape(nz, rows, rows)
    for n in range(width // 256):
        cols = pl.ds(256 * n, 256)
        y = dot(u_ref[...], w2_ref[:, cols])
        y_ref[:, cols] = y if first else y + yin_ref[:, cols]
    for n in range(width // 256):
        d = dot(dz_ref[...], w1_ref[pl.ds(256 * n, 256), :], NT)
        for q in range(256 // rows):
            p, i = divmod((256 // rows) * n + q, nz)
            v = d[:, q * rows : (q + 1) * rows]
            dh_ref[:, at(i, p)] = v if first else v + dhin_ref[:, at(i, p)]


def mlp_piece(core, h2, h2t, dy, mine, other, c1, acc):
    rows = mine[0].shape[2]
    t, width = h2.shape
    nz = width // (2 * rows)
    first = acc is None
    ins = [core, h2, h2t, dy, *mine, *other, c1] + ([] if first else list(acc))
    gradient = ((nz, 2, rows, width), BF16)
    return kernel_call(
        functools.partial(
            mlp_piece_kernel, first=first, nz=nz, counts=(len(mine), len(other))
        ),
        "mlp_piece",
        ins,
        [((t, width), F32), ((t, width), F32), gradient, gradient, (c1.shape, F32)],
        scratch=[pltpu.VMEM((t, width), BF16), pltpu.VMEM(h2t.shape, BF16)]
        + [pltpu.VMEM((width, width), BF16)] * 2
        + [pltpu.VMEM((t, width), BF16)] * 2,
        scalars=1,
        aliases={} if first else {len(ins) - 2: 0, len(ins) - 1: 1},
        vmem=24,
    )


def project_kernel(*refs, clips):
    moved, rest = refs[:clips], refs[clips:]
    x_ref, wo_ref, bo_ref, g_ref, b_ref, att_ref, mid_ref, h_ref, ht_ref = rest
    ring, rows, local = moved[0].shape
    for c in range(clips):
        at = pl.ds(c * rows, rows)
        for s in range(ring):
            att_ref[at, pl.ds(s * local, local)] = moved[c][s]
        middle = x_ref[c].astype(F32) + (dot(att_ref[at, :], wo_ref[...]) + bo_ref[...])
        mid_ref[at, :] = middle
        h = (normalize(middle)[0] * g_ref[...] + b_ref[...]).astype(BF16)
        h_ref[at, :] = h
        ht_ref[c] = jnp.transpose(h)


def project_norm(moved, tokens, wo, bo, gain, shift):
    clips, rows, width = tokens.shape
    flat = (clips * rows, width)
    return kernel_call(
        functools.partial(project_kernel, clips=clips),
        "project_norm",
        [*moved, tokens, wo, bo[None], gain[None], shift[None]],
        [(flat, BF16), (flat, F32), (flat, BF16), ((clips, width, rows), BF16)],
    )


def project_back_kernel(*refs, clip, first):
    y_ref, dh_ref, mid_ref, dy_ref, wo_ref, g_ref, c2_ref = refs[:7]
    out_ref, gm_ref, da_ref, do_ref, sum_ref = refs[-5:]
    ring, rows, local = do_ref.shape
    middle = mid_ref[...]
    out_ref[0] = (middle + (y_ref[...] + c2_ref[...])).astype(BF16)
    normed, rstd = normalize(middle)
    dh = dh_ref[...]
    dy = dy_ref[...].astype(F32)
    grad = dy + normalize_back(dh, normed, rstd, g_ref[...])
    gm_ref[0] = grad
    da = grad.astype(BF16)
    da_ref[...] = da
    do = dot(da, wo_ref[...], NT).astype(BF16)
    for s in range(ring):
        do_ref[s] = do[:, s * local : (s + 1) * local]
    sum_ref[...] = jnp.zeros_like(sum_ref)
    for i, terms in enumerate((dh * normed, dh, dy, da.astype(F32))):
        sum_ref[pl.ds(i, 1), :] = jnp.sum(terms, axis=0, keepdims=True)


def project_back(c, y, dh, middle, dy, wo, gain, c2, shape, ring, out, grad):
    clips, rows, width = shape
    at = pl.BlockSpec((rows, width), lambda i: (c, 0))
    at_c = pl.BlockSpec((1, rows, width), lambda i: (c, 0, 0))
    one = pl.BlockSpec((1, width), lambda i: (0, 0))
    back = [] if out is None else [out, grad]
    return pl.pallas_call(
        functools.partial(project_back_kernel, clip=c, first=out is None),
        grid=(1,),
        in_specs=[at] * 4
        + [pl.BlockSpec((width, width), lambda i: (0, 0)), one, one]
        + [pl.BlockSpec(memory_space=pl.ANY)] * len(back),
        out_specs=[
            at_c,
            at_c,
            pl.BlockSpec((rows, width), lambda i: (0, 0)),
            pl.BlockSpec((ring, rows, width // ring), lambda i: (0, 0, 0)),
            pl.BlockSpec((8, width), lambda i: (0, 0)),
        ],
        out_shape=[
            jax.ShapeDtypeStruct(shape, BF16),
            jax.ShapeDtypeStruct(shape, F32),
            jax.ShapeDtypeStruct((rows, width), BF16),
            jax.ShapeDtypeStruct((ring, rows, width // ring), BF16),
            jax.ShapeDtypeStruct((8, width), F32),
        ],
        input_output_aliases={7: 0, 8: 1} if back else {},
        compiler_params=pltpu.CompilerParams(vmem_limit_bytes=LARGE),
        cost_estimate=pl.CostEstimate(flops=1 << 20, bytes_accessed=1 << 20, transcendentals=0),
        name="project_back",
    )(y, dh, middle, dy, wo, gain[None], c2[None], *back)


def project_weight_kernel(*refs, clips):
    das, att_ref, sums = refs[:clips], refs[clips], refs[clips + 1 : 2 * clips + 1]
    c1_ref, gw_ref, sum_ref = refs[2 * clips + 1 :]
    rows, width = das[0].shape
    term = dot(att_ref[pl.ds(0, rows), :], das[0][...], TN)
    total = sums[0][...]
    for c in range(1, clips):
        term = term + dot(att_ref[pl.ds(c * rows, rows), :], das[c][...], TN)
        total = total + sums[c][...]
    sum_ref[...] = jnp.zeros_like(sum_ref)
    sum_ref[pl.ds(0, 8), :] = total
    sum_ref[pl.ds(4, c1_ref.shape[0]), :] = c1_ref[...]
    gw_ref[:, pl.ds(0, width)] = term.astype(BF16)
    gw_ref[:, pl.ds(width, 128)] = jnp.transpose(sum_ref[...]).astype(BF16)


def project_weight(das, attended, sums, c1_sum):
    width = attended.shape[1]
    return kernel_call(
        functools.partial(project_weight_kernel, clips=len(das)),
        "project_weight",
        [*das, attended, *sums, c1_sum],
        [((width, width + 128), BF16)],
        scratch=[pltpu.VMEM((128, width), F32)],
        vmem=56,
    )[0]


def qkv_back_kernel(d_ref, w_ref, part_ref):
    part_ref[0] = dot(d_ref[...], w_ref[...], NT).astype(BF16)


def qkv_back(d, weight, ring):
    whole, triple = d.shape
    width, rows = weight.shape[0], whole // ring
    return pl.pallas_call(
        qkv_back_kernel,
        grid=(ring,),
        in_specs=[
            pl.BlockSpec((rows, triple), lambda r: (r, 0)),
            pl.BlockSpec((width, triple), lambda r: (0, 0)),
        ],
        out_specs=pl.BlockSpec((1, rows, width), lambda r: (r, 0, 0)),
        out_shape=jax.ShapeDtypeStruct((ring, rows, width), BF16),
        compiler_params=pltpu.CompilerParams(vmem_limit_bytes=LARGE),
        cost_estimate=pl.CostEstimate(flops=1 << 20, bytes_accessed=1 << 20, transcendentals=0),
        name="qkv_back",
    )(d, weight)


def qkv_weight_kernel(me_ref, d_ref, h_ref, w_ref, *rest, first, last):
    rest = list(rest)
    acc_ref, bias_ref = (None, None) if first else (rest.pop(0), rest.pop(0))
    triple = d_ref.shape[1]
    local = triple // 3
    term = dot(h_ref[...], d_ref[...], TN)
    bias = jnp.sum(d_ref[...].astype(F32), axis=0, keepdims=True)
    if not first:
        term = term + acc_ref[...]
        bias = bias + bias_ref[pl.ds(0, 1), :]
    if not last:
        out_ref, sum_ref = rest
        out_ref[...] = term
        sum_ref[...] = jnp.broadcast_to(bias, sum_ref.shape)
        return
    out_ref, part_ref, row_ref = rest
    ring, rows, _ = part_ref.shape
    for r in range(ring):
        at = pl.ds(r * rows, rows)
        part_ref[r] = dot(d_ref[at, :], w_ref[:, pl.ds(0, triple)], NT).astype(BF16)
    out_ref[:, pl.ds(0, triple)] = term.astype(BF16)
    weight = w_ref[:, pl.ds(0, triple)].astype(F32)
    vectors = w_ref[:, pl.ds(triple, 128)].astype(F32)
    gain, shift = vectors[:, 0:1], vectors[:, 1:2]
    shift_sum = jnp.sum(weight * bias, axis=1, keepdims=True)
    gain_sum = (jnp.sum(weight * term, axis=1, keepdims=True) - shift * shift_sum) / gain
    row_ref[...] = jnp.zeros_like(row_ref)
    at_me = pl.ds(pl.multiple_of(me_ref[0] * local, local), local)
    row_ref[pl.ds(2, 1), at_me] = bias[:, :local]
    row_ref[pl.ds(3, 1), at_me] = bias[:, 2 * local :]
    lane = lax.broadcasted_iota(jnp.int32, (1, 128), 1)
    sums = jnp.transpose(row_ref[...])
    sums = jnp.where(lane == 0, gain_sum, jnp.where(lane == 1, shift_sum, sums))
    out_ref[:, pl.ds(triple, 128)] = sums.astype(BF16)


def qkv_weight(me, d, h, mine, acc, ring, last):
    (whole, triple), width = d.shape, h.shape[1]
    outs = [((width, triple), F32), ((8, triple), F32)]
    if last:
        outs = [((width, triple + 128), BF16), ((ring, whole // ring, width), BF16)]
    return kernel_call(
        functools.partial(qkv_weight_kernel, first=acc is None, last=last),
        "qkv_weight",
        [me[None], d, h, mine] + list(acc or ()),
        outs,
        scratch=[pltpu.VMEM((128, width), F32)] if last else (),
        scalars=1,
        vmem=56,
    )


def tokens_back_kernel(*refs, ring):
    term_ref, x_ref, gm_ref, g_ref = refs[:4]
    out_ref = refs[-1]
    grad = term_ref[0].astype(F32)
    for r in range(1, ring):
        grad = grad + term_ref[r].astype(F32)
    normed, rstd = normalize(x_ref[0].astype(F32))
    out_ref[0] = gm_ref[0] + normalize_back(grad, normed, rstd, g_ref[...])


def tokens_back(c, terms, tokens, grad_middle, gain, out):
    clips, rows, width = tokens.shape
    steps = max(n for n in (7, 4, 2, 1) if rows % (8 * n) == 0)
    block = rows // steps
    at_c = pl.BlockSpec((1, block, width), lambda i: (c, i, 0))
    ring = terms.shape[0]
    specs = [pl.BlockSpec((ring, block, width), lambda i: (0, i, 0)), at_c, at_c]
    specs.append(pl.BlockSpec((1, width), lambda i: (0, 0)))
    operands = [terms, tokens, grad_middle, gain[None]]
    if out is not None:
        specs.append(pl.BlockSpec(memory_space=pl.ANY))
        operands.append(out)
    return pl.pallas_call(
        functools.partial(tokens_back_kernel, ring=ring),
        grid=(steps,),
        in_specs=specs,
        out_specs=at_c,
        out_shape=jax.ShapeDtypeStruct((clips, rows, width), F32),
        input_output_aliases={} if out is None else {len(operands) - 1: 0},
        compiler_params=pltpu.CompilerParams(vmem_limit_bytes=LARGE),
        cost_estimate=pl.CostEstimate(flops=1 << 20, bytes_accessed=1 << 20, transcendentals=0),
        name="tokens_back",
    )(*operands)


def spread_mlp_kernel(part_ref, w1_ref, w2_ref, *, ring):
    own = part_ref.shape[2]
    for q in range(ring):
        part = part_ref[q, 0].astype(F32)
        for f in range(part.shape[1] // own):
            w1_ref[:, pl.ds((f * ring + q) * own, own)] = part[:, f * own : (f + 1) * own]
        w2_ref[pl.ds(q * own, own), :] = part_ref[q, 1].astype(F32)


def spread_mlp(parts):
    ring, _, own, width = parts.shape
    return kernel_call(
        functools.partial(spread_mlp_kernel, ring=ring),
        "spread_mlp",
        [parts],
        [((own, ring * width), F32), ((ring * own, width), F32)],
    )


def spread_attn_kernel(me_ref, *refs, ring):
    wo_refs, qkv_refs = refs[:ring], refs[ring : 2 * ring]
    gwo_ref, gqkv_ref, vec_ref, more_ref = refs[2 * ring :]
    own, width = gwo_ref.shape
    rows = wo_refs[0].shape[0]
    triple = qkv_refs[0].shape[1] - 128
    local = triple // 3
    last = jnp.zeros((own, 128), F32)
    for r in range(ring):
        q = me_ref[0] ^ r
        at = pl.ds(pl.multiple_of(q * rows, rows), rows)
        gwo_ref[at, :] = wo_refs[r][:, :width].astype(F32)
        more_ref[at, :] = wo_refs[r][:, width:].astype(F32)
        last = last + qkv_refs[r][:, triple:].astype(F32)
        for i in range(3):
            part = qkv_refs[r][:, i * local : (i + 1) * local].astype(F32)
            gqkv_ref[:, pl.ds(pl.multiple_of(i * width + q * local, local), local)] = part
    vec_ref[0] = jnp.transpose(more_ref[...])
    vec_ref[1] = jnp.transpose(last)


def spread_attn(me, wo_parts, qkv_parts):
    ring, own = len(qkv_parts), qkv_parts[0].shape[0]
    width = wo_parts[0].shape[1] - 128
    return kernel_call(
        functools.partial(spread_attn_kernel, ring=ring),
        "spread_attn",
        [me[None], *wo_parts, *qkv_parts],
        [((own, width), F32), ((own, 3 * width), F32), ((2, 128, own), F32)],
        scratch=[pltpu.VMEM((own, 128), F32)],
        scalars=1,
    )


def swap(value, ring, r):
    return lax.ppermute(value, "seq", [(i, i ^ r) for i in range(ring)])


def gather_seq(value, ring, me):
    out = jnp.zeros((ring,) + value.shape, value.dtype)
    out = lax.dynamic_update_index_in_dim(out, value, me, 0)
    for r in range(1, ring):
        out = lax.dynamic_update_index_in_dim(out, swap(value, ring, r), me ^ r, 0)
    return out


def sum_seq(terms, ring, me):
    total = lax.dynamic_index_in_dim(terms, me, 0, keepdims=False).astype(F32)
    for r in range(1, ring):
        term = lax.dynamic_index_in_dim(terms, me ^ r, 0, keepdims=False)
        total = total + swap(term, ring, r).astype(F32)
    return total


def to_owners(grad):
    return lax.psum_scatter(grad, "fsdp", scatter_dimension=0, tiled=True)


def sum_owned(owned, ring, me):
    rows, width = owned.shape
    part = sum_seq(owned.reshape(ring, rows // ring, width), ring, me).astype(BF16)
    return gather_seq(part, ring, me).reshape(rows, width).astype(F32)


def sum_vectors(rows, devices, ring):
    count, width = rows.shape
    sent = rows.reshape(count, devices, width // devices).transpose(1, 0, 2)
    total = jnp.sum(lax.all_to_all(sent, "fsdp", split_axis=0, concat_axis=0, tiled=True), axis=0)
    return total + sum(swap(total, ring, r) for r in range(1, ring))


def normalize(values):
    centered = values - jnp.mean(values, axis=-1, keepdims=True)
    variance = jnp.mean(centered * centered, axis=-1, keepdims=True)
    rstd = lax.rsqrt(variance + EPSILON)
    return centered * rstd, rstd


def normalize_back(grad, normed, rstd, gain):
    e = grad * gain
    mean = jnp.mean(e, axis=-1, keepdims=True)
    along = jnp.mean(e * normed, axis=-1, keepdims=True)
    return rstd * (e - mean - normed * along)


def shards_any(
    ring,
    devices,
    tokens,
    lengths,
    ln1_gain,
    ln1_bias,
    w_qkv,
    q_bias,
    v_bias,
    w_out,
    b_out,
    ln2_gain,
    ln2_bias,
    w_fc1,
    b_fc1,
    w_fc2,
    b_fc2,
    cotangent,
):
    clips, rows, width = tokens.shape
    total_rows = clips * rows
    clip_rows = rows * ring
    local = width // ring
    me = lax.axis_index("seq")

    whole = [gather_seq(tokens[c], ring, me).reshape(clip_rows, width) for c in range(clips)]

    own = ln1_gain.shape[0]
    packed = jnp.concatenate(
        [
            jnp.stack([ln1_gain, ln1_bias, q_bias, v_bias, b_out, ln2_gain, ln2_bias, b_fc2]),
            b_fc1.reshape(-1, own),
        ]
    )
    vectors = lax.all_gather(packed, "fsdp", axis=0, tiled=False)
    c1 = vectors[:, 8:].reshape(-1).astype(F32)
    vectors = vectors[:, :8].transpose(1, 0, 2).reshape(8, width).astype(F32)
    g1, b1, qb, vb, bo, g2, b2, c2 = (vectors[i] for i in range(8))
    qb_mine = lax.dynamic_slice_in_dim(qb, me * local, local)
    vb_mine = lax.dynamic_slice_in_dim(vb, me * local, local)
    bias_mine = jnp.concatenate([qb_mine, jnp.zeros_like(qb_mine), vb_mine])

    mine = lax.dynamic_index_in_dim(w_qkv.reshape(own, 3, ring, local), me, 2, keepdims=False)
    wqkv = lax.all_gather(mine.reshape(own, 3 * local), "fsdp", axis=0, tiled=True)
    wo = lax.all_gather(w_out, "fsdp", axis=0, tiled=True)
    w1 = lax.all_gather(w_fc1, "fsdp", axis=0, tiled=True)
    w2 = lax.all_gather(w_fc2, "fsdp", axis=0, tiled=True)

    normed, qkv, heads_out, logs, attended = [], [], [], [], []
    for c in range(clips):
        n1 = normalize(whole[c].astype(F32))[0]
        h1 = (n1 * g1 + b1).astype(BF16)
        part = (dot(h1, wqkv) + bias_mine).astype(BF16)[None]
        out, log = attend(part, lax.dynamic_slice_in_dim(lengths, c, 1))
        moved = lax.all_to_all(
            out.reshape(ring, rows, local), "seq", split_axis=0, concat_axis=0, tiled=True
        )
        normed.append(h1)
        qkv.append(part)
        heads_out.append(out)
        logs.append(log)
        attended.append(moved.transpose(1, 0, 2).reshape(rows, width))
    attended = jnp.concatenate(attended, axis=0)

    inputs = tokens.astype(F32).reshape(total_rows, width)
    middle = inputs + (dot(attended, wo) + bo)
    n2, r2 = normalize(middle)
    h2 = (n2 * g2 + b2).astype(BF16)
    z = dot(h2, w1) + c1
    phi = 0.5 * (1.0 + lax.erf(z * (2.0 ** -0.5)))
    hidden = (z * phi).astype(BF16)
    slope = phi + z * (jnp.exp(-0.5 * z * z) * 0.3989422804014327)
    layer_out = (middle + (dot(hidden, w2) + c2)).astype(BF16).reshape(clips, rows, width)

    dy = cotangent.reshape(total_rows, width)
    dy_f = dy.astype(F32)
    term_w2 = dot(hidden, dy, TN).astype(BF16)
    dz = (dot(dy, w2, NT) * slope).astype(BF16)
    term_w1 = dot(h2, dz, TN).astype(BF16)
    dh2 = dot(dz, w1, NT)
    grad_middle = dy_f + normalize_back(dh2, n2, r2, g2)
    da = grad_middle.astype(BF16)
    term_wo = dot(attended, da, TN).astype(BF16)
    do = dot(da, wo, NT).astype(BF16)
    do, term_w2, term_w1, term_wo = lax.optimization_barrier((do, term_w2, term_w1, term_wo))
    owned_w2, owned_w1, owned_wo = (to_owners(t) for t in (term_w2, term_w1, term_wo))

    dqkv, own_terms, gain_sum, shift_sum = [], [], 0.0, 0.0
    for c in range(clips):
        sent = do[c * rows : (c + 1) * rows].reshape(rows, ring, local).transpose(1, 0, 2)
        moved = lax.all_to_all(sent, "seq", split_axis=0, concat_axis=0, tiled=True)
        moved = moved.reshape(1, clip_rows, local)
        d = attend_back(
            qkv[c], moved, heads_out[c], logs[c], lax.dynamic_slice_in_dim(lengths, c, 1)
        )[0]
        dh1 = dot(d, wqkv, NT)
        n1 = normalize(whole[c].astype(F32))[0]
        gain_sum = gain_sum + jnp.sum(dh1 * n1, axis=0)
        shift_sum = shift_sum + jnp.sum(dh1, axis=0)
        own_terms.append(sum_seq(dh1.astype(BF16).reshape(ring, rows, width), ring, me))
        dqkv.append(d)
    dqkv = jnp.concatenate(dqkv, axis=0)
    grad_mine = dot(jnp.concatenate(normed, axis=0), dqkv, TN).astype(BF16)
    grad_mine, owned_w2, owned_w1, owned_wo = lax.optimization_barrier(
        (grad_mine, owned_w2, owned_w1, owned_wo)
    )
    owned = to_owners(grad_mine)
    grad_w2, grad_w1, grad_wo = (sum_owned(o, ring, me) for o in (owned_w2, owned_w1, owned_wo))
    grad_qkv = gather_seq(owned, ring, me).astype(F32)
    grad_qkv = jnp.concatenate(
        [grad_qkv[r, :, i * local : (i + 1) * local] for i in range(3) for r in range(ring)], axis=1
    )

    bias_sum = jnp.sum(dqkv.astype(F32), axis=0)
    zeros = jnp.zeros((width,), F32)
    first = jnp.stack(
        [
            gain_sum,
            shift_sum,
            lax.dynamic_update_slice_in_dim(zeros, bias_sum[:local], me * local, 0),
            lax.dynamic_update_slice_in_dim(zeros, bias_sum[2 * local :], me * local, 0),
        ]
    )
    second = jnp.stack(
        [
            jnp.sum(dh2 * n2, axis=0),
            jnp.sum(dh2, axis=0),
            jnp.sum(dy_f, axis=0),
            jnp.sum(da.astype(F32), axis=0),
        ]
    )
    c1_sum = jnp.sum(dz.astype(F32), axis=0).reshape(devices, -1, own).transpose(1, 0, 2)
    second = jnp.concatenate([second, c1_sum.reshape(-1, width)])
    four = sum_vectors(second, devices, ring)
    grad_c1 = four[4:].reshape(-1)
    late = sum_vectors(first, devices, ring)

    terms = jnp.concatenate(own_terms, axis=0)
    n1, r1 = normalize(inputs)
    grad_inputs = (grad_middle + normalize_back(terms, n1, r1, g1)).reshape(clips, rows, width)
    return (
        layer_out,
        grad_inputs,
        late[0],
        late[1],
        grad_qkv,
        late[2],
        late[3],
        grad_wo,
        four[3],
        four[0],
        four[1],
        grad_w1,
        grad_c1,
        grad_w2,
        four[2],
    )


def twin(value, devices):
    return lax.ppermute(value, "fsdp", [(i, i ^ 1) for i in range(devices)])


def columns(vectors):
    vectors = jnp.pad(vectors.astype(BF16), ((0, -vectors.shape[0] % 128), (0, 0)))
    return dot(jnp.eye(vectors.shape[1], dtype=BF16), vectors, NT).astype(BF16)


def as_rows(block, count):
    return dot(block, jnp.eye(block.shape[0], dtype=BF16), TN)[:count]


def plus(a, b):
    return (a.astype(F32) + b.astype(F32)).astype(BF16)


def plus_rows(a, b, more, row):
    total = a.astype(F32) + b.astype(F32)
    pad = [(row, a.shape[0] - row - more.shape[0])] + [(0, 0)] * (a.ndim - 1)
    return (total + jnp.pad(more.astype(F32), pad)).astype(BF16)


def stage(*values):
    return lax.optimization_barrier(values)


def placed(parts, me):
    out = jnp.zeros((len(parts),) + parts[0].shape, parts[0].dtype)
    for r, part in enumerate(parts):
        out = lax.dynamic_update_index_in_dim(out, part, me ^ r, 0)
    return out


def shards(
    ring,
    devices,
    tokens,
    lengths,
    ln1_gain,
    ln1_bias,
    w_qkv,
    q_bias,
    v_bias,
    w_out,
    b_out,
    ln2_gain,
    ln2_bias,
    w_fc1,
    b_fc1,
    w_fc2,
    b_fc2,
    cotangent,
):
    clips, rows, width = tokens.shape
    total_rows, clip_rows, local = clips * rows, rows * ring, width // ring
    own, half, cut = ln1_gain.shape[0], clips // 2, devices // 4
    me, core = lax.axis_index("seq"), lax.axis_index("fsdp") % 2
    same_core = [list(range(p, devices, 2)) for p in range(2)]

    def over(value, r):
        return swap(value, ring, r)

    vectors = jnp.concatenate(
        [
            jnp.stack([ln1_gain, ln1_bias, q_bias, v_bias, b_out, ln2_gain, ln2_bias, b_fc2]),
            b_fc1.reshape(-1, own),
        ]
    )
    count = vectors.shape[0]
    mine = lax.dynamic_index_in_dim(w_qkv.reshape(own, 3, ring, local), me, 2, keepdims=False)
    mine = jnp.concatenate([mine.reshape(own, 3 * local), columns(vectors)], axis=1)
    mine = lax.all_gather(mine, "fsdp", axis=0, tiled=True)
    part1 = lax.dynamic_index_in_dim(w_fc1.reshape(own, devices, ring, own), me, 2)
    part2 = lax.dynamic_index_in_dim(w_fc2.reshape(ring, own, width), me, 0)
    quarter = jnp.concatenate([part1.reshape(1, own, width), part2], axis=0)
    quarter = lax.all_gather(quarter, "fsdp", axis=0, axis_index_groups=same_core)
    wo = lax.all_gather(w_out, "fsdp", axis=0, tiled=True)

    middle_row = rows // 16 * 8
    one, two = stage(over(tokens[0], 1), over(tokens[0], 2))
    far = [over(two[:middle_row], 1), over(one[middle_row:], 2)]
    mine, *far = stage(mine, *far)
    vectors = as_rows(mine[:, 3 * local :], count)
    g1, b1, qb, vb, bo, g2, b2, c2 = (vectors[i] for i in range(8))
    c1_rows = vectors[8:]
    qb_mine = lax.dynamic_slice_in_dim(qb, me * local, local)
    vb_mine = lax.dynamic_slice_in_dim(vb, me * local, local)
    bias_mine = jnp.concatenate([qb_mine, jnp.zeros_like(qb_mine), vb_mine])

    normed, qkv, outs, logs = ([None] * clips for _ in range(4))

    def project(c, groups):
        normed[c], qkv[c] = norm_project(me, groups, g1, b1, mine, bias_mine)

    def to_rows(out):
        return lax.all_to_all(
            out.reshape(ring, rows, local), "seq", split_axis=0, concat_axis=0, tiled=True
        )

    def length(c):
        return lax.dynamic_slice_in_dim(lengths, c, 1)

    project(0, [[(tokens, 0)], [one], [two], far])
    outs[0], logs[0] = attend(qkv[0], length(0))
    others = [over(tokens[1:], r) for r in range(1, ring)]
    outs[0], *others = stage(outs[0], *others)
    moved = []
    for c in range(1, clips):
        moved.append(to_rows(outs[c - 1]))
        project(c, [[(tokens, c)]] + [[(t, c - 1)] for t in others])
        if c == 1:
            qkv[c], quarter, moved[0] = stage(qkv[c], quarter, moved[0])
            ends_of = [quarter[:cut], quarter[cut:]]
            low1, top2 = over(ends_of[1], 1), over(ends_of[0], 2)
            twin0 = twin(quarter, devices)
        outs[c], logs[c] = attend(qkv[c], length(c))
        if c == 1:
            outs[c], low1, top2, twin0 = stage(outs[c], low1, top2, twin0)
    moved.append(to_rows(outs[-1]))
    moved, low1, top2, ends_of = lax.optimization_barrier((moved, low1, top2, ends_of))
    top1, low2 = over(ends_of[0], 1), over(ends_of[1], 2)
    attended, middle, h2, h2t = project_norm(moved, tokens, wo, bo, g2, b2)
    dy = cotangent.reshape(total_rows, width)

    sums = [None] * ring

    def quarter_of(r, mine_r, twin_r, acc):
        shift = lax.dynamic_index_in_dim(c1_rows, me ^ r, 0)
        y, dh2, keep, send, sums[r] = mlp_piece(
            core[None], h2, h2t, dy, mine_r, twin_r, shift, acc
        )
        return (y, dh2), keep, send

    early = [twin(low1, devices), twin(top2, devices)]
    acc, keep0, send0 = quarter_of(0, [quarter], [twin0], None)
    acc, keep0, send0, early, top1, low2 = lax.optimization_barrier(
        (acc, keep0, send0, early, top1, low2)
    )
    far = [over(top2, 1), over(low1, 2)]
    got0, later2 = twin(send0, devices), twin(low2, devices)
    (later1,) = stage(twin(top1, devices))
    acc, keep1, send1 = quarter_of(1, [top1, low1], [later1, early[0]], acc)
    acc, keep1, send1, far, later2, got0 = lax.optimization_barrier(
        (acc, keep1, send1, far, later2, got0)
    )
    twin_far, got1 = [twin(f, devices) for f in far], twin(send1, devices)
    acc, keep2, send2 = quarter_of(2, [top2, low2], [early[1], later2], acc)
    acc, keep2, send2, twin_far, got1 = lax.optimization_barrier(
        (acc, keep2, send2, twin_far, got1)
    )
    got2 = twin(send2, devices)
    acc, keep3, send3 = quarter_of(3, far, twin_far, acc)
    (y, dh2), keep3, send3, got2 = lax.optimization_barrier((acc, keep3, send3, got2))
    (got3,) = stage(twin(send3, devices))
    term3 = plus(keep3, got3)
    ends = [over(term3[:cut], 1), over(term3[cut:], 2)]

    c1_sum = placed([v[0] for v in sums], me)
    def to_heads(part):
        part = lax.all_to_all(part, "seq", split_axis=0, concat_axis=0, tiled=True)
        return part.reshape(1, clip_rows, local)

    layer_out = grad_middle = None
    das, heads, column_sums = ([None] * clips for _ in range(3))
    for c in range(clips):
        layer_out, grad_middle, das[c], heads[c], column_sums[c] = project_back(
            c, y, dh2, middle, dy, wo, g2, c2, tokens.shape, ring, layer_out, grad_middle
        )
        if c == 0:
            moved = to_heads(heads[0])
    term_wo = project_weight(das, attended, column_sums, c1_sum)
    moved, term_wo, end2, end1 = stage(moved, term_wo, *ends)
    owned_wo = to_owners(term_wo)

    second = [
        over(plus_rows(keep1, got1, end1, cut), 1),
        over(plus_rows(keep2, got2, end2, 0), 2),
    ]
    acc, flying, token_terms = None, [], [None] * clips

    def exchange(parts):
        return lax.all_to_all(parts, "seq", 0, 0, tiled=True)

    def to_all(part):
        return exchange(jnp.broadcast_to(part[None], (ring,) + part.shape))

    for c in range(clips):
        later = [to_heads(heads[c + 1])] if c + 1 < clips else []
        if c == clips - 1:
            owned_wo = owned_wo.reshape(ring, own // ring, width + 128)
            later = [lax.dynamic_index_in_dim(owned_wo, me ^ r, 0, False) for r in range(ring)]
            later = [over(t, r) if r else t for r, t in enumerate(later)]
        d = attend_back(qkv[c], moved, outs[c], logs[c], length(c))
        if c < clips - 1:
            acc = qkv_weight(me, d[0], normed[c], mine, acc, ring, False)
        d, later, flying, second, acc = lax.optimization_barrier((d, later, flying, second, acc))
        moved, wo_terms = later[0], later
        if c:
            token_terms[c - 1] = flying[0]
        else:
            total = plus(keep0, got0).astype(F32)
            total = total + second[0].astype(F32) + second[1].astype(F32)
            owned_mlp = lax.psum_scatter(
                total.astype(BF16),
                "fsdp",
                scatter_dimension=0,
                tiled=True,
                axis_index_groups=same_core,
            )[0]
            second = []
        last = c == clips - 1
        if c == clips - 1:
            d, owned_mlp = stage(d, owned_mlp)
            copies = jnp.broadcast_to(owned_mlp[None], (ring,) + owned_mlp.shape)
            d, copies = stage(d, copies)
            shared = exchange(copies)
            grad_mine, parts = qkv_weight(me, d[0], normed[c], mine, acc, ring, True)
            parts, shared, grad_mine = stage(parts, shared, grad_mine)
            owned = to_owners(grad_mine)
        else:
            parts = qkv_back(d[0], mine, ring)
        flying = [exchange(parts)]

    wo_term = sum(t.astype(F32) for t in wo_terms).astype(BF16)
    wo_parts = [over(wo_term, r) if r else wo_term for r in range(ring)]
    grad_inputs = None
    for c in range(clips - 1):
        grad_inputs = tokens_back(c, token_terms[c], tokens, grad_middle, g1, grad_inputs)
    grad_w1, grad_w2 = spread_mlp(shared)
    grad_inputs, grad_w1, grad_w2, flying, wo_parts = lax.optimization_barrier(
        (grad_inputs, grad_w1, grad_w2, flying, wo_parts)
    )
    owned, flying = lax.optimization_barrier((owned, flying))
    owned = [over(owned, r) if r else owned for r in range(ring)]
    grad_inputs = tokens_back(clips - 1, flying[0], tokens, grad_middle, g1, grad_inputs)
    grad_wo, grad_qkv, sums = spread_attn(me, wo_parts, owned)
    middle_sums, last_sums = sums[0], sums[1]
    return (
        layer_out,
        grad_inputs,
        last_sums[0],
        last_sums[1],
        grad_qkv,
        last_sums[2],
        last_sums[3],
        grad_wo,
        middle_sums[3],
        middle_sums[0],
        middle_sums[1],
        grad_w1,
        middle_sums[4 : count - 4].reshape(-1),
        grad_w2,
        middle_sums[2],
    )


def solution(mesh):
    act, vec, mat = P("fsdp", "seq", None), P("fsdp"), P("fsdp", None)
    in_specs = (act, vec, vec, vec, mat, vec, vec, mat, vec, vec, vec, mat, vec, mat, vec, act)
    out_specs = (act, act, vec, vec, mat, vec, vec, mat, vec, vec, vec, mat, vec, mat, vec)
    ring, devices = mesh.shape["seq"], mesh.shape["fsdp"]

    def layer(*args):
        clips, rows, width = args[0].shape
        square = ring == 4 and args[11].shape[1] == ring * width and devices % 4 == 0
        square = square and clips % (2 * devices) == 0 and width % (128 * devices) == 0
        return jax.shard_map(
            functools.partial(shards if square else shards_any, ring, devices),
            mesh=mesh,
            in_specs=in_specs,
            out_specs=out_specs,
            check_vma=False,
        )(*args)

    return layer
```

```python
import functools

import jax
import jax.numpy as jnp
from jax import lax
from jax.experimental import pallas as pl
from jax.experimental.pallas import tpu as pltpu
from jax.sharding import PartitionSpec as P

HEAD_DIM = 64
PAIR = 2 * HEAD_DIM
EPSILON = 1e-06
NEGATIVE = -1e30
F32, BF16 = jnp.float32, jnp.bfloat16
SCALE = HEAD_DIM ** -0.5
SCALE2 = SCALE * 1.4426950408889634
NT = (((1,), (1,)), ((), ()))
NN = (((1,), (0,)), ((), ()))
TN = (((0,), (0,)), ((), ()))


def dot(a, b, dims=NN):
    return lax.dot_general(a, b, dims, preferred_element_type=F32)


LARGE = 56 << 20
WHOLE = pl.BlockSpec(memory_space=pltpu.VMEM)
SCALAR = pl.BlockSpec(memory_space=pltpu.SMEM)


def kernel_call(body, name, operands, outs, scratch=(), scalars=0, aliases=None, vmem=40):
    return pl.pallas_call(
        body,
        in_specs=[SCALAR] * scalars + [WHOLE] * (len(operands) - scalars),
        out_specs=[WHOLE] * len(outs),
        out_shape=[jax.ShapeDtypeStruct(*out) for out in outs],
        scratch_shapes=list(scratch),
        input_output_aliases=aliases or {},
        compiler_params=pltpu.CompilerParams(vmem_limit_bytes=vmem << 20),
        cost_estimate=pl.CostEstimate(flops=1 << 20, bytes_accessed=1 << 20, transcendentals=0),
        name=name,
    )(*operands)


def of_head(block, h):
    lane = lax.broadcasted_iota(jnp.int32, (1, PAIR), 1)
    return jnp.where(lane // HEAD_DIM == h, block, jnp.zeros_like(block))


def valid_rows(j, bk, length):
    return j * bk + lax.broadcasted_iota(jnp.int32, (bk, 1), 0) < length


def transposed_chunks(out_ref, in_ref, cols, bk):
    for j in range(in_ref.shape[1] // bk):
        out_ref[j] = jnp.transpose(in_ref[0, pl.ds(j * bk, bk), cols])


def attend_kernel(len_ref, q_ref, k_ref, v_ref, o_ref, lse_ref, s_ref, vt_ref, ot_ref, *, bk):
    length = len_ref[pl.program_id(0)]
    rows_all, width = q_ref.shape[1:]
    chunks = pl.cdiv(length, bk)
    for pair in range(width // PAIR):
        cols = pl.ds(PAIR * pair, PAIR)
        transposed_chunks(vt_ref, v_ref, cols, bk)
        queries = [of_head(q_ref[0, :, cols], h) for h in range(2)]

        def score(j, tops):
            keys = k_ref[0, pl.ds(pl.multiple_of(j * bk, bk), bk), cols]
            ok = valid_rows(j, bk, length)
            out = []
            for h in range(2):
                s = jnp.where(ok, dot(keys, queries[h], NT), NEGATIVE)
                s_ref[h, j] = s
                top = tops[h]
                for i in range(bk // 8):
                    top = jnp.maximum(top, s[8 * i : 8 * i + 8])
                out.append(top)
            return tuple(out)

        low = jnp.full((8, rows_all), NEGATIVE, F32)
        tops = lax.fori_loop(0, chunks, score, (low, low))
        peaks = [jnp.max(top, axis=0, keepdims=True) * SCALE2 for top in tops]
        ot_ref[...] = jnp.zeros_like(ot_ref)

        def mix(j, sums):
            out = []
            for h in range(2):
                p = jnp.exp2(s_ref[h, j] * SCALE2 - peaks[h])
                total = sums[h]
                for i in range(bk // 8):
                    total = total + p[8 * i : 8 * i + 8]
                out.append(total)
                half = pl.ds(HEAD_DIM * h, HEAD_DIM)
                ot_ref[half] += dot(vt_ref[j, half], p.astype(BF16))
            return tuple(out)

        zero = jnp.zeros((8, rows_all), F32)
        sums = lax.fori_loop(0, chunks, mix, (zero, zero))
        for h in range(2):
            total = jnp.sum(sums[h], axis=0, keepdims=True)
            half = pl.ds(HEAD_DIM * h, HEAD_DIM)
            lse_ref[0, pl.ds(2 * pair + h, 1)] = peaks[h] + jnp.log2(total)
            ot_ref[half] = ot_ref[half] / total
        o_ref[0, :, cols] = jnp.transpose(ot_ref[...]).astype(BF16)


def attend_back_kernel(
    len_ref, q_ref, k_ref, v_ref, do_ref, o_ref, lse_ref, d_ref, kt_ref, dqt_ref, *, bk
):
    length = len_ref[pl.program_id(0)]
    width = q_ref.shape[2]
    chunks = pl.cdiv(length, bk)
    d_ref[...] = jnp.zeros_like(d_ref)
    for pair in range(width // PAIR):
        cols = pl.ds(PAIR * pair, PAIR)
        outs = do_ref[0, :, cols]
        both = jnp.transpose(outs.astype(F32) * o_ref[0, :, cols].astype(F32))
        inner = [
            jnp.sum(both[HEAD_DIM * h : HEAD_DIM * (h + 1)], axis=0, keepdims=True)
            for h in range(2)
        ]
        queries = [of_head(q_ref[0, :, cols], h) for h in range(2)]
        grads = [of_head(outs, h) for h in range(2)]
        logs = [lse_ref[0, pl.ds(2 * pair + h, 1)] for h in range(2)]
        transposed_chunks(kt_ref, k_ref, cols, bk)
        dqt_ref[...] = jnp.zeros_like(dqt_ref)

        def step(j, carry):
            rows = pl.ds(pl.multiple_of(j * bk, bk), bk)
            keys = k_ref[0, rows, cols]
            values = v_ref[0, rows, cols]
            ok = valid_rows(j, bk, length)
            dk = jnp.zeros((bk, PAIR), F32)
            dv = jnp.zeros((bk, PAIR), F32)
            for h in range(2):
                p = jnp.exp2(dot(keys, queries[h], NT) * SCALE2 - logs[h])
                p = jnp.where(ok, p, 0.0)
                g = (p * (dot(values, grads[h], NT) - inner[h])).astype(BF16)
                dv = dv + dot(p.astype(BF16), grads[h])
                dk = dk + dot(g, queries[h])
                half = pl.ds(HEAD_DIM * h, HEAD_DIM)
                dqt_ref[half] += dot(kt_ref[j, half], g)
            d_ref[0, rows, pl.ds(width + PAIR * pair, PAIR)] = (dk * SCALE).astype(BF16)
            d_ref[0, rows, pl.ds(2 * width + PAIR * pair, PAIR)] = dv.astype(BF16)
            return carry

        lax.fori_loop(0, chunks, step, 0)
        d_ref[0, :, cols] = jnp.transpose(dqt_ref[...] * SCALE).astype(BF16)


def chunk_rows(rows):
    return max(b for b in range(8, 225, 8) if rows % b == 0)


def block(rows, width, at):
    return pl.BlockSpec((1, rows, width), lambda c, n: (c, 0, at))


def attend(qkv, lengths):
    clips, rows, triple = qkv.shape
    width = triple // 3
    heads, bk = width // HEAD_DIM, chunk_rows(rows)
    cost = clips * heads * rows * rows
    return pl.pallas_call(
        functools.partial(attend_kernel, bk=bk),
        grid_spec=pltpu.PrefetchScalarGridSpec(
            num_scalar_prefetch=1,
            grid=(clips,),
            in_specs=[block(rows, width, i) for i in range(3)],
            out_specs=[block(rows, width, 0), block(heads, rows, 0)],
            scratch_shapes=[
                pltpu.VMEM((2, rows // bk, bk, rows), F32),
                pltpu.VMEM((rows // bk, PAIR, bk), BF16),
                pltpu.VMEM((PAIR, rows), F32),
            ],
        ),
        out_shape=[
            jax.ShapeDtypeStruct((clips, rows, width), BF16),
            jax.ShapeDtypeStruct((clips, heads, rows), F32),
        ],
        compiler_params=pltpu.CompilerParams(vmem_limit_bytes=LARGE),
        cost_estimate=pl.CostEstimate(
            flops=1 << 20, bytes_accessed=1 << 20, transcendentals=0
        ),
        name="attend",
    )(lengths, qkv, qkv, qkv)


def attend_back(qkv, grads, outs, logs, lengths):
    clips, rows, triple = qkv.shape
    width = triple // 3
    heads, bk = width // HEAD_DIM, chunk_rows(rows)
    cost = clips * heads * rows * rows
    return pl.pallas_call(
        functools.partial(attend_back_kernel, bk=bk),
        grid_spec=pltpu.PrefetchScalarGridSpec(
            num_scalar_prefetch=1,
            grid=(clips,),
            in_specs=[block(rows, width, i) for i in (0, 1, 2, 0, 0)] + [block(heads, rows, 0)],
            out_specs=block(rows, triple, 0),
            scratch_shapes=[
                pltpu.VMEM((rows // bk, PAIR, bk), BF16),
                pltpu.VMEM((PAIR, rows), F32),
            ],
        ),
        out_shape=jax.ShapeDtypeStruct((clips, rows, triple), BF16),
        compiler_params=pltpu.CompilerParams(vmem_limit_bytes=LARGE),
        cost_estimate=pl.CostEstimate(
            flops=1 << 20, bytes_accessed=1 << 20, transcendentals=0
        ),
        name="attend_back",
    )(lengths, qkv, qkv, qkv, grads, outs, logs)


def norm_kernel(me_ref, *refs, counts):
    parts, rest = refs[: sum(counts)], refs[sum(counts) :]
    g_ref, b_ref, w_ref, bias_ref, h_ref, qkv_ref, x_ref = rest
    taken = 0
    for r, count in enumerate(counts):
        group = parts[taken : taken + count]
        taken += count

        @pl.when(pl.program_id(0) == r)
        def _():
            row = 0
            for ref in group:
                x_ref[pl.ds(row, ref.shape[0])] = ref[...]
                row += ref.shape[0]

    normed, _ = normalize(x_ref[...].astype(F32))
    h = (normed * g_ref[...] + b_ref[...]).astype(BF16)
    h_ref[0] = h
    qkv_ref[0] = (dot(h, w_ref[...]) + bias_ref[...]).astype(BF16)


def norm_project(me, groups, gain, shift, weight, bias):
    flat = [part if isinstance(part, tuple) else (part, None) for g in groups for part in g]
    triple, ring = bias.shape[-1], len(groups)
    rows, width = flat[0][0].shape[-2:]

    def part_spec(array, clip):
        if clip is None:
            return pl.BlockSpec(array.shape, lambda r, m: (0, 0))
        return pl.BlockSpec((None, rows, width), lambda r, m: (clip, 0, 0))

    def out(cols):
        return pl.BlockSpec((1, rows, cols), lambda r, m: (m[0] ^ r, 0, 0))

    h, qkv = pl.pallas_call(
        functools.partial(norm_kernel, counts=[len(g) for g in groups]),
        grid_spec=pltpu.PrefetchScalarGridSpec(
            num_scalar_prefetch=1,
            grid=(ring,),
            in_specs=[part_spec(*part) for part in flat]
            + [WHOLE] * 2
            + [pl.BlockSpec((width, triple), lambda r, m: (0, 0)), WHOLE],
            out_specs=[out(width), out(triple)],
            scratch_shapes=[pltpu.VMEM((rows, width), BF16)],
        ),
        out_shape=[jax.ShapeDtypeStruct((ring, rows, c), BF16) for c in (width, triple)],
        compiler_params=pltpu.CompilerParams(vmem_limit_bytes=LARGE),
        cost_estimate=pl.CostEstimate(flops=1 << 20, bytes_accessed=1 << 20, transcendentals=0),
        name="norm_project",
    )(me[None], *[part[0] for part in flat], gain[None], shift[None], weight, bias[None])
    return h.reshape(ring * rows, width), qkv.reshape(1, ring * rows, triple)


def mlp_piece_kernel(core_ref, h_ref, ht_ref, dy_ref, *refs, first, nz, counts):
    mines, others, refs = refs[: counts[0]], refs[counts[0] : sum(counts)], refs[sum(counts) :]
    c1_ref, *refs = refs
    yin_ref, dhin_ref = (None, None) if first else (refs.pop(0), refs.pop(0))
    y_ref, dh_ref, keep_ref, send_ref, sums_ref, hm_ref, hmt_ref, w1_ref, w2_ref, u_ref, dz_ref = refs
    core = core_ref[0]
    width = h_ref.shape[1]
    clips, _, share = ht_ref.shape
    rows = mines[0].shape[2]
    half = nz * rows

    def at(i, p):
        block = 2 * i + (core if p == 0 else 1 - core)
        return pl.ds(pl.multiple_of(block * rows, rows), rows)

    def put(i, p):
        return pl.ds(p * half + i * rows, rows)

    def source(i, p):
        parts = (mines, others)[p]
        size = nz // len(parts)
        return parts[i // size], i % size

    for i in range(nz):
        for p in range(2):
            hm_ref[:, put(i, p)] = h_ref[:, at(i, p)]
            for c in range(clips):
                hmt_ref[c, put(i, p), :] = ht_ref[c, at(i, p), :]
            src, z = source(i, p)
            w2_ref[pl.ds((2 * i + p) * rows, rows), :] = src[z, 1]
            for j in range(nz):
                for r in range(2):
                    w1_ref[put(i, p), pl.ds((2 * j + r) * rows, rows)] = src[z, 0, :, at(j, r)]
    for i in range(nz):
        cols = pl.ds(2 * i * rows, 2 * rows)
        bias = jnp.concatenate([c1_ref[:, at(i, p)] for p in range(2)], axis=1)
        z = dot(hm_ref[...], w1_ref[:, cols]) + bias
        phi = 0.5 * (1.0 + lax.erf(z * (2.0 ** -0.5)))
        u_ref[:, cols] = (z * phi).astype(BF16)
        slope = phi + z * (jnp.exp(z * z * -0.5) * 0.3989422804014327)
        dz = (dot(dy_ref[...], w2_ref[cols, :], NT) * slope).astype(BF16)
        dz_ref[:, cols] = dz
        total = jnp.sum(dz.astype(F32), axis=0, keepdims=True)
        for p in range(2):
            sums_ref[:, at(i, p)] = total[:, p * rows : (p + 1) * rows]
        g2 = dot(u_ref[:, cols], dy_ref[...], TN).astype(BF16)
        keep_ref[i, 1] = g2[:rows]
        send_ref[i, 1] = g2[rows:]
        g1 = sum(dot(hmt_ref[c], dz_ref[pl.ds(c * share, share), cols]) for c in range(clips))
        g1 = g1.astype(BF16)
        for p in range(2):
            part = g1[:, p * rows : (p + 1) * rows]
            keep_ref[:, 0, :, at(i, p)] = part[:half].reshape(nz, rows, rows)
            send_ref[:, 0, :, at(i, p)] = part[half:].reshape(nz, rows, rows)
    for n in range(width // 256):
        cols = pl.ds(256 * n, 256)
        y = dot(u_ref[...], w2_ref[:, cols])
        y_ref[:, cols] = y if first else y + yin_ref[:, cols]
    for n in range(width // 256):
        d = dot(dz_ref[...], w1_ref[pl.ds(256 * n, 256), :], NT)
        for q in range(256 // rows):
            p, i = divmod((256 // rows) * n + q, nz)
            v = d[:, q * rows : (q + 1) * rows]
            dh_ref[:, at(i, p)] = v if first else v + dhin_ref[:, at(i, p)]


def mlp_piece(core, h2, h2t, dy, mine, other, c1, acc):
    rows = mine[0].shape[2]
    t, width = h2.shape
    nz = width // (2 * rows)
    first = acc is None
    ins = [core, h2, h2t, dy, *mine, *other, c1] + ([] if first else list(acc))
    gradient = ((nz, 2, rows, width), BF16)
    return kernel_call(
        functools.partial(
            mlp_piece_kernel, first=first, nz=nz, counts=(len(mine), len(other))
        ),
        "mlp_piece",
        ins,
        [((t, width), F32), ((t, width), F32), gradient, gradient, (c1.shape, F32)],
        scratch=[pltpu.VMEM((t, width), BF16), pltpu.VMEM(h2t.shape, BF16)]
        + [pltpu.VMEM((width, width), BF16)] * 2
        + [pltpu.VMEM((t, width), BF16)] * 2,
        scalars=1,
        aliases={} if first else {len(ins) - 2: 0, len(ins) - 1: 1},
        vmem=24,
    )


def project_kernel(*refs, clips):
    moved, rest = refs[:clips], refs[clips:]
    x_ref, wo_ref, bo_ref, g_ref, b_ref, att_ref, mid_ref, h_ref, ht_ref = rest
    ring, rows, local = moved[0].shape
    for c in range(clips):
        at = pl.ds(c * rows, rows)
        for s in range(ring):
            att_ref[at, pl.ds(s * local, local)] = moved[c][s]
        middle = x_ref[c].astype(F32) + (dot(att_ref[at, :], wo_ref[...]) + bo_ref[...])
        mid_ref[at, :] = middle
        h = (normalize(middle)[0] * g_ref[...] + b_ref[...]).astype(BF16)
        h_ref[at, :] = h
        ht_ref[c] = jnp.transpose(h)


def project_norm(moved, tokens, wo, bo, gain, shift):
    clips, rows, width = tokens.shape
    flat = (clips * rows, width)
    return kernel_call(
        functools.partial(project_kernel, clips=clips),
        "project_norm",
        [*moved, tokens, wo, bo[None], gain[None], shift[None]],
        [(flat, BF16), (flat, F32), (flat, BF16), ((clips, width, rows), BF16)],
    )


def project_back_kernel(*refs, clip, first):
    y_ref, dh_ref, mid_ref, dy_ref, wo_ref, g_ref, c2_ref = refs[:7]
    out_ref, gm_ref, da_ref, do_ref, sum_ref = refs[-5:]
    ring, rows, local = do_ref.shape
    middle = mid_ref[...]
    out_ref[0] = (middle + (y_ref[...] + c2_ref[...])).astype(BF16)
    normed, rstd = normalize(middle)
    dh = dh_ref[...]
    dy = dy_ref[...].astype(F32)
    grad = dy + normalize_back(dh, normed, rstd, g_ref[...])
    gm_ref[0] = grad
    da = grad.astype(BF16)
    da_ref[...] = da
    do = dot(da, wo_ref[...], NT).astype(BF16)
    for s in range(ring):
        do_ref[s] = do[:, s * local : (s + 1) * local]
    sum_ref[...] = jnp.zeros_like(sum_ref)
    for i, terms in enumerate((dh * normed, dh, dy, da.astype(F32))):
        sum_ref[pl.ds(i, 1), :] = jnp.sum(terms, axis=0, keepdims=True)


def project_back(c, y, dh, middle, dy, wo, gain, c2, shape, ring, out, grad):
    clips, rows, width = shape
    at = pl.BlockSpec((rows, width), lambda i: (c, 0))
    at_c = pl.BlockSpec((1, rows, width), lambda i: (c, 0, 0))
    one = pl.BlockSpec((1, width), lambda i: (0, 0))
    back = [] if out is None else [out, grad]
    return pl.pallas_call(
        functools.partial(project_back_kernel, clip=c, first=out is None),
        grid=(1,),
        in_specs=[at] * 4
        + [pl.BlockSpec((width, width), lambda i: (0, 0)), one, one]
        + [pl.BlockSpec(memory_space=pl.ANY)] * len(back),
        out_specs=[
            at_c,
            at_c,
            pl.BlockSpec((rows, width), lambda i: (0, 0)),
            pl.BlockSpec((ring, rows, width // ring), lambda i: (0, 0, 0)),
            pl.BlockSpec((8, width), lambda i: (0, 0)),
        ],
        out_shape=[
            jax.ShapeDtypeStruct(shape, BF16),
            jax.ShapeDtypeStruct(shape, F32),
            jax.ShapeDtypeStruct((rows, width), BF16),
            jax.ShapeDtypeStruct((ring, rows, width // ring), BF16),
            jax.ShapeDtypeStruct((8, width), F32),
        ],
        input_output_aliases={7: 0, 8: 1} if back else {},
        compiler_params=pltpu.CompilerParams(vmem_limit_bytes=LARGE),
        cost_estimate=pl.CostEstimate(flops=1 << 20, bytes_accessed=1 << 20, transcendentals=0),
        name="project_back",
    )(y, dh, middle, dy, wo, gain[None], c2[None], *back)


def project_weight_kernel(*refs, clips):
    das, att_ref, sums = refs[:clips], refs[clips], refs[clips + 1 : 2 * clips + 1]
    c1_ref, gw_ref, sum_ref = refs[2 * clips + 1 :]
    rows, width = das[0].shape
    term = dot(att_ref[pl.ds(0, rows), :], das[0][...], TN)
    total = sums[0][...]
    for c in range(1, clips):
        term = term + dot(att_ref[pl.ds(c * rows, rows), :], das[c][...], TN)
        total = total + sums[c][...]
    sum_ref[...] = jnp.zeros_like(sum_ref)
    sum_ref[pl.ds(0, 8), :] = total
    sum_ref[pl.ds(4, c1_ref.shape[0]), :] = c1_ref[...]
    gw_ref[:, pl.ds(0, width)] = term.astype(BF16)
    gw_ref[:, pl.ds(width, 128)] = jnp.transpose(sum_ref[...]).astype(BF16)


def project_weight(das, attended, sums, c1_sum):
    width = attended.shape[1]
    return kernel_call(
        functools.partial(project_weight_kernel, clips=len(das)),
        "project_weight",
        [*das, attended, *sums, c1_sum],
        [((width, width + 128), BF16)],
        scratch=[pltpu.VMEM((128, width), F32)],
        vmem=56,
    )[0]


def qkv_back_kernel(d_ref, w_ref, part_ref):
    part_ref[0] = dot(d_ref[...], w_ref[...], NT).astype(BF16)


def qkv_back(d, weight, ring):
    whole, triple = d.shape
    width, rows = weight.shape[0], whole // ring
    return pl.pallas_call(
        qkv_back_kernel,
        grid=(ring,),
        in_specs=[
            pl.BlockSpec((rows, triple), lambda r: (r, 0)),
            pl.BlockSpec((width, triple), lambda r: (0, 0)),
        ],
        out_specs=pl.BlockSpec((1, rows, width), lambda r: (r, 0, 0)),
        out_shape=jax.ShapeDtypeStruct((ring, rows, width), BF16),
        compiler_params=pltpu.CompilerParams(vmem_limit_bytes=LARGE),
        cost_estimate=pl.CostEstimate(flops=1 << 20, bytes_accessed=1 << 20, transcendentals=0),
        name="qkv_back",
    )(d, weight)


def qkv_weight_kernel(me_ref, d_ref, h_ref, w_ref, *rest, first, last):
    rest = list(rest)
    acc_ref, bias_ref = (None, None) if first else (rest.pop(0), rest.pop(0))
    triple = d_ref.shape[1]
    local = triple // 3
    term = dot(h_ref[...], d_ref[...], TN)
    bias = jnp.sum(d_ref[...].astype(F32), axis=0, keepdims=True)
    if not first:
        term = term + acc_ref[...]
        bias = bias + bias_ref[pl.ds(0, 1), :]
    if not last:
        out_ref, sum_ref = rest
        out_ref[...] = term
        sum_ref[...] = jnp.broadcast_to(bias, sum_ref.shape)
        return
    out_ref, own_ref, one_ref, two_ref, top_ref, low_ref, row_ref = rest
    rows, cut = own_ref.shape[1], top_ref.shape[0]
    for r in (3, 1, 2, 0):
        at = pl.ds(pl.multiple_of((me_ref[0] ^ r) * rows, 8), rows)
        part = dot(d_ref[at, :], w_ref[:, pl.ds(0, triple)], NT).astype(BF16)
        if r == 3:
            top_ref[...] = part[:cut]
            low_ref[...] = part[cut:]
        else:
            (own_ref, one_ref, two_ref)[r][0] = part
    out_ref[:, pl.ds(0, triple)] = term.astype(BF16)
    weight = w_ref[:, pl.ds(0, triple)].astype(F32)
    vectors = w_ref[:, pl.ds(triple, 128)].astype(F32)
    gain, shift = vectors[:, 0:1], vectors[:, 1:2]
    shift_sum = jnp.sum(weight * bias, axis=1, keepdims=True)
    gain_sum = (jnp.sum(weight * term, axis=1, keepdims=True) - shift * shift_sum) / gain
    row_ref[...] = jnp.zeros_like(row_ref)
    at_me = pl.ds(pl.multiple_of(me_ref[0] * local, local), local)
    row_ref[pl.ds(2, 1), at_me] = bias[:, :local]
    row_ref[pl.ds(3, 1), at_me] = bias[:, 2 * local :]
    lane = lax.broadcasted_iota(jnp.int32, (1, 128), 1)
    sums = jnp.transpose(row_ref[...])
    sums = jnp.where(lane == 0, gain_sum, jnp.where(lane == 1, shift_sum, sums))
    out_ref[:, pl.ds(triple, 128)] = sums.astype(BF16)


def qkv_weight(me, d, h, mine, acc, ring, last):
    (whole, triple), width = d.shape, h.shape[1]
    outs = [((width, triple), F32), ((8, triple), F32)]
    if last:
        rows = whole // ring
        cut = rows // 16 * 8
        outs = [((width, triple + 128), BF16)] + [((1, rows, width), BF16)] * 3
        outs += [((cut, width), BF16), ((rows - cut, width), BF16)]
    return kernel_call(
        functools.partial(qkv_weight_kernel, first=acc is None, last=last),
        "qkv_weight",
        [me[None], d, h, mine] + list(acc or ()),
        outs,
        scratch=[pltpu.VMEM((128, width), F32)] if last else (),
        scalars=1,
        vmem=56,
    )


def tokens_back_kernel(*refs, counts):
    term_refs, (x_ref, gm_ref, g_ref) = refs[: len(counts)], refs[len(counts) : len(counts) + 3]
    out_ref = refs[-1]
    grad = None
    for count, ref in zip(counts, term_refs):
        for r in range(count):
            term = ref[r].astype(F32)
            grad = term if grad is None else grad + term
    normed, rstd = normalize(x_ref[0].astype(F32))
    out_ref[0] = gm_ref[0] + normalize_back(grad, normed, rstd, g_ref[...])


def tokens_back(c, terms, tokens, grad_middle, gain, out):
    clips, rows, width = tokens.shape
    steps = max(n for n in (7, 4, 2, 1) if rows % (8 * n) == 0)
    block = rows // steps
    at_c = pl.BlockSpec((1, block, width), lambda i: (c, i, 0))
    counts = [count for _, count in terms]
    specs = [pl.BlockSpec((n, block, width), lambda i: (0, i, 0)) for n in counts] + [at_c, at_c]
    specs.append(pl.BlockSpec((1, width), lambda i: (0, 0)))
    operands = [*[array for array, _ in terms], tokens, grad_middle, gain[None]]
    if out is not None:
        specs.append(pl.BlockSpec(memory_space=pl.ANY))
        operands.append(out)
    return pl.pallas_call(
        functools.partial(tokens_back_kernel, counts=counts),
        grid=(steps,),
        in_specs=specs,
        out_specs=at_c,
        out_shape=jax.ShapeDtypeStruct((clips, rows, width), F32),
        input_output_aliases={} if out is None else {len(operands) - 1: 0},
        compiler_params=pltpu.CompilerParams(vmem_limit_bytes=LARGE),
        cost_estimate=pl.CostEstimate(flops=1 << 20, bytes_accessed=1 << 20, transcendentals=0),
        name="tokens_back",
    )(*operands)


def add_kernel(*refs, ranges):
    out_ref = refs[-1]
    step = pl.program_id(0)
    total = None
    for (start, stop), ref in zip(ranges, refs):
        term = ref[...].astype(F32)
        if start is not None:
            inside = (step >= start) & (step < stop)
            term = jnp.where(inside, term, 0.0)
        total = term if total is None else total + term
    out_ref[...] = total.astype(BF16)


def add_terms(terms):
    shape = terms[0][0].shape
    block = (1,) + shape[1:]
    rest = (0,) * (len(shape) - 1)

    def spec(count, row):
        if row is None:
            return pl.BlockSpec(block, lambda z: (z, *rest))
        return pl.BlockSpec(block, lambda z: (jnp.clip(z - row, 0, count - 1), *rest))

    return pl.pallas_call(
        functools.partial(
            add_kernel,
            ranges=[(r, None if r is None else r + t.shape[0]) for t, r in terms],
        ),
        grid=shape[:1],
        in_specs=[spec(t.shape[0], row) for t, row in terms],
        out_specs=pl.BlockSpec(block, lambda z: (z, *rest)),
        out_shape=jax.ShapeDtypeStruct(shape, BF16),
        compiler_params=pltpu.CompilerParams(vmem_limit_bytes=24 << 20),
        cost_estimate=pl.CostEstimate(flops=1 << 20, bytes_accessed=1 << 20, transcendentals=0),
        name="add_terms",
    )(*[t for t, _ in terms])


def spread_mlp_kernel(me_ref, own_ref, one_ref, two_ref, far1_ref, far2_ref, w1_ref, w2_ref):
    own = own_ref.shape[1]
    ring = w1_ref.shape[1] // own_ref.shape[2]
    firsts = [own_ref.at[0], one_ref.at[0], two_ref.at[0], far1_ref.at[0]]
    seconds = [own_ref.at[1], one_ref.at[1], two_ref.at[1], far2_ref.at[0]]
    for r in range(ring):
        q = me_ref[0] ^ r
        part = firsts[r][...].astype(F32)
        for f in range(part.shape[1] // own):
            at = pl.ds(pl.multiple_of((f * ring + q) * own, own), own)
            w1_ref[:, at] = part[:, f * own : (f + 1) * own]
        w2_ref[pl.ds(pl.multiple_of(q * own, own), own), :] = seconds[r][...].astype(F32)


def spread_mlp(me, parts, ring):
    _, own, width = parts[0].shape
    return kernel_call(
        spread_mlp_kernel,
        "spread_mlp",
        [me[None], *parts],
        [((own, ring * width), F32), ((ring * own, width), F32)],
        scalars=1,
    )


def spread_attn_kernel(me_ref, *refs, ring):
    wo_ref, qkv_refs = refs[0], refs[1 : ring + 1]
    gwo_ref, gqkv_ref, vec_ref, more_ref = refs[ring + 1 :]
    own, width = gwo_ref.shape
    rows = wo_ref.shape[1]
    triple = qkv_refs[0].shape[1] - 128
    local = triple // 3
    last = jnp.zeros((own, 128), F32)
    for r in range(ring):
        q = me_ref[0] ^ r
        gwo_ref[pl.ds(r * rows, rows), :] = wo_ref[r, :, :width].astype(F32)
        more_ref[pl.ds(r * rows, rows), :] = wo_ref[r, :, width:].astype(F32)
        last = last + qkv_refs[r][:, triple:].astype(F32)
        for i in range(3):
            part = qkv_refs[r][:, i * local : (i + 1) * local].astype(F32)
            gqkv_ref[:, pl.ds(pl.multiple_of(i * width + q * local, local), local)] = part
    vec_ref[0] = jnp.transpose(more_ref[...])
    vec_ref[1] = jnp.transpose(last)


def spread_attn(me, wo_parts, qkv_parts):
    ring, own = len(qkv_parts), qkv_parts[0].shape[0]
    width = wo_parts.shape[2] - 128
    return kernel_call(
        functools.partial(spread_attn_kernel, ring=ring),
        "spread_attn",
        [me[None], wo_parts, *qkv_parts],
        [((own, width), F32), ((own, 3 * width), F32), ((2, 128, own), F32)],
        scratch=[pltpu.VMEM((own, 128), F32)],
        scalars=1,
    )


def swap(value, ring, r):
    return lax.ppermute(value, "seq", [(i, i ^ r) for i in range(ring)])


def gather_seq(value, ring, me):
    out = jnp.zeros((ring,) + value.shape, value.dtype)
    out = lax.dynamic_update_index_in_dim(out, value, me, 0)
    for r in range(1, ring):
        out = lax.dynamic_update_index_in_dim(out, swap(value, ring, r), me ^ r, 0)
    return out


def sum_seq(terms, ring, me):
    total = lax.dynamic_index_in_dim(terms, me, 0, keepdims=False).astype(F32)
    for r in range(1, ring):
        term = lax.dynamic_index_in_dim(terms, me ^ r, 0, keepdims=False)
        total = total + swap(term, ring, r).astype(F32)
    return total


def to_owners(grad):
    return lax.psum_scatter(grad, "fsdp", scatter_dimension=0, tiled=True)


def sum_owned(owned, ring, me):
    rows, width = owned.shape
    part = sum_seq(owned.reshape(ring, rows // ring, width), ring, me).astype(BF16)
    return gather_seq(part, ring, me).reshape(rows, width).astype(F32)


def sum_vectors(rows, devices, ring):
    count, width = rows.shape
    sent = rows.reshape(count, devices, width // devices).transpose(1, 0, 2)
    total = jnp.sum(lax.all_to_all(sent, "fsdp", split_axis=0, concat_axis=0, tiled=True), axis=0)
    return total + sum(swap(total, ring, r) for r in range(1, ring))


def normalize(values):
    centered = values - jnp.mean(values, axis=-1, keepdims=True)
    variance = jnp.mean(centered * centered, axis=-1, keepdims=True)
    rstd = lax.rsqrt(variance + EPSILON)
    return centered * rstd, rstd


def normalize_back(grad, normed, rstd, gain):
    e = grad * gain
    mean = jnp.mean(e, axis=-1, keepdims=True)
    along = jnp.mean(e * normed, axis=-1, keepdims=True)
    return rstd * (e - mean - normed * along)


def shards_any(
    ring,
    devices,
    tokens,
    lengths,
    ln1_gain,
    ln1_bias,
    w_qkv,
    q_bias,
    v_bias,
    w_out,
    b_out,
    ln2_gain,
    ln2_bias,
    w_fc1,
    b_fc1,
    w_fc2,
    b_fc2,
    cotangent,
):
    clips, rows, width = tokens.shape
    total_rows = clips * rows
    clip_rows = rows * ring
    local = width // ring
    me = lax.axis_index("seq")

    whole = [gather_seq(tokens[c], ring, me).reshape(clip_rows, width) for c in range(clips)]

    own = ln1_gain.shape[0]
    packed = jnp.concatenate(
        [
            jnp.stack([ln1_gain, ln1_bias, q_bias, v_bias, b_out, ln2_gain, ln2_bias, b_fc2]),
            b_fc1.reshape(-1, own),
        ]
    )
    vectors = lax.all_gather(packed, "fsdp", axis=0, tiled=False)
    c1 = vectors[:, 8:].reshape(-1).astype(F32)
    vectors = vectors[:, :8].transpose(1, 0, 2).reshape(8, width).astype(F32)
    g1, b1, qb, vb, bo, g2, b2, c2 = (vectors[i] for i in range(8))
    qb_mine = lax.dynamic_slice_in_dim(qb, me * local, local)
    vb_mine = lax.dynamic_slice_in_dim(vb, me * local, local)
    bias_mine = jnp.concatenate([qb_mine, jnp.zeros_like(qb_mine), vb_mine])

    mine = lax.dynamic_index_in_dim(w_qkv.reshape(own, 3, ring, local), me, 2, keepdims=False)
    wqkv = lax.all_gather(mine.reshape(own, 3 * local), "fsdp", axis=0, tiled=True)
    wo = lax.all_gather(w_out, "fsdp", axis=0, tiled=True)
    w1 = lax.all_gather(w_fc1, "fsdp", axis=0, tiled=True)
    w2 = lax.all_gather(w_fc2, "fsdp", axis=0, tiled=True)

    normed, qkv, heads_out, logs, attended = [], [], [], [], []
    for c in range(clips):
        n1 = normalize(whole[c].astype(F32))[0]
        h1 = (n1 * g1 + b1).astype(BF16)
        part = (dot(h1, wqkv) + bias_mine).astype(BF16)[None]
        out, log = attend(part, lax.dynamic_slice_in_dim(lengths, c, 1))
        moved = lax.all_to_all(
            out.reshape(ring, rows, local), "seq", split_axis=0, concat_axis=0, tiled=True
        )
        normed.append(h1)
        qkv.append(part)
        heads_out.append(out)
        logs.append(log)
        attended.append(moved.transpose(1, 0, 2).reshape(rows, width))
    attended = jnp.concatenate(attended, axis=0)

    inputs = tokens.astype(F32).reshape(total_rows, width)
    middle = inputs + (dot(attended, wo) + bo)
    n2, r2 = normalize(middle)
    h2 = (n2 * g2 + b2).astype(BF16)
    z = dot(h2, w1) + c1
    phi = 0.5 * (1.0 + lax.erf(z * (2.0 ** -0.5)))
    hidden = (z * phi).astype(BF16)
    slope = phi + z * (jnp.exp(-0.5 * z * z) * 0.3989422804014327)
    layer_out = (middle + (dot(hidden, w2) + c2)).astype(BF16).reshape(clips, rows, width)

    dy = cotangent.reshape(total_rows, width)
    dy_f = dy.astype(F32)
    term_w2 = dot(hidden, dy, TN).astype(BF16)
    dz = (dot(dy, w2, NT) * slope).astype(BF16)
    term_w1 = dot(h2, dz, TN).astype(BF16)
    dh2 = dot(dz, w1, NT)
    grad_middle = dy_f + normalize_back(dh2, n2, r2, g2)
    da = grad_middle.astype(BF16)
    term_wo = dot(attended, da, TN).astype(BF16)
    do = dot(da, wo, NT).astype(BF16)
    do, term_w2, term_w1, term_wo = lax.optimization_barrier((do, term_w2, term_w1, term_wo))
    owned_w2, owned_w1, owned_wo = (to_owners(t) for t in (term_w2, term_w1, term_wo))

    dqkv, own_terms, gain_sum, shift_sum = [], [], 0.0, 0.0
    for c in range(clips):
        sent = do[c * rows : (c + 1) * rows].reshape(rows, ring, local).transpose(1, 0, 2)
        moved = lax.all_to_all(sent, "seq", split_axis=0, concat_axis=0, tiled=True)
        moved = moved.reshape(1, clip_rows, local)
        d = attend_back(
            qkv[c], moved, heads_out[c], logs[c], lax.dynamic_slice_in_dim(lengths, c, 1)
        )[0]
        dh1 = dot(d, wqkv, NT)
        n1 = normalize(whole[c].astype(F32))[0]
        gain_sum = gain_sum + jnp.sum(dh1 * n1, axis=0)
        shift_sum = shift_sum + jnp.sum(dh1, axis=0)
        own_terms.append(sum_seq(dh1.astype(BF16).reshape(ring, rows, width), ring, me))
        dqkv.append(d)
    dqkv = jnp.concatenate(dqkv, axis=0)
    grad_mine = dot(jnp.concatenate(normed, axis=0), dqkv, TN).astype(BF16)
    grad_mine, owned_w2, owned_w1, owned_wo = lax.optimization_barrier(
        (grad_mine, owned_w2, owned_w1, owned_wo)
    )
    owned = to_owners(grad_mine)
    grad_w2, grad_w1, grad_wo = (sum_owned(o, ring, me) for o in (owned_w2, owned_w1, owned_wo))
    grad_qkv = gather_seq(owned, ring, me).astype(F32)
    grad_qkv = jnp.concatenate(
        [grad_qkv[r, :, i * local : (i + 1) * local] for i in range(3) for r in range(ring)], axis=1
    )

    bias_sum = jnp.sum(dqkv.astype(F32), axis=0)
    zeros = jnp.zeros((width,), F32)
    first = jnp.stack(
        [
            gain_sum,
            shift_sum,
            lax.dynamic_update_slice_in_dim(zeros, bias_sum[:local], me * local, 0),
            lax.dynamic_update_slice_in_dim(zeros, bias_sum[2 * local :], me * local, 0),
        ]
    )
    second = jnp.stack(
        [
            jnp.sum(dh2 * n2, axis=0),
            jnp.sum(dh2, axis=0),
            jnp.sum(dy_f, axis=0),
            jnp.sum(da.astype(F32), axis=0),
        ]
    )
    c1_sum = jnp.sum(dz.astype(F32), axis=0).reshape(devices, -1, own).transpose(1, 0, 2)
    second = jnp.concatenate([second, c1_sum.reshape(-1, width)])
    four = sum_vectors(second, devices, ring)
    grad_c1 = four[4:].reshape(-1)
    late = sum_vectors(first, devices, ring)

    terms = jnp.concatenate(own_terms, axis=0)
    n1, r1 = normalize(inputs)
    grad_inputs = (grad_middle + normalize_back(terms, n1, r1, g1)).reshape(clips, rows, width)
    return (
        layer_out,
        grad_inputs,
        late[0],
        late[1],
        grad_qkv,
        late[2],
        late[3],
        grad_wo,
        four[3],
        four[0],
        four[1],
        grad_w1,
        grad_c1,
        grad_w2,
        four[2],
    )


def twin(value, devices):
    return lax.ppermute(value, "fsdp", [(i, i ^ 1) for i in range(devices)])


def columns(vectors):
    vectors = jnp.pad(vectors.astype(BF16), ((0, -vectors.shape[0] % 128), (0, 0)))
    return dot(jnp.eye(vectors.shape[1], dtype=BF16), vectors, NT).astype(BF16)


def as_rows(block, count):
    return dot(block, jnp.eye(block.shape[0], dtype=BF16), TN)[:count]


def plus(a, b):
    return (a.astype(F32) + b.astype(F32)).astype(BF16)


def plus_rows(a, b, more, row):
    total = a.astype(F32) + b.astype(F32)
    pad = [(row, a.shape[0] - row - more.shape[0])] + [(0, 0)] * (a.ndim - 1)
    return (total + jnp.pad(more.astype(F32), pad)).astype(BF16)


def stage(*values):
    return lax.optimization_barrier(values)


def placed(parts, me):
    out = jnp.zeros((len(parts),) + parts[0].shape, parts[0].dtype)
    for r, part in enumerate(parts):
        out = lax.dynamic_update_index_in_dim(out, part, me ^ r, 0)
    return out


def shards(
    ring,
    devices,
    tokens,
    lengths,
    ln1_gain,
    ln1_bias,
    w_qkv,
    q_bias,
    v_bias,
    w_out,
    b_out,
    ln2_gain,
    ln2_bias,
    w_fc1,
    b_fc1,
    w_fc2,
    b_fc2,
    cotangent,
):
    clips, rows, width = tokens.shape
    total_rows, clip_rows, local = clips * rows, rows * ring, width // ring
    own, half, cut = ln1_gain.shape[0], clips // 2, devices // 4
    me, core = lax.axis_index("seq"), lax.axis_index("fsdp") % 2
    same_core = [list(range(p, devices, 2)) for p in range(2)]

    def over(value, r):
        return swap(value, ring, r)

    vectors = jnp.concatenate(
        [
            jnp.stack([ln1_gain, ln1_bias, q_bias, v_bias, b_out, ln2_gain, ln2_bias, b_fc2]),
            b_fc1.reshape(-1, own),
        ]
    )
    count = vectors.shape[0]
    mine = lax.dynamic_index_in_dim(w_qkv.reshape(own, 3, ring, local), me, 2, keepdims=False)
    mine = jnp.concatenate([mine.reshape(own, 3 * local), columns(vectors)], axis=1)
    mine = lax.all_gather(mine, "fsdp", axis=0, tiled=True)
    part1 = lax.dynamic_index_in_dim(w_fc1.reshape(own, devices, ring, own), me, 2)
    part2 = lax.dynamic_index_in_dim(w_fc2.reshape(ring, own, width), me, 0)
    quarter = jnp.concatenate([part1.reshape(1, own, width), part2], axis=0)
    quarter = lax.all_gather(quarter, "fsdp", axis=0, axis_index_groups=same_core)
    wo = lax.all_gather(w_out, "fsdp", axis=0, tiled=True)

    middle_row = rows // 16 * 8
    one, two = stage(over(tokens[0], 1), over(tokens[0], 2))
    far = [over(two[:middle_row], 1), over(one[middle_row:], 2)]
    mine, *far = stage(mine, *far)
    vectors = as_rows(mine[:, 3 * local :], count)
    g1, b1, qb, vb, bo, g2, b2, c2 = (vectors[i] for i in range(8))
    c1_rows = vectors[8:]
    qb_mine = lax.dynamic_slice_in_dim(qb, me * local, local)
    vb_mine = lax.dynamic_slice_in_dim(vb, me * local, local)
    bias_mine = jnp.concatenate([qb_mine, jnp.zeros_like(qb_mine), vb_mine])

    normed, qkv, outs, logs = ([None] * clips for _ in range(4))

    def project(c, groups):
        normed[c], qkv[c] = norm_project(me, groups, g1, b1, mine, bias_mine)

    def to_rows(out):
        return lax.all_to_all(
            out.reshape(ring, rows, local), "seq", split_axis=0, concat_axis=0, tiled=True
        )

    def length(c):
        return lax.dynamic_slice_in_dim(lengths, c, 1)

    project(0, [[(tokens, 0)], [one], [two], far])
    outs[0], logs[0] = attend(qkv[0], length(0))
    others = [over(tokens[1:], r) for r in range(1, ring)]
    outs[0], *others = stage(outs[0], *others)
    moved = []
    for c in range(1, clips):
        moved.append(to_rows(outs[c - 1]))
        project(c, [[(tokens, c)]] + [[(t, c - 1)] for t in others])
        if c == 1:
            qkv[c], quarter, moved[0] = stage(qkv[c], quarter, moved[0])
            ends_of = [quarter[:cut], quarter[cut:]]
            low1, top2 = over(ends_of[1], 1), over(ends_of[0], 2)
            twin0 = twin(quarter, devices)
        outs[c], logs[c] = attend(qkv[c], length(c))
        if c == 1:
            outs[c], low1, top2, twin0 = stage(outs[c], low1, top2, twin0)
    moved.append(to_rows(outs[-1]))
    moved, low1, top2, ends_of = lax.optimization_barrier((moved, low1, top2, ends_of))
    top1, low2 = over(ends_of[0], 1), over(ends_of[1], 2)
    attended, middle, h2, h2t = project_norm(moved, tokens, wo, bo, g2, b2)
    dy = cotangent.reshape(total_rows, width)

    sums = [None] * ring

    def quarter_of(r, mine_r, twin_r, acc):
        shift = lax.dynamic_index_in_dim(c1_rows, me ^ r, 0)
        y, dh2, keep, send, sums[r] = mlp_piece(
            core[None], h2, h2t, dy, mine_r, twin_r, shift, acc
        )
        return (y, dh2), keep, send

    early = [twin(low1, devices), twin(top2, devices)]
    acc, keep0, send0 = quarter_of(0, [quarter], [twin0], None)
    acc, keep0, send0, early, top1, low2 = lax.optimization_barrier(
        (acc, keep0, send0, early, top1, low2)
    )
    far = [over(top2, 1), over(low1, 2)]
    got0, later2 = twin(send0, devices), twin(low2, devices)
    (later1,) = stage(twin(top1, devices))
    acc, keep1, send1 = quarter_of(1, [top1, low1], [later1, early[0]], acc)
    acc, keep1, send1, far, later2, got0 = lax.optimization_barrier(
        (acc, keep1, send1, far, later2, got0)
    )
    twin_far, got1 = [twin(f, devices) for f in far], twin(send1, devices)
    acc, keep2, send2 = quarter_of(2, [top2, low2], [early[1], later2], acc)
    acc, keep2, send2, twin_far, got1 = lax.optimization_barrier(
        (acc, keep2, send2, twin_far, got1)
    )
    got2 = twin(send2, devices)
    acc, keep3, send3 = quarter_of(3, far, twin_far, acc)
    (y, dh2), keep3, send3, got2 = lax.optimization_barrier((acc, keep3, send3, got2))
    (got3,) = stage(twin(send3, devices))
    term3 = plus(keep3, got3)
    ends = [over(term3[:cut], 1), over(term3[cut:], 2)]

    c1_sum = placed([v[0] for v in sums], me)
    def to_heads(part):
        part = lax.all_to_all(part, "seq", split_axis=0, concat_axis=0, tiled=True)
        return part.reshape(1, clip_rows, local)

    layer_out = grad_middle = None
    das, heads, column_sums = ([None] * clips for _ in range(3))
    for c in range(clips):
        layer_out, grad_middle, das[c], heads[c], column_sums[c] = project_back(
            c, y, dh2, middle, dy, wo, g2, c2, tokens.shape, ring, layer_out, grad_middle
        )
        if c == 0:
            moved = to_heads(heads[0])
    term_wo = project_weight(das, attended, column_sums, c1_sum)
    moved, term_wo, end2, end1 = stage(moved, term_wo, *ends)
    owned_wo = to_owners(term_wo)

    second = [
        over(add_terms([(keep1, None), (got1, None), (end1, cut)]), 1),
        over(add_terms([(keep2, None), (got2, None), (end2, 0)]), 2),
    ]
    acc, flying, token_terms = None, [], [None] * clips

    def exchange(parts):
        return lax.all_to_all(parts, "seq", 0, 0, tiled=True)

    def to_all(part):
        return exchange(jnp.broadcast_to(part[None], (ring,) + part.shape))

    for c in range(clips):
        later = [to_heads(heads[c + 1])] if c + 1 < clips else []
        if c == clips - 1:
            owned_wo = owned_wo.reshape(ring, own // ring, width + 128)
            later = [lax.dynamic_index_in_dim(owned_wo, me ^ r, 0, False) for r in range(ring)]
            later = [over(t, r) if r else t for r, t in enumerate(later)]
        d = attend_back(qkv[c], moved, outs[c], logs[c], length(c))
        if c < clips - 1:
            acc = qkv_weight(me, d[0], normed[c], mine, acc, ring, False)
        d, later, flying, second, acc = lax.optimization_barrier((d, later, flying, second, acc))
        moved, wo_terms = later[0], later
        if c:
            token_terms[c - 1] = flying[0]
        else:
            total = add_terms([(t, None) for t in (keep0, got0, *second)])
            owned_mlp = lax.psum_scatter(
                total,
                "fsdp",
                scatter_dimension=0,
                tiled=True,
                axis_index_groups=same_core,
            )[0]
            second = []
        last = c == clips - 1
        if c < clips - 1:
            flying = [exchange(qkv_back(d[0], mine, ring))]

    d, owned_mlp = stage(d, owned_mlp)
    shared = [over(owned_mlp, 1), over(owned_mlp, 2)]
    grad_mine, kept, one, two, top, low = qkv_weight(
        me, d[0], normed[-1], mine, acc, ring, True
    )
    one, two, top, low, shared, grad_mine = lax.optimization_barrier(
        (one, two, top, low, shared, grad_mine)
    )
    owned = to_owners(grad_mine)

    cross = [over(top, 1), over(low, 2)]
    grad_inputs = None
    for c in range(clips - 1):
        terms = [(token_terms[c], ring)]
        grad_inputs = tokens_back(c, terms, tokens, grad_middle, g1, grad_inputs)
    grad_inputs, cross = lax.optimization_barrier((grad_inputs, cross))
    flying = [
        over(jnp.concatenate([one[:, :middle_row], plus(one[:, middle_row:], cross[1][None])], 1), 1),
        over(jnp.concatenate([plus(two[:, :middle_row], cross[0][None]), two[:, middle_row:]], 1), 2),
    ]
    wo_term = sum(t.astype(F32) for t in wo_terms).astype(BF16)
    wo_parts = to_all(wo_term)
    flying, wo_parts = lax.optimization_barrier((flying, wo_parts))
    owned, flying, shared = lax.optimization_barrier((owned, flying, shared))
    far = [over(shared[1][:1], 1), over(shared[0][1:], 2)]
    grad_w1, grad_w2 = spread_mlp(me, [owned_mlp, *shared, *far], ring)
    owned = [over(owned, r) if r else owned for r in range(ring)]
    terms = [(kept, 1)] + [(f, 1) for f in flying]
    grad_inputs = tokens_back(clips - 1, terms, tokens, grad_middle, g1, grad_inputs)
    grad_wo, grad_qkv, sums = spread_attn(me, wo_parts, owned)
    middle_sums, last_sums = sums[0], sums[1]
    return (
        layer_out,
        grad_inputs,
        last_sums[0],
        last_sums[1],
        grad_qkv,
        last_sums[2],
        last_sums[3],
        grad_wo,
        middle_sums[3],
        middle_sums[0],
        middle_sums[1],
        grad_w1,
        middle_sums[4 : count - 4].reshape(-1),
        grad_w2,
        middle_sums[2],
    )


def solution(mesh):
    act, vec, mat = P("fsdp", "seq", None), P("fsdp"), P("fsdp", None)
    in_specs = (act, vec, vec, vec, mat, vec, vec, mat, vec, vec, vec, mat, vec, mat, vec, act)
    out_specs = (act, act, vec, vec, mat, vec, vec, mat, vec, vec, vec, mat, vec, mat, vec)
    ring, devices = mesh.shape["seq"], mesh.shape["fsdp"]

    def layer(*args):
        clips, rows, width = args[0].shape
        square = ring == 4 and args[11].shape[1] == ring * width and devices % 4 == 0
        square = square and clips % (2 * devices) == 0 and width % (128 * devices) == 0
        return jax.shard_map(
            functools.partial(shards if square else shards_any, ring, devices),
            mesh=mesh,
            in_specs=in_specs,
            out_specs=out_specs,
            check_vma=False,
        )(*args)

    return layer
```

```python
import functools

import jax
import jax.numpy as jnp
from jax import lax
from jax.experimental import pallas as pl
from jax.experimental.pallas import tpu as pltpu
from jax.sharding import PartitionSpec as P

HEAD_DIM = 64
PAIR = 2 * HEAD_DIM
EPSILON = 1e-06
NEGATIVE = -1e30
F32, BF16 = jnp.float32, jnp.bfloat16
SCALE = HEAD_DIM ** -0.5
SCALE2 = SCALE * 1.4426950408889634
NT = (((1,), (1,)), ((), ()))
NN = (((1,), (0,)), ((), ()))
TN = (((0,), (0,)), ((), ()))


def dot(a, b, dims=NN):
    return lax.dot_general(a, b, dims, preferred_element_type=F32)


LARGE = 56 << 20
WHOLE = pl.BlockSpec(memory_space=pltpu.VMEM)
SCALAR = pl.BlockSpec(memory_space=pltpu.SMEM)


def kernel_call(body, name, operands, outs, scratch=(), scalars=0, aliases=None, vmem=40):
    return pl.pallas_call(
        body,
        in_specs=[SCALAR] * scalars + [WHOLE] * (len(operands) - scalars),
        out_specs=[WHOLE] * len(outs),
        out_shape=[jax.ShapeDtypeStruct(*out) for out in outs],
        scratch_shapes=list(scratch),
        input_output_aliases=aliases or {},
        compiler_params=pltpu.CompilerParams(vmem_limit_bytes=vmem << 20),
        cost_estimate=pl.CostEstimate(flops=1 << 20, bytes_accessed=1 << 20, transcendentals=0),
        name=name,
    )(*operands)


def of_head(block, h):
    lane = lax.broadcasted_iota(jnp.int32, (1, PAIR), 1)
    return jnp.where(lane // HEAD_DIM == h, block, jnp.zeros_like(block))


def valid_rows(j, bk, length):
    return j * bk + lax.broadcasted_iota(jnp.int32, (bk, 1), 0) < length


def transposed_chunks(out_ref, in_ref, cols, bk):
    for j in range(in_ref.shape[1] // bk):
        out_ref[j] = jnp.transpose(in_ref[0, pl.ds(j * bk, bk), cols])


def attend_kernel(len_ref, q_ref, k_ref, v_ref, o_ref, lse_ref, s_ref, vt_ref, ot_ref, *, bk):
    length = len_ref[pl.program_id(0)]
    rows_all, width = q_ref.shape[1:]
    chunks = pl.cdiv(length, bk)
    for pair in range(width // PAIR):
        cols = pl.ds(PAIR * pair, PAIR)
        transposed_chunks(vt_ref, v_ref, cols, bk)
        queries = [of_head(q_ref[0, :, cols], h) for h in range(2)]

        def score(j, tops):
            keys = k_ref[0, pl.ds(pl.multiple_of(j * bk, bk), bk), cols]
            ok = valid_rows(j, bk, length)
            out = []
            for h in range(2):
                s = jnp.where(ok, dot(keys, queries[h], NT), NEGATIVE)
                s_ref[h, j] = s
                top = tops[h]
                for i in range(bk // 8):
                    top = jnp.maximum(top, s[8 * i : 8 * i + 8])
                out.append(top)
            return tuple(out)

        low = jnp.full((8, rows_all), NEGATIVE, F32)
        tops = lax.fori_loop(0, chunks, score, (low, low))
        peaks = [jnp.max(top, axis=0, keepdims=True) * SCALE2 for top in tops]
        ot_ref[...] = jnp.zeros_like(ot_ref)

        def mix(j, sums):
            out = []
            for h in range(2):
                p = jnp.exp2(s_ref[h, j] * SCALE2 - peaks[h])
                total = sums[h]
                for i in range(bk // 8):
                    total = total + p[8 * i : 8 * i + 8]
                out.append(total)
                half = pl.ds(HEAD_DIM * h, HEAD_DIM)
                ot_ref[half] += dot(vt_ref[j, half], p.astype(BF16))
            return tuple(out)

        zero = jnp.zeros((8, rows_all), F32)
        sums = lax.fori_loop(0, chunks, mix, (zero, zero))
        for h in range(2):
            total = jnp.sum(sums[h], axis=0, keepdims=True)
            half = pl.ds(HEAD_DIM * h, HEAD_DIM)
            lse_ref[0, pl.ds(2 * pair + h, 1)] = peaks[h] + jnp.log2(total)
            ot_ref[half] = ot_ref[half] / total
        o_ref[0, :, cols] = jnp.transpose(ot_ref[...]).astype(BF16)


def attend_back_kernel(
    len_ref, q_ref, k_ref, v_ref, do_ref, o_ref, lse_ref, d_ref, kt_ref, dqt_ref, *, bk
):
    length = len_ref[pl.program_id(0)]
    width = q_ref.shape[2]
    chunks = pl.cdiv(length, bk)
    d_ref[...] = jnp.zeros_like(d_ref)
    for pair in range(width // PAIR):
        cols = pl.ds(PAIR * pair, PAIR)
        outs = do_ref[0, :, cols]
        both = jnp.transpose(outs.astype(F32) * o_ref[0, :, cols].astype(F32))
        inner = [
            jnp.sum(both[HEAD_DIM * h : HEAD_DIM * (h + 1)], axis=0, keepdims=True)
            for h in range(2)
        ]
        queries = [of_head(q_ref[0, :, cols], h) for h in range(2)]
        grads = [of_head(outs, h) for h in range(2)]
        logs = [lse_ref[0, pl.ds(2 * pair + h, 1)] for h in range(2)]
        transposed_chunks(kt_ref, k_ref, cols, bk)
        dqt_ref[...] = jnp.zeros_like(dqt_ref)

        def step(j, carry):
            rows = pl.ds(pl.multiple_of(j * bk, bk), bk)
            keys = k_ref[0, rows, cols]
            values = v_ref[0, rows, cols]
            ok = valid_rows(j, bk, length)
            dk = jnp.zeros((bk, PAIR), F32)
            dv = jnp.zeros((bk, PAIR), F32)
            for h in range(2):
                p = jnp.exp2(dot(keys, queries[h], NT) * SCALE2 - logs[h])
                p = jnp.where(ok, p, 0.0)
                g = (p * (dot(values, grads[h], NT) - inner[h])).astype(BF16)
                dv = dv + dot(p.astype(BF16), grads[h])
                dk = dk + dot(g, queries[h])
                half = pl.ds(HEAD_DIM * h, HEAD_DIM)
                dqt_ref[half] += dot(kt_ref[j, half], g)
            d_ref[0, rows, pl.ds(width + PAIR * pair, PAIR)] = (dk * SCALE).astype(BF16)
            d_ref[0, rows, pl.ds(2 * width + PAIR * pair, PAIR)] = dv.astype(BF16)
            return carry

        lax.fori_loop(0, chunks, step, 0)
        d_ref[0, :, cols] = jnp.transpose(dqt_ref[...] * SCALE).astype(BF16)


def chunk_rows(rows):
    return max(b for b in range(8, 225, 8) if rows % b == 0)


def block(rows, width, at):
    return pl.BlockSpec((1, rows, width), lambda c, n: (c, 0, at))


def attend(qkv, lengths):
    clips, rows, triple = qkv.shape
    width = triple // 3
    heads, bk = width // HEAD_DIM, chunk_rows(rows)
    cost = clips * heads * rows * rows
    return pl.pallas_call(
        functools.partial(attend_kernel, bk=bk),
        grid_spec=pltpu.PrefetchScalarGridSpec(
            num_scalar_prefetch=1,
            grid=(clips,),
            in_specs=[block(rows, width, i) for i in range(3)],
            out_specs=[block(rows, width, 0), block(heads, rows, 0)],
            scratch_shapes=[
                pltpu.VMEM((2, rows // bk, bk, rows), F32),
                pltpu.VMEM((rows // bk, PAIR, bk), BF16),
                pltpu.VMEM((PAIR, rows), F32),
            ],
        ),
        out_shape=[
            jax.ShapeDtypeStruct((clips, rows, width), BF16),
            jax.ShapeDtypeStruct((clips, heads, rows), F32),
        ],
        compiler_params=pltpu.CompilerParams(vmem_limit_bytes=LARGE),
        cost_estimate=pl.CostEstimate(
            flops=1 << 20, bytes_accessed=1 << 20, transcendentals=0
        ),
        name="attend",
    )(lengths, qkv, qkv, qkv)


def attend_back(qkv, grads, outs, logs, lengths):
    clips, rows, triple = qkv.shape
    width = triple // 3
    heads, bk = width // HEAD_DIM, chunk_rows(rows)
    cost = clips * heads * rows * rows
    return pl.pallas_call(
        functools.partial(attend_back_kernel, bk=bk),
        grid_spec=pltpu.PrefetchScalarGridSpec(
            num_scalar_prefetch=1,
            grid=(clips,),
            in_specs=[block(rows, width, i) for i in (0, 1, 2, 0, 0)] + [block(heads, rows, 0)],
            out_specs=block(rows, triple, 0),
            scratch_shapes=[
                pltpu.VMEM((rows // bk, PAIR, bk), BF16),
                pltpu.VMEM((PAIR, rows), F32),
            ],
        ),
        out_shape=jax.ShapeDtypeStruct((clips, rows, triple), BF16),
        compiler_params=pltpu.CompilerParams(vmem_limit_bytes=LARGE),
        cost_estimate=pl.CostEstimate(
            flops=1 << 20, bytes_accessed=1 << 20, transcendentals=0
        ),
        name="attend_back",
    )(lengths, qkv, qkv, qkv, grads, outs, logs)


def norm_kernel(me_ref, *refs, counts):
    parts, rest = refs[: sum(counts)], refs[sum(counts) :]
    g_ref, b_ref, w_ref, bias_ref, h_ref, qkv_ref, x_ref = rest
    taken = 0
    for r, count in enumerate(counts):
        group = parts[taken : taken + count]
        taken += count

        @pl.when(pl.program_id(0) == r)
        def _():
            row = 0
            for ref in group:
                x_ref[pl.ds(row, ref.shape[0])] = ref[...]
                row += ref.shape[0]

    normed, _ = normalize(x_ref[...].astype(F32))
    h = (normed * g_ref[...] + b_ref[...]).astype(BF16)
    h_ref[0] = h
    qkv_ref[0] = (dot(h, w_ref[...]) + bias_ref[...]).astype(BF16)


def norm_project(me, groups, gain, shift, weight, bias):
    flat = [part if isinstance(part, tuple) else (part, None) for g in groups for part in g]
    triple, ring = bias.shape[-1], len(groups)
    rows, width = flat[0][0].shape[-2:]

    def part_spec(array, clip):
        if clip is None:
            return pl.BlockSpec(array.shape, lambda r, m: (0, 0))
        return pl.BlockSpec((None, rows, width), lambda r, m: (clip, 0, 0))

    def out(cols):
        return pl.BlockSpec((1, rows, cols), lambda r, m: (m[0] ^ r, 0, 0))

    h, qkv = pl.pallas_call(
        functools.partial(norm_kernel, counts=[len(g) for g in groups]),
        grid_spec=pltpu.PrefetchScalarGridSpec(
            num_scalar_prefetch=1,
            grid=(ring,),
            in_specs=[part_spec(*part) for part in flat]
            + [WHOLE] * 2
            + [pl.BlockSpec((width, triple), lambda r, m: (0, 0)), WHOLE],
            out_specs=[out(width), out(triple)],
            scratch_shapes=[pltpu.VMEM((rows, width), BF16)],
        ),
        out_shape=[jax.ShapeDtypeStruct((ring, rows, c), BF16) for c in (width, triple)],
        compiler_params=pltpu.CompilerParams(vmem_limit_bytes=LARGE),
        cost_estimate=pl.CostEstimate(flops=1 << 20, bytes_accessed=1 << 20, transcendentals=0),
        name="norm_project",
    )(me[None], *[part[0] for part in flat], gain[None], shift[None], weight, bias[None])
    return h.reshape(ring * rows, width), qkv.reshape(1, ring * rows, triple)


def mlp_piece_kernel(core_ref, h_ref, ht_ref, dy_ref, *refs, first, nz, counts):
    mines, others, refs = refs[: counts[0]], refs[counts[0] : sum(counts)], refs[sum(counts) :]
    c1_ref, *refs = refs
    yin_ref, dhin_ref = (None, None) if first else (refs.pop(0), refs.pop(0))
    y_ref, dh_ref, keep_ref, send_ref, sums_ref, hm_ref, hmt_ref, w1_ref, w2_ref, u_ref, dz_ref = refs
    core = core_ref[0]
    width = h_ref.shape[1]
    clips, _, share = ht_ref.shape
    rows = mines[0].shape[2]
    half = nz * rows

    def at(i, p):
        block = 2 * i + (core if p == 0 else 1 - core)
        return pl.ds(pl.multiple_of(block * rows, rows), rows)

    def put(i, p):
        return pl.ds(p * half + i * rows, rows)

    def source(i, p):
        parts = (mines, others)[p]
        size = nz // len(parts)
        return parts[i // size], i % size

    for i in range(nz):
        for p in range(2):
            hm_ref[:, put(i, p)] = h_ref[:, at(i, p)]
            for c in range(clips):
                hmt_ref[c, put(i, p), :] = ht_ref[c, at(i, p), :]
            src, z = source(i, p)
            w2_ref[pl.ds((2 * i + p) * rows, rows), :] = src[z, 1]
            for j in range(nz):
                for r in range(2):
                    w1_ref[put(i, p), pl.ds((2 * j + r) * rows, rows)] = src[z, 0, :, at(j, r)]
    for i in range(nz):
        cols = pl.ds(2 * i * rows, 2 * rows)
        bias = jnp.concatenate([c1_ref[:, at(i, p)] for p in range(2)], axis=1)
        z = dot(hm_ref[...], w1_ref[:, cols]) + bias
        phi = 0.5 * (1.0 + lax.erf(z * (2.0 ** -0.5)))
        u_ref[:, cols] = (z * phi).astype(BF16)
        slope = phi + z * (jnp.exp(z * z * -0.5) * 0.3989422804014327)
        dz = (dot(dy_ref[...], w2_ref[cols, :], NT) * slope).astype(BF16)
        dz_ref[:, cols] = dz
        total = jnp.sum(dz.astype(F32), axis=0, keepdims=True)
        for p in range(2):
            sums_ref[:, at(i, p)] = total[:, p * rows : (p + 1) * rows]
        g2 = dot(u_ref[:, cols], dy_ref[...], TN).astype(BF16)
        keep_ref[i, 1] = g2[:rows]
        send_ref[i, 1] = g2[rows:]
        g1 = sum(dot(hmt_ref[c], dz_ref[pl.ds(c * share, share), cols]) for c in range(clips))
        g1 = g1.astype(BF16)
        for p in range(2):
            part = g1[:, p * rows : (p + 1) * rows]
            keep_ref[:, 0, :, at(i, p)] = part[:half].reshape(nz, rows, rows)
            send_ref[:, 0, :, at(i, p)] = part[half:].reshape(nz, rows, rows)
    for n in range(width // 256):
        cols = pl.ds(256 * n, 256)
        y = dot(u_ref[...], w2_ref[:, cols])
        y_ref[:, cols] = y if first else y + yin_ref[:, cols]
    for n in range(width // 256):
        d = dot(dz_ref[...], w1_ref[pl.ds(256 * n, 256), :], NT)
        for q in range(256 // rows):
            p, i = divmod((256 // rows) * n + q, nz)
            v = d[:, q * rows : (q + 1) * rows]
            dh_ref[:, at(i, p)] = v if first else v + dhin_ref[:, at(i, p)]


def mlp_piece(core, h2, h2t, dy, mine, other, c1, acc):
    rows = mine[0].shape[2]
    t, width = h2.shape
    nz = width // (2 * rows)
    first = acc is None
    ins = [core, h2, h2t, dy, *mine, *other, c1] + ([] if first else list(acc))
    gradient = ((nz, 2, rows, width), BF16)
    return kernel_call(
        functools.partial(
            mlp_piece_kernel, first=first, nz=nz, counts=(len(mine), len(other))
        ),
        "mlp_piece",
        ins,
        [((t, width), F32), ((t, width), F32), gradient, gradient, (c1.shape, F32)],
        scratch=[pltpu.VMEM((t, width), BF16), pltpu.VMEM(h2t.shape, BF16)]
        + [pltpu.VMEM((width, width), BF16)] * 2
        + [pltpu.VMEM((t, width), BF16)] * 2,
        scalars=1,
        aliases={} if first else {len(ins) - 2: 0, len(ins) - 1: 1},
        vmem=24,
    )


def project_kernel(*refs, clips):
    moved, rest = refs[:clips], refs[clips:]
    x_ref, wo_ref, bo_ref, g_ref, b_ref, att_ref, mid_ref, h_ref, ht_ref = rest
    ring, rows, local = moved[0].shape
    for c in range(clips):
        at = pl.ds(c * rows, rows)
        for s in range(ring):
            att_ref[at, pl.ds(s * local, local)] = moved[c][s]
        middle = x_ref[c].astype(F32) + (dot(att_ref[at, :], wo_ref[...]) + bo_ref[...])
        mid_ref[at, :] = middle
        h = (normalize(middle)[0] * g_ref[...] + b_ref[...]).astype(BF16)
        h_ref[at, :] = h
        ht_ref[c] = jnp.transpose(h)


def project_norm(moved, tokens, wo, bo, gain, shift):
    clips, rows, width = tokens.shape
    flat = (clips * rows, width)
    return kernel_call(
        functools.partial(project_kernel, clips=clips),
        "project_norm",
        [*moved, tokens, wo, bo[None], gain[None], shift[None]],
        [(flat, BF16), (flat, F32), (flat, BF16), ((clips, width, rows), BF16)],
        vmem=20,
    )


def project_back_kernel(*refs, clip, first):
    y_ref, dh_ref, mid_ref, dy_ref, wo_ref, g_ref, c2_ref = refs[:7]
    out_ref, gm_ref, da_ref, do_ref, sum_ref = refs[-5:]
    ring, rows, local = do_ref.shape
    middle = mid_ref[...]
    out_ref[0] = (middle + (y_ref[...] + c2_ref[...])).astype(BF16)
    normed, rstd = normalize(middle)
    dh = dh_ref[...]
    dy = dy_ref[...].astype(F32)
    grad = dy + normalize_back(dh, normed, rstd, g_ref[...])
    gm_ref[0] = grad
    da = grad.astype(BF16)
    da_ref[...] = da
    do = dot(da, wo_ref[...], NT).astype(BF16)
    for s in range(ring):
        do_ref[s] = do[:, s * local : (s + 1) * local]
    sum_ref[...] = jnp.zeros_like(sum_ref)
    for i, terms in enumerate((dh * normed, dh, dy, da.astype(F32))):
        sum_ref[pl.ds(i, 1), :] = jnp.sum(terms, axis=0, keepdims=True)


def project_back(c, y, dh, middle, dy, wo, gain, c2, shape, ring, out, grad):
    clips, rows, width = shape
    at = pl.BlockSpec((rows, width), lambda i: (c, 0))
    at_c = pl.BlockSpec((1, rows, width), lambda i: (c, 0, 0))
    one = pl.BlockSpec((1, width), lambda i: (0, 0))
    back = [] if out is None else [out, grad]
    return pl.pallas_call(
        functools.partial(project_back_kernel, clip=c, first=out is None),
        grid=(1,),
        in_specs=[at] * 4
        + [pl.BlockSpec((width, width), lambda i: (0, 0)), one, one]
        + [pl.BlockSpec(memory_space=pl.ANY)] * len(back),
        out_specs=[
            at_c,
            at_c,
            pl.BlockSpec((rows, width), lambda i: (0, 0)),
            pl.BlockSpec((ring, rows, width // ring), lambda i: (0, 0, 0)),
            pl.BlockSpec((8, width), lambda i: (0, 0)),
        ],
        out_shape=[
            jax.ShapeDtypeStruct(shape, BF16),
            jax.ShapeDtypeStruct(shape, F32),
            jax.ShapeDtypeStruct((rows, width), BF16),
            jax.ShapeDtypeStruct((ring, rows, width // ring), BF16),
            jax.ShapeDtypeStruct((8, width), F32),
        ],
        input_output_aliases={7: 0, 8: 1} if back else {},
        compiler_params=pltpu.CompilerParams(vmem_limit_bytes=LARGE),
        cost_estimate=pl.CostEstimate(flops=1 << 20, bytes_accessed=1 << 20, transcendentals=0),
        name="project_back",
    )(y, dh, middle, dy, wo, gain[None], c2[None], *back)


def project_weight_kernel(*refs, clips):
    das, att_ref, sums = refs[:clips], refs[clips], refs[clips + 1 : 2 * clips + 1]
    c1_ref, gw_ref, sum_ref = refs[2 * clips + 1 :]
    rows, width = das[0].shape
    term = dot(att_ref[pl.ds(0, rows), :], das[0][...], TN)
    total = sums[0][...]
    for c in range(1, clips):
        term = term + dot(att_ref[pl.ds(c * rows, rows), :], das[c][...], TN)
        total = total + sums[c][...]
    sum_ref[...] = jnp.zeros_like(sum_ref)
    sum_ref[pl.ds(0, 8), :] = total
    sum_ref[pl.ds(4, c1_ref.shape[0]), :] = c1_ref[...]
    gw_ref[:, pl.ds(0, width)] = term.astype(BF16)
    gw_ref[:, pl.ds(width, 128)] = jnp.transpose(sum_ref[...]).astype(BF16)


def project_weight(das, attended, sums, c1_sum):
    width = attended.shape[1]
    return kernel_call(
        functools.partial(project_weight_kernel, clips=len(das)),
        "project_weight",
        [*das, attended, *sums, c1_sum],
        [((width, width + 128), BF16)],
        scratch=[pltpu.VMEM((128, width), F32)],
        vmem=56,
    )[0]


def qkv_back_kernel(d_ref, w_ref, part_ref):
    part_ref[0] = dot(d_ref[...], w_ref[...], NT).astype(BF16)


def qkv_back(d, weight, ring):
    whole, triple = d.shape
    width, rows = weight.shape[0], whole // ring
    return pl.pallas_call(
        qkv_back_kernel,
        grid=(ring,),
        in_specs=[
            pl.BlockSpec((rows, triple), lambda r: (r, 0)),
            pl.BlockSpec((width, triple), lambda r: (0, 0)),
        ],
        out_specs=pl.BlockSpec((1, rows, width), lambda r: (r, 0, 0)),
        out_shape=jax.ShapeDtypeStruct((ring, rows, width), BF16),
        compiler_params=pltpu.CompilerParams(vmem_limit_bytes=LARGE),
        cost_estimate=pl.CostEstimate(flops=1 << 20, bytes_accessed=1 << 20, transcendentals=0),
        name="qkv_back",
    )(d, weight)


def qkv_weight_kernel(me_ref, d_ref, h_ref, w_ref, *rest, first, last):
    rest = list(rest)
    acc_ref, bias_ref = (None, None) if first else (rest.pop(0), rest.pop(0))
    triple = d_ref.shape[1]
    local = triple // 3
    term = dot(h_ref[...], d_ref[...], TN)
    bias = jnp.sum(d_ref[...].astype(F32), axis=0, keepdims=True)
    if not first:
        term = term + acc_ref[...]
        bias = bias + bias_ref[pl.ds(0, 1), :]
    if not last:
        out_ref, sum_ref = rest
        out_ref[...] = term
        sum_ref[...] = jnp.broadcast_to(bias, sum_ref.shape)
        return
    out_ref, own_ref, one_ref, two_ref, top_ref, low_ref, row_ref = rest
    rows, cut = own_ref.shape[1], top_ref.shape[0]
    for r in (3, 1, 2, 0):
        at = pl.ds(pl.multiple_of((me_ref[0] ^ r) * rows, 8), rows)
        part = dot(d_ref[at, :], w_ref[:, pl.ds(0, triple)], NT).astype(BF16)
        if r == 3:
            top_ref[...] = part[:cut]
            low_ref[...] = part[cut:]
        else:
            (own_ref, one_ref, two_ref)[r][0] = part
    out_ref[:, pl.ds(0, triple)] = term.astype(BF16)
    weight = w_ref[:, pl.ds(0, triple)].astype(F32)
    vectors = w_ref[:, pl.ds(triple, 128)].astype(F32)
    gain, shift = vectors[:, 0:1], vectors[:, 1:2]
    shift_sum = jnp.sum(weight * bias, axis=1, keepdims=True)
    gain_sum = (jnp.sum(weight * term, axis=1, keepdims=True) - shift * shift_sum) / gain
    row_ref[...] = jnp.zeros_like(row_ref)
    at_me = pl.ds(pl.multiple_of(me_ref[0] * local, local), local)
    row_ref[pl.ds(2, 1), at_me] = bias[:, :local]
    row_ref[pl.ds(3, 1), at_me] = bias[:, 2 * local :]
    lane = lax.broadcasted_iota(jnp.int32, (1, 128), 1)
    sums = jnp.transpose(row_ref[...])
    sums = jnp.where(lane == 0, gain_sum, jnp.where(lane == 1, shift_sum, sums))
    out_ref[:, pl.ds(triple, 128)] = sums.astype(BF16)


def qkv_weight(me, d, h, mine, acc, ring, last):
    (whole, triple), width = d.shape, h.shape[1]
    outs = [((width, triple), F32), ((8, triple), F32)]
    if last:
        rows = whole // ring
        cut = rows // 16 * 8
        outs = [((width, triple + 128), BF16)] + [((1, rows, width), BF16)] * 3
        outs += [((cut, width), BF16), ((rows - cut, width), BF16)]
    return kernel_call(
        functools.partial(qkv_weight_kernel, first=acc is None, last=last),
        "qkv_weight",
        [me[None], d, h, mine] + list(acc or ()),
        outs,
        scratch=[pltpu.VMEM((128, width), F32)] if last else (),
        scalars=1,
        vmem=56,
    )


def tokens_back_kernel(*refs, counts):
    term_refs, (x_ref, gm_ref, g_ref) = refs[: len(counts)], refs[len(counts) : len(counts) + 3]
    out_ref = refs[-1]
    grad = None
    for count, ref in zip(counts, term_refs):
        for r in range(count):
            term = ref[r].astype(F32)
            grad = term if grad is None else grad + term
    normed, rstd = normalize(x_ref[0].astype(F32))
    out_ref[0] = gm_ref[0] + normalize_back(grad, normed, rstd, g_ref[...])


def tokens_back(c, terms, tokens, grad_middle, gain, out):
    clips, rows, width = tokens.shape
    steps = max(n for n in (7, 4, 2, 1) if rows % (8 * n) == 0)
    block = rows // steps
    at_c = pl.BlockSpec((1, block, width), lambda i: (c, i, 0))
    counts = [count for _, count in terms]
    specs = [pl.BlockSpec((n, block, width), lambda i: (0, i, 0)) for n in counts] + [at_c, at_c]
    specs.append(pl.BlockSpec((1, width), lambda i: (0, 0)))
    operands = [*[array for array, _ in terms], tokens, grad_middle, gain[None]]
    if out is not None:
        specs.append(pl.BlockSpec(memory_space=pl.ANY))
        operands.append(out)
    return pl.pallas_call(
        functools.partial(tokens_back_kernel, counts=counts),
        grid=(steps,),
        in_specs=specs,
        out_specs=at_c,
        out_shape=jax.ShapeDtypeStruct((clips, rows, width), F32),
        input_output_aliases={} if out is None else {len(operands) - 1: 0},
        compiler_params=pltpu.CompilerParams(vmem_limit_bytes=LARGE),
        cost_estimate=pl.CostEstimate(flops=1 << 20, bytes_accessed=1 << 20, transcendentals=0),
        name="tokens_back",
    )(*operands)


def add_kernel(*refs, ranges):
    out_ref = refs[-1]
    step = pl.program_id(0)
    total = None
    for (start, stop), ref in zip(ranges, refs):
        term = ref[...].astype(F32)
        if start is not None:
            inside = (step >= start) & (step < stop)
            term = jnp.where(inside, term, 0.0)
        total = term if total is None else total + term
    out_ref[...] = total.astype(BF16)


def add_terms(terms):
    shape = terms[0][0].shape
    block = (1,) + shape[1:]
    rest = (0,) * (len(shape) - 1)

    def spec(count, row):
        if row is None:
            return pl.BlockSpec(block, lambda z: (z, *rest))
        return pl.BlockSpec(block, lambda z: (jnp.clip(z - row, 0, count - 1), *rest))

    return pl.pallas_call(
        functools.partial(
            add_kernel,
            ranges=[(r, None if r is None else r + t.shape[0]) for t, r in terms],
        ),
        grid=shape[:1],
        in_specs=[spec(t.shape[0], row) for t, row in terms],
        out_specs=pl.BlockSpec(block, lambda z: (z, *rest)),
        out_shape=jax.ShapeDtypeStruct(shape, BF16),
        compiler_params=pltpu.CompilerParams(vmem_limit_bytes=24 << 20),
        cost_estimate=pl.CostEstimate(flops=1 << 20, bytes_accessed=1 << 20, transcendentals=0),
        name="add_terms",
    )(*[t for t, _ in terms])


def spread_mlp_kernel(me_ref, own_ref, one_ref, two_ref, far1_ref, far2_ref, w1_ref, w2_ref):
    own = own_ref.shape[1]
    ring = w1_ref.shape[1] // own_ref.shape[2]
    firsts = [own_ref.at[0], one_ref.at[0], two_ref.at[0], far1_ref.at[0]]
    seconds = [own_ref.at[1], one_ref.at[1], two_ref.at[1], far2_ref.at[0]]
    for r in range(ring):
        q = me_ref[0] ^ r
        part = firsts[r][...].astype(F32)
        for f in range(part.shape[1] // own):
            at = pl.ds(pl.multiple_of((f * ring + q) * own, own), own)
            w1_ref[:, at] = part[:, f * own : (f + 1) * own]
        w2_ref[pl.ds(pl.multiple_of(q * own, own), own), :] = seconds[r][...].astype(F32)


def spread_mlp(me, parts, ring):
    _, own, width = parts[0].shape
    return kernel_call(
        spread_mlp_kernel,
        "spread_mlp",
        [me[None], *parts],
        [((own, ring * width), F32), ((ring * own, width), F32)],
        scalars=1,
    )


def spread_attn_kernel(me_ref, *refs, ring):
    wo_ref, qkv_refs = refs[0], refs[1 : ring + 1]
    gwo_ref, gqkv_ref, vec_ref, more_ref = refs[ring + 1 :]
    own, width = gwo_ref.shape
    rows = wo_ref.shape[1]
    triple = qkv_refs[0].shape[1] - 128
    local = triple // 3
    last = jnp.zeros((own, 128), F32)
    for r in range(ring):
        q = me_ref[0] ^ r
        gwo_ref[pl.ds(r * rows, rows), :] = wo_ref[r, :, :width].astype(F32)
        more_ref[pl.ds(r * rows, rows), :] = wo_ref[r, :, width:].astype(F32)
        last = last + qkv_refs[r][:, triple:].astype(F32)
        for i in range(3):
            part = qkv_refs[r][:, i * local : (i + 1) * local].astype(F32)
            gqkv_ref[:, pl.ds(pl.multiple_of(i * width + q * local, local), local)] = part
    vec_ref[0] = jnp.transpose(more_ref[...])
    vec_ref[1] = jnp.transpose(last)


def spread_attn(me, wo_parts, qkv_parts):
    ring, own = len(qkv_parts), qkv_parts[0].shape[0]
    width = wo_parts.shape[2] - 128
    return kernel_call(
        functools.partial(spread_attn_kernel, ring=ring),
        "spread_attn",
        [me[None], wo_parts, *qkv_parts],
        [((own, width), F32), ((own, 3 * width), F32), ((2, 128, own), F32)],
        scratch=[pltpu.VMEM((own, 128), F32)],
        scalars=1,
    )


def swap(value, ring, r):
    return lax.ppermute(value, "seq", [(i, i ^ r) for i in range(ring)])


def gather_seq(value, ring, me):
    out = jnp.zeros((ring,) + value.shape, value.dtype)
    out = lax.dynamic_update_index_in_dim(out, value, me, 0)
    for r in range(1, ring):
        out = lax.dynamic_update_index_in_dim(out, swap(value, ring, r), me ^ r, 0)
    return out


def sum_seq(terms, ring, me):
    total = lax.dynamic_index_in_dim(terms, me, 0, keepdims=False).astype(F32)
    for r in range(1, ring):
        term = lax.dynamic_index_in_dim(terms, me ^ r, 0, keepdims=False)
        total = total + swap(term, ring, r).astype(F32)
    return total


def to_owners(grad):
    return lax.psum_scatter(grad, "fsdp", scatter_dimension=0, tiled=True)


def sum_owned(owned, ring, me):
    rows, width = owned.shape
    part = sum_seq(owned.reshape(ring, rows // ring, width), ring, me).astype(BF16)
    return gather_seq(part, ring, me).reshape(rows, width).astype(F32)


def sum_vectors(rows, devices, ring):
    count, width = rows.shape
    sent = rows.reshape(count, devices, width // devices).transpose(1, 0, 2)
    total = jnp.sum(lax.all_to_all(sent, "fsdp", split_axis=0, concat_axis=0, tiled=True), axis=0)
    return total + sum(swap(total, ring, r) for r in range(1, ring))


def normalize(values):
    centered = values - jnp.mean(values, axis=-1, keepdims=True)
    variance = jnp.mean(centered * centered, axis=-1, keepdims=True)
    rstd = lax.rsqrt(variance + EPSILON)
    return centered * rstd, rstd


def normalize_back(grad, normed, rstd, gain):
    e = grad * gain
    mean = jnp.mean(e, axis=-1, keepdims=True)
    along = jnp.mean(e * normed, axis=-1, keepdims=True)
    return rstd * (e - mean - normed * along)


def shards_any(
    ring,
    devices,
    tokens,
    lengths,
    ln1_gain,
    ln1_bias,
    w_qkv,
    q_bias,
    v_bias,
    w_out,
    b_out,
    ln2_gain,
    ln2_bias,
    w_fc1,
    b_fc1,
    w_fc2,
    b_fc2,
    cotangent,
):
    clips, rows, width = tokens.shape
    total_rows = clips * rows
    clip_rows = rows * ring
    local = width // ring
    me = lax.axis_index("seq")

    whole = [gather_seq(tokens[c], ring, me).reshape(clip_rows, width) for c in range(clips)]

    own = ln1_gain.shape[0]
    packed = jnp.concatenate(
        [
            jnp.stack([ln1_gain, ln1_bias, q_bias, v_bias, b_out, ln2_gain, ln2_bias, b_fc2]),
            b_fc1.reshape(-1, own),
        ]
    )
    vectors = lax.all_gather(packed, "fsdp", axis=0, tiled=False)
    c1 = vectors[:, 8:].reshape(-1).astype(F32)
    vectors = vectors[:, :8].transpose(1, 0, 2).reshape(8, width).astype(F32)
    g1, b1, qb, vb, bo, g2, b2, c2 = (vectors[i] for i in range(8))
    qb_mine = lax.dynamic_slice_in_dim(qb, me * local, local)
    vb_mine = lax.dynamic_slice_in_dim(vb, me * local, local)
    bias_mine = jnp.concatenate([qb_mine, jnp.zeros_like(qb_mine), vb_mine])

    mine = lax.dynamic_index_in_dim(w_qkv.reshape(own, 3, ring, local), me, 2, keepdims=False)
    wqkv = lax.all_gather(mine.reshape(own, 3 * local), "fsdp", axis=0, tiled=True)
    wo = lax.all_gather(w_out, "fsdp", axis=0, tiled=True)
    w1 = lax.all_gather(w_fc1, "fsdp", axis=0, tiled=True)
    w2 = lax.all_gather(w_fc2, "fsdp", axis=0, tiled=True)

    normed, qkv, heads_out, logs, attended = [], [], [], [], []
    for c in range(clips):
        n1 = normalize(whole[c].astype(F32))[0]
        h1 = (n1 * g1 + b1).astype(BF16)
        part = (dot(h1, wqkv) + bias_mine).astype(BF16)[None]
        out, log = attend(part, lax.dynamic_slice_in_dim(lengths, c, 1))
        moved = lax.all_to_all(
            out.reshape(ring, rows, local), "seq", split_axis=0, concat_axis=0, tiled=True
        )
        normed.append(h1)
        qkv.append(part)
        heads_out.append(out)
        logs.append(log)
        attended.append(moved.transpose(1, 0, 2).reshape(rows, width))
    attended = jnp.concatenate(attended, axis=0)

    inputs = tokens.astype(F32).reshape(total_rows, width)
    middle = inputs + (dot(attended, wo) + bo)
    n2, r2 = normalize(middle)
    h2 = (n2 * g2 + b2).astype(BF16)
    z = dot(h2, w1) + c1
    phi = 0.5 * (1.0 + lax.erf(z * (2.0 ** -0.5)))
    hidden = (z * phi).astype(BF16)
    slope = phi + z * (jnp.exp(-0.5 * z * z) * 0.3989422804014327)
    layer_out = (middle + (dot(hidden, w2) + c2)).astype(BF16).reshape(clips, rows, width)

    dy = cotangent.reshape(total_rows, width)
    dy_f = dy.astype(F32)
    term_w2 = dot(hidden, dy, TN).astype(BF16)
    dz = (dot(dy, w2, NT) * slope).astype(BF16)
    term_w1 = dot(h2, dz, TN).astype(BF16)
    dh2 = dot(dz, w1, NT)
    grad_middle = dy_f + normalize_back(dh2, n2, r2, g2)
    da = grad_middle.astype(BF16)
    term_wo = dot(attended, da, TN).astype(BF16)
    do = dot(da, wo, NT).astype(BF16)
    do, term_w2, term_w1, term_wo = lax.optimization_barrier((do, term_w2, term_w1, term_wo))
    owned_w2, owned_w1, owned_wo = (to_owners(t) for t in (term_w2, term_w1, term_wo))

    dqkv, own_terms, gain_sum, shift_sum = [], [], 0.0, 0.0
    for c in range(clips):
        sent = do[c * rows : (c + 1) * rows].reshape(rows, ring, local).transpose(1, 0, 2)
        moved = lax.all_to_all(sent, "seq", split_axis=0, concat_axis=0, tiled=True)
        moved = moved.reshape(1, clip_rows, local)
        d = attend_back(
            qkv[c], moved, heads_out[c], logs[c], lax.dynamic_slice_in_dim(lengths, c, 1)
        )[0]
        dh1 = dot(d, wqkv, NT)
        n1 = normalize(whole[c].astype(F32))[0]
        gain_sum = gain_sum + jnp.sum(dh1 * n1, axis=0)
        shift_sum = shift_sum + jnp.sum(dh1, axis=0)
        own_terms.append(sum_seq(dh1.astype(BF16).reshape(ring, rows, width), ring, me))
        dqkv.append(d)
    dqkv = jnp.concatenate(dqkv, axis=0)
    grad_mine = dot(jnp.concatenate(normed, axis=0), dqkv, TN).astype(BF16)
    grad_mine, owned_w2, owned_w1, owned_wo = lax.optimization_barrier(
        (grad_mine, owned_w2, owned_w1, owned_wo)
    )
    owned = to_owners(grad_mine)
    grad_w2, grad_w1, grad_wo = (sum_owned(o, ring, me) for o in (owned_w2, owned_w1, owned_wo))
    grad_qkv = gather_seq(owned, ring, me).astype(F32)
    grad_qkv = jnp.concatenate(
        [grad_qkv[r, :, i * local : (i + 1) * local] for i in range(3) for r in range(ring)], axis=1
    )

    bias_sum = jnp.sum(dqkv.astype(F32), axis=0)
    zeros = jnp.zeros((width,), F32)
    first = jnp.stack(
        [
            gain_sum,
            shift_sum,
            lax.dynamic_update_slice_in_dim(zeros, bias_sum[:local], me * local, 0),
            lax.dynamic_update_slice_in_dim(zeros, bias_sum[2 * local :], me * local, 0),
        ]
    )
    second = jnp.stack(
        [
            jnp.sum(dh2 * n2, axis=0),
            jnp.sum(dh2, axis=0),
            jnp.sum(dy_f, axis=0),
            jnp.sum(da.astype(F32), axis=0),
        ]
    )
    c1_sum = jnp.sum(dz.astype(F32), axis=0).reshape(devices, -1, own).transpose(1, 0, 2)
    second = jnp.concatenate([second, c1_sum.reshape(-1, width)])
    four = sum_vectors(second, devices, ring)
    grad_c1 = four[4:].reshape(-1)
    late = sum_vectors(first, devices, ring)

    terms = jnp.concatenate(own_terms, axis=0)
    n1, r1 = normalize(inputs)
    grad_inputs = (grad_middle + normalize_back(terms, n1, r1, g1)).reshape(clips, rows, width)
    return (
        layer_out,
        grad_inputs,
        late[0],
        late[1],
        grad_qkv,
        late[2],
        late[3],
        grad_wo,
        four[3],
        four[0],
        four[1],
        grad_w1,
        grad_c1,
        grad_w2,
        four[2],
    )


def twin(value, devices):
    return lax.ppermute(value, "fsdp", [(i, i ^ 1) for i in range(devices)])


def columns(vectors):
    vectors = jnp.pad(vectors.astype(BF16), ((0, -vectors.shape[0] % 128), (0, 0)))
    return dot(jnp.eye(vectors.shape[1], dtype=BF16), vectors, NT).astype(BF16)


def as_rows(block, count):
    return dot(block, jnp.eye(block.shape[0], dtype=BF16), TN)[:count]


def plus(a, b):
    return (a.astype(F32) + b.astype(F32)).astype(BF16)


def plus_rows(a, b, more, row):
    total = a.astype(F32) + b.astype(F32)
    pad = [(row, a.shape[0] - row - more.shape[0])] + [(0, 0)] * (a.ndim - 1)
    return (total + jnp.pad(more.astype(F32), pad)).astype(BF16)


def stage(*values):
    return lax.optimization_barrier(values)


def placed(parts, me):
    out = jnp.zeros((len(parts),) + parts[0].shape, parts[0].dtype)
    for r, part in enumerate(parts):
        out = lax.dynamic_update_index_in_dim(out, part, me ^ r, 0)
    return out


def shards(
    ring,
    devices,
    tokens,
    lengths,
    ln1_gain,
    ln1_bias,
    w_qkv,
    q_bias,
    v_bias,
    w_out,
    b_out,
    ln2_gain,
    ln2_bias,
    w_fc1,
    b_fc1,
    w_fc2,
    b_fc2,
    cotangent,
):
    clips, rows, width = tokens.shape
    total_rows, clip_rows, local = clips * rows, rows * ring, width // ring
    own, half, cut = ln1_gain.shape[0], clips // 2, devices // 4
    me, core = lax.axis_index("seq"), lax.axis_index("fsdp") % 2
    same_core = [list(range(p, devices, 2)) for p in range(2)]

    def over(value, r):
        return swap(value, ring, r)

    vectors = jnp.concatenate(
        [
            jnp.stack([ln1_gain, ln1_bias, q_bias, v_bias, b_out, ln2_gain, ln2_bias, b_fc2]),
            b_fc1.reshape(-1, own),
        ]
    )
    count = vectors.shape[0]
    mine = lax.dynamic_index_in_dim(w_qkv.reshape(own, 3, ring, local), me, 2, keepdims=False)
    mine = jnp.concatenate([mine.reshape(own, 3 * local), columns(vectors)], axis=1)
    mine = lax.all_gather(mine, "fsdp", axis=0, tiled=True)
    part1 = lax.dynamic_index_in_dim(w_fc1.reshape(own, devices, ring, own), me, 2)
    part2 = lax.dynamic_index_in_dim(w_fc2.reshape(ring, own, width), me, 0)
    quarter = jnp.concatenate([part1.reshape(1, own, width), part2], axis=0)
    quarter = lax.all_gather(quarter, "fsdp", axis=0, axis_index_groups=same_core)
    wo = lax.all_gather(w_out, "fsdp", axis=0, tiled=True)

    middle_row = rows // 16 * 8
    one, two = stage(over(tokens[0], 1), over(tokens[0], 2))
    far = [over(two[:middle_row], 1), over(one[middle_row:], 2)]
    mine, *far = stage(mine, *far)
    vectors = as_rows(mine[:, 3 * local :], count)
    g1, b1, qb, vb, bo, g2, b2, c2 = (vectors[i] for i in range(8))
    c1_rows = vectors[8:]
    qb_mine = lax.dynamic_slice_in_dim(qb, me * local, local)
    vb_mine = lax.dynamic_slice_in_dim(vb, me * local, local)
    bias_mine = jnp.concatenate([qb_mine, jnp.zeros_like(qb_mine), vb_mine])

    normed, qkv, outs, logs = ([None] * clips for _ in range(4))

    def project(c, groups):
        normed[c], qkv[c] = norm_project(me, groups, g1, b1, mine, bias_mine)

    def to_rows(out):
        return lax.all_to_all(
            out.reshape(ring, rows, local), "seq", split_axis=0, concat_axis=0, tiled=True
        )

    def length(c):
        return lax.dynamic_slice_in_dim(lengths, c, 1)

    project(0, [[(tokens, 0)], [one], [two], far])
    outs[0], logs[0] = attend(qkv[0], length(0))
    others = [over(tokens[1:], r) for r in range(1, ring)]
    outs[0], *others = stage(outs[0], *others)
    moved = []
    for c in range(1, clips):
        moved.append(to_rows(outs[c - 1]))
        project(c, [[(tokens, c)]] + [[(t, c - 1)] for t in others])
        if c == 1:
            qkv[c], quarter, moved[0] = stage(qkv[c], quarter, moved[0])
            ends_of = [quarter[:cut], quarter[cut:]]
            low1, top2 = over(ends_of[1], 1), over(ends_of[0], 2)
            twin0 = twin(quarter, devices)
        outs[c], logs[c] = attend(qkv[c], length(c))
        if c == 1:
            outs[c], low1, top2, twin0 = stage(outs[c], low1, top2, twin0)
    moved.append(to_rows(outs[-1]))
    moved, low1, top2, ends_of = lax.optimization_barrier((moved, low1, top2, ends_of))
    top1, low2 = over(ends_of[0], 1), over(ends_of[1], 2)
    attended, middle, h2, h2t = project_norm(moved, tokens, wo, bo, g2, b2)
    dy = cotangent.reshape(total_rows, width)

    sums = [None] * ring

    def quarter_of(r, mine_r, twin_r, acc):
        shift = lax.dynamic_index_in_dim(c1_rows, me ^ r, 0)
        y, dh2, keep, send, sums[r] = mlp_piece(
            core[None], h2, h2t, dy, mine_r, twin_r, shift, acc
        )
        return (y, dh2), keep, send

    early = [twin(low1, devices), twin(top2, devices)]
    acc, keep0, send0 = quarter_of(0, [quarter], [twin0], None)
    acc, keep0, send0, early, top1, low2 = lax.optimization_barrier(
        (acc, keep0, send0, early, top1, low2)
    )
    far = [over(top2, 1), over(low1, 2)]
    got0, later2 = twin(send0, devices), twin(low2, devices)
    (later1,) = stage(twin(top1, devices))
    acc, keep1, send1 = quarter_of(1, [top1, low1], [later1, early[0]], acc)
    acc, keep1, send1, far, later2, got0 = lax.optimization_barrier(
        (acc, keep1, send1, far, later2, got0)
    )
    twin_far, got1 = [twin(f, devices) for f in far], twin(send1, devices)
    acc, keep2, send2 = quarter_of(2, [top2, low2], [early[1], later2], acc)
    acc, keep2, send2, twin_far, got1 = lax.optimization_barrier(
        (acc, keep2, send2, twin_far, got1)
    )
    got2 = twin(send2, devices)
    acc, keep3, send3 = quarter_of(3, far, twin_far, acc)
    (y, dh2), keep3, send3, got2 = lax.optimization_barrier((acc, keep3, send3, got2))
    (got3,) = stage(twin(send3, devices))
    term3 = plus(keep3, got3)
    ends = [over(term3[:cut], 1), over(term3[cut:], 2)]

    c1_sum = placed([v[0] for v in sums], me)
    def to_heads(part):
        part = lax.all_to_all(part, "seq", split_axis=0, concat_axis=0, tiled=True)
        return part.reshape(1, clip_rows, local)

    layer_out = grad_middle = None
    das, heads, column_sums = ([None] * clips for _ in range(3))
    for c in range(clips):
        layer_out, grad_middle, das[c], heads[c], column_sums[c] = project_back(
            c, y, dh2, middle, dy, wo, g2, c2, tokens.shape, ring, layer_out, grad_middle
        )
        if c == 0:
            moved = to_heads(heads[0])
    term_wo = project_weight(das, attended, column_sums, c1_sum)
    moved, term_wo, end2, end1 = stage(moved, term_wo, *ends)
    owned_wo = to_owners(term_wo)

    second = [
        add_terms([(keep1, None), (got1, None), (end1, cut)]),
        add_terms([(keep2, None), (got2, None), (end2, 0)]),
    ]
    *second, next_moved = stage(*second, to_heads(heads[1]))
    second = [over(second[0], 1), over(second[1], 2)]
    acc, flying, token_terms = None, [], [None] * clips

    def exchange(parts):
        return lax.all_to_all(parts, "seq", 0, 0, tiled=True)

    def to_all(part):
        return exchange(jnp.broadcast_to(part[None], (ring,) + part.shape))

    for c in range(clips):
        later = [to_heads(heads[c + 1])] if 0 < c < clips - 1 else []
        if c == clips - 1:
            owned_wo = owned_wo.reshape(ring, own // ring, width + 128)
            later = [lax.dynamic_index_in_dim(owned_wo, me ^ r, 0, False) for r in range(ring)]
            later = [over(t, r) if r else t for r, t in enumerate(later)]
        d = attend_back(qkv[c], moved, outs[c], logs[c], length(c))
        if c < clips - 1:
            acc = qkv_weight(me, d[0], normed[c], mine, acc, ring, False)
        d, later, flying, second, acc = lax.optimization_barrier((d, later, flying, second, acc))
        moved, wo_terms = (later[0], later) if later else (next_moved, later)
        if c:
            token_terms[c - 1] = flying[0]
        else:
            total = add_terms([(t, None) for t in (keep0, got0, *second)])
            owned_mlp = lax.psum_scatter(
                total,
                "fsdp",
                scatter_dimension=0,
                tiled=True,
                axis_index_groups=same_core,
            )[0]
            second = []
        last = c == clips - 1
        if c < clips - 1:
            flying = [exchange(qkv_back(d[0], mine, ring))]

    d, owned_mlp = stage(d, owned_mlp)
    shared = [over(owned_mlp, 1), over(owned_mlp, 2)]
    grad_mine, kept, one, two, top, low = qkv_weight(
        me, d[0], normed[-1], mine, acc, ring, True
    )
    one, two, top, low, shared, grad_mine = lax.optimization_barrier(
        (one, two, top, low, shared, grad_mine)
    )
    owned = to_owners(grad_mine)

    cross = [over(top, 1), over(low, 2)]
    grad_inputs = None
    for c in range(clips - 1):
        terms = [(token_terms[c], ring)]
        grad_inputs = tokens_back(c, terms, tokens, grad_middle, g1, grad_inputs)
    grad_inputs, cross = lax.optimization_barrier((grad_inputs, cross))
    flying = [
        over(jnp.concatenate([one[:, :middle_row], plus(one[:, middle_row:], cross[1][None])], 1), 1),
        over(jnp.concatenate([plus(two[:, :middle_row], cross[0][None]), two[:, middle_row:]], 1), 2),
    ]
    wo_term = sum(t.astype(F32) for t in wo_terms).astype(BF16)
    wo_parts = to_all(wo_term)
    flying, wo_parts = lax.optimization_barrier((flying, wo_parts))
    owned, flying, shared = lax.optimization_barrier((owned, flying, shared))
    far = [over(shared[1][:1], 1), over(shared[0][1:], 2)]
    grad_w1, grad_w2 = spread_mlp(me, [owned_mlp, *shared, *far], ring)
    owned = [over(owned, r) if r else owned for r in range(ring)]
    terms = [(kept, 1)] + [(f, 1) for f in flying]
    grad_inputs = tokens_back(clips - 1, terms, tokens, grad_middle, g1, grad_inputs)
    grad_wo, grad_qkv, sums = spread_attn(me, wo_parts, owned)
    middle_sums, last_sums = sums[0], sums[1]
    return (
        layer_out,
        grad_inputs,
        last_sums[0],
        last_sums[1],
        grad_qkv,
        last_sums[2],
        last_sums[3],
        grad_wo,
        middle_sums[3],
        middle_sums[0],
        middle_sums[1],
        grad_w1,
        middle_sums[4 : count - 4].reshape(-1),
        grad_w2,
        middle_sums[2],
    )


def solution(mesh):
    act, vec, mat = P("fsdp", "seq", None), P("fsdp"), P("fsdp", None)
    in_specs = (act, vec, vec, vec, mat, vec, vec, mat, vec, vec, vec, mat, vec, mat, vec, act)
    out_specs = (act, act, vec, vec, mat, vec, vec, mat, vec, vec, vec, mat, vec, mat, vec)
    ring, devices = mesh.shape["seq"], mesh.shape["fsdp"]

    def layer(*args):
        clips, rows, width = args[0].shape
        square = ring == 4 and args[11].shape[1] == ring * width and devices % 4 == 0
        square = square and clips % (2 * devices) == 0 and width % (128 * devices) == 0
        return jax.shard_map(
            functools.partial(shards if square else shards_any, ring, devices),
            mesh=mesh,
            in_specs=in_specs,
            out_specs=out_specs,
            check_vma=False,
        )(*args)

    return layer
```

```python
import functools

import jax
import jax.numpy as jnp
from jax import lax
from jax.experimental import pallas as pl
from jax.experimental.pallas import tpu as pltpu
from jax.sharding import PartitionSpec as P

HEAD_DIM = 64
PAIR = 2 * HEAD_DIM
EPSILON = 1e-06
NEGATIVE = -1e30
F32, BF16 = jnp.float32, jnp.bfloat16
SCALE = HEAD_DIM ** -0.5
SCALE2 = SCALE * 1.4426950408889634
NT = (((1,), (1,)), ((), ()))
NN = (((1,), (0,)), ((), ()))
TN = (((0,), (0,)), ((), ()))


def dot(a, b, dims=NN):
    return lax.dot_general(a, b, dims, preferred_element_type=F32)


LARGE = 56 << 20
WHOLE = pl.BlockSpec(memory_space=pltpu.VMEM)
SCALAR = pl.BlockSpec(memory_space=pltpu.SMEM)


def kernel_call(body, name, operands, outs, scratch=(), scalars=0, aliases=None, vmem=40):
    return pl.pallas_call(
        body,
        in_specs=[SCALAR] * scalars + [WHOLE] * (len(operands) - scalars),
        out_specs=[WHOLE] * len(outs),
        out_shape=[jax.ShapeDtypeStruct(*out) for out in outs],
        scratch_shapes=list(scratch),
        input_output_aliases=aliases or {},
        compiler_params=pltpu.CompilerParams(vmem_limit_bytes=vmem << 20),
        cost_estimate=pl.CostEstimate(flops=1 << 20, bytes_accessed=1 << 20, transcendentals=0),
        name=name,
    )(*operands)


def of_head(block, h):
    lane = lax.broadcasted_iota(jnp.int32, (1, PAIR), 1)
    return jnp.where(lane // HEAD_DIM == h, block, jnp.zeros_like(block))


def valid_rows(j, bk, length):
    return j * bk + lax.broadcasted_iota(jnp.int32, (bk, 1), 0) < length


def transposed_chunks(out_ref, in_ref, cols, bk):
    for j in range(in_ref.shape[1] // bk):
        out_ref[j] = jnp.transpose(in_ref[0, pl.ds(j * bk, bk), cols])


def attend_kernel(len_ref, q_ref, k_ref, v_ref, o_ref, lse_ref, s_ref, vt_ref, ot_ref, *, bk):
    length = len_ref[pl.program_id(0)]
    rows_all, width = q_ref.shape[1:]
    chunks = pl.cdiv(length, bk)
    for pair in range(width // PAIR):
        cols = pl.ds(PAIR * pair, PAIR)
        transposed_chunks(vt_ref, v_ref, cols, bk)
        queries = [of_head(q_ref[0, :, cols], h) for h in range(2)]

        def score(j, tops):
            keys = k_ref[0, pl.ds(pl.multiple_of(j * bk, bk), bk), cols]
            ok = valid_rows(j, bk, length)
            out = []
            for h in range(2):
                s = jnp.where(ok, dot(keys, queries[h], NT), NEGATIVE)
                s_ref[h, j] = s
                top = tops[h]
                for i in range(bk // 8):
                    top = jnp.maximum(top, s[8 * i : 8 * i + 8])
                out.append(top)
            return tuple(out)

        low = jnp.full((8, rows_all), NEGATIVE, F32)
        tops = lax.fori_loop(0, chunks, score, (low, low))
        peaks = [jnp.max(top, axis=0, keepdims=True) * SCALE2 for top in tops]
        ot_ref[...] = jnp.zeros_like(ot_ref)

        def mix(j, sums):
            out = []
            for h in range(2):
                p = jnp.exp2(s_ref[h, j] * SCALE2 - peaks[h])
                total = sums[h]
                for i in range(bk // 8):
                    total = total + p[8 * i : 8 * i + 8]
                out.append(total)
                half = pl.ds(HEAD_DIM * h, HEAD_DIM)
                ot_ref[half] += dot(vt_ref[j, half], p.astype(BF16))
            return tuple(out)

        zero = jnp.zeros((8, rows_all), F32)
        sums = lax.fori_loop(0, chunks, mix, (zero, zero))
        for h in range(2):
            total = jnp.sum(sums[h], axis=0, keepdims=True)
            half = pl.ds(HEAD_DIM * h, HEAD_DIM)
            lse_ref[0, pl.ds(2 * pair + h, 1)] = peaks[h] + jnp.log2(total)
            ot_ref[half] = ot_ref[half] / total
        o_ref[0, :, cols] = jnp.transpose(ot_ref[...]).astype(BF16)


def attend_back_kernel(
    len_ref, q_ref, k_ref, v_ref, do_ref, o_ref, lse_ref, d_ref, kt_ref, dqt_ref, *, bk
):
    length = len_ref[pl.program_id(0)]
    width = q_ref.shape[2]
    chunks = pl.cdiv(length, bk)
    d_ref[...] = jnp.zeros_like(d_ref)
    for pair in range(width // PAIR):
        cols = pl.ds(PAIR * pair, PAIR)
        outs = do_ref[0, :, cols]
        both = jnp.transpose(outs.astype(F32) * o_ref[0, :, cols].astype(F32))
        inner = [
            jnp.sum(both[HEAD_DIM * h : HEAD_DIM * (h + 1)], axis=0, keepdims=True)
            for h in range(2)
        ]
        queries = [of_head(q_ref[0, :, cols], h) for h in range(2)]
        grads = [of_head(outs, h) for h in range(2)]
        logs = [lse_ref[0, pl.ds(2 * pair + h, 1)] for h in range(2)]
        transposed_chunks(kt_ref, k_ref, cols, bk)
        dqt_ref[...] = jnp.zeros_like(dqt_ref)

        def step(j, carry):
            rows = pl.ds(pl.multiple_of(j * bk, bk), bk)
            keys = k_ref[0, rows, cols]
            values = v_ref[0, rows, cols]
            ok = valid_rows(j, bk, length)
            dk = jnp.zeros((bk, PAIR), F32)
            dv = jnp.zeros((bk, PAIR), F32)
            for h in range(2):
                p = jnp.exp2(dot(keys, queries[h], NT) * SCALE2 - logs[h])
                p = jnp.where(ok, p, 0.0)
                g = (p * (dot(values, grads[h], NT) - inner[h])).astype(BF16)
                dv = dv + dot(p.astype(BF16), grads[h])
                dk = dk + dot(g, queries[h])
                half = pl.ds(HEAD_DIM * h, HEAD_DIM)
                dqt_ref[half] += dot(kt_ref[j, half], g)
            d_ref[0, rows, pl.ds(width + PAIR * pair, PAIR)] = (dk * SCALE).astype(BF16)
            d_ref[0, rows, pl.ds(2 * width + PAIR * pair, PAIR)] = dv.astype(BF16)
            return carry

        lax.fori_loop(0, chunks, step, 0)
        d_ref[0, :, cols] = jnp.transpose(dqt_ref[...] * SCALE).astype(BF16)


def chunk_rows(rows):
    return max(b for b in range(8, 225, 8) if rows % b == 0)


def block(rows, width, at):
    return pl.BlockSpec((1, rows, width), lambda c, n: (c, 0, at))


def attend(qkv, lengths):
    clips, rows, triple = qkv.shape
    width = triple // 3
    heads, bk = width // HEAD_DIM, chunk_rows(rows)
    cost = clips * heads * rows * rows
    return pl.pallas_call(
        functools.partial(attend_kernel, bk=bk),
        grid_spec=pltpu.PrefetchScalarGridSpec(
            num_scalar_prefetch=1,
            grid=(clips,),
            in_specs=[block(rows, width, i) for i in range(3)],
            out_specs=[block(rows, width, 0), block(heads, rows, 0)],
            scratch_shapes=[
                pltpu.VMEM((2, rows // bk, bk, rows), F32),
                pltpu.VMEM((rows // bk, PAIR, bk), BF16),
                pltpu.VMEM((PAIR, rows), F32),
            ],
        ),
        out_shape=[
            jax.ShapeDtypeStruct((clips, rows, width), BF16),
            jax.ShapeDtypeStruct((clips, heads, rows), F32),
        ],
        compiler_params=pltpu.CompilerParams(vmem_limit_bytes=LARGE),
        cost_estimate=pl.CostEstimate(
            flops=1 << 20, bytes_accessed=1 << 20, transcendentals=0
        ),
        name="attend",
    )(lengths, qkv, qkv, qkv)


def attend_back(qkv, grads, outs, logs, lengths):
    clips, rows, triple = qkv.shape
    width = triple // 3
    heads, bk = width // HEAD_DIM, chunk_rows(rows)
    cost = clips * heads * rows * rows
    return pl.pallas_call(
        functools.partial(attend_back_kernel, bk=bk),
        grid_spec=pltpu.PrefetchScalarGridSpec(
            num_scalar_prefetch=1,
            grid=(clips,),
            in_specs=[block(rows, width, i) for i in (0, 1, 2, 0, 0)] + [block(heads, rows, 0)],
            out_specs=block(rows, triple, 0),
            scratch_shapes=[
                pltpu.VMEM((rows // bk, PAIR, bk), BF16),
                pltpu.VMEM((PAIR, rows), F32),
            ],
        ),
        out_shape=jax.ShapeDtypeStruct((clips, rows, triple), BF16),
        compiler_params=pltpu.CompilerParams(vmem_limit_bytes=LARGE),
        cost_estimate=pl.CostEstimate(
            flops=1 << 20, bytes_accessed=1 << 20, transcendentals=0
        ),
        name="attend_back",
    )(lengths, qkv, qkv, qkv, grads, outs, logs)


def norm_kernel(me_ref, *refs, counts):
    parts, rest = refs[: sum(counts)], refs[sum(counts) :]
    g_ref, b_ref, w_ref, bias_ref = rest[:4]
    h_ref, qkv_ref, x_ref = rest[-3:]
    taken = 0
    for r, count in enumerate(counts):
        group = parts[taken : taken + count]
        taken += count

        @pl.when(pl.program_id(0) == r)
        def _():
            row = 0
            for ref in group:
                x_ref[pl.ds(row, ref.shape[0])] = ref[...]
                row += ref.shape[0]

    normed, _ = normalize(x_ref[...].astype(F32))
    h = (normed * g_ref[...] + b_ref[...]).astype(BF16)
    h_ref[0] = h
    qkv_ref[0] = (dot(h, w_ref[...]) + bias_ref[...]).astype(BF16)


def norm_project(me, groups, gain, shift, weight, bias, ring, start=0, made=()):
    flat = [part if isinstance(part, tuple) else (part, None) for g in groups for part in g]
    triple, width = bias.shape[-1], flat[0][0].shape[-1]
    rows = sum(p.shape[-2] for p, _ in flat) // len(groups)

    def part_spec(array, clip):
        if clip is None:
            return pl.BlockSpec(array.shape, lambda r, m: (0, 0))
        return pl.BlockSpec((None, rows, width), lambda r, m: (clip, 0, 0))

    def out(cols):
        return pl.BlockSpec((1, rows, cols), lambda r, m: (m[0] ^ (r + start), 0, 0))

    h, qkv = pl.pallas_call(
        functools.partial(norm_kernel, counts=[len(g) for g in groups]),
        grid_spec=pltpu.PrefetchScalarGridSpec(
            num_scalar_prefetch=1,
            grid=(len(groups),),
            in_specs=[part_spec(*part) for part in flat]
            + [WHOLE] * 2
            + [pl.BlockSpec((width, triple), lambda r, m: (0, 0)), WHOLE]
            + [pl.BlockSpec(memory_space=pl.ANY)] * len(made),
            out_specs=[out(width), out(triple)],
            scratch_shapes=[pltpu.VMEM((rows, width), BF16)],
        ),
        out_shape=[jax.ShapeDtypeStruct((ring, rows, c), BF16) for c in (width, triple)],
        input_output_aliases={len(flat) + 5 + i: i for i in range(len(made))},
        compiler_params=pltpu.CompilerParams(vmem_limit_bytes=LARGE),
        cost_estimate=pl.CostEstimate(flops=1 << 20, bytes_accessed=1 << 20, transcendentals=0),
        name="norm_project",
    )(me[None], *[part[0] for part in flat], gain[None], shift[None], weight, bias[None], *made)
    return h, qkv


def mlp_piece_kernel(core_ref, h_ref, ht_ref, dy_ref, *refs, first, nz, counts):
    mines, others, refs = refs[: counts[0]], refs[counts[0] : sum(counts)], refs[sum(counts) :]
    c1_ref, *refs = refs
    yin_ref, dhin_ref = (None, None) if first else (refs.pop(0), refs.pop(0))
    y_ref, dh_ref, keep_ref, send_ref, sums_ref, hm_ref, hmt_ref, w1_ref, w2_ref, u_ref, dz_ref = refs
    core = core_ref[0]
    width = h_ref.shape[1]
    clips, _, share = ht_ref.shape
    rows = mines[0].shape[2]
    half = nz * rows

    def at(i, p):
        block = 2 * i + (core if p == 0 else 1 - core)
        return pl.ds(pl.multiple_of(block * rows, rows), rows)

    def put(i, p):
        return pl.ds(p * half + i * rows, rows)

    def source(i, p):
        parts = (mines, others)[p]
        size = nz // len(parts)
        return parts[i // size], i % size

    for i in range(nz):
        for p in range(2):
            hm_ref[:, put(i, p)] = h_ref[:, at(i, p)]
            for c in range(clips):
                hmt_ref[c, put(i, p), :] = ht_ref[c, at(i, p), :]
            src, z = source(i, p)
            w2_ref[pl.ds((2 * i + p) * rows, rows), :] = src[z, 1]
            for j in range(nz):
                for r in range(2):
                    w1_ref[put(i, p), pl.ds((2 * j + r) * rows, rows)] = src[z, 0, :, at(j, r)]
    for i in range(nz):
        cols = pl.ds(2 * i * rows, 2 * rows)
        bias = jnp.concatenate([c1_ref[:, at(i, p)] for p in range(2)], axis=1)
        z = dot(hm_ref[...], w1_ref[:, cols]) + bias
        phi = 0.5 * (1.0 + lax.erf(z * (2.0 ** -0.5)))
        u_ref[:, cols] = (z * phi).astype(BF16)
        slope = phi + z * (jnp.exp(z * z * -0.5) * 0.3989422804014327)
        dz = (dot(dy_ref[...], w2_ref[cols, :], NT) * slope).astype(BF16)
        dz_ref[:, cols] = dz
        total = jnp.sum(dz.astype(F32), axis=0, keepdims=True)
        for p in range(2):
            sums_ref[:, at(i, p)] = total[:, p * rows : (p + 1) * rows]
        g2 = dot(u_ref[:, cols], dy_ref[...], TN).astype(BF16)
        keep_ref[i, 1] = g2[:rows]
        send_ref[i, 1] = g2[rows:]
        g1 = sum(dot(hmt_ref[c], dz_ref[pl.ds(c * share, share), cols]) for c in range(clips))
        g1 = g1.astype(BF16)
        for p in range(2):
            part = g1[:, p * rows : (p + 1) * rows]
            keep_ref[:, 0, :, at(i, p)] = part[:half].reshape(nz, rows, rows)
            send_ref[:, 0, :, at(i, p)] = part[half:].reshape(nz, rows, rows)
    for n in range(width // 256):
        cols = pl.ds(256 * n, 256)
        y = dot(u_ref[...], w2_ref[:, cols])
        y_ref[:, cols] = y if first else y + yin_ref[:, cols]
    for n in range(width // 256):
        d = dot(dz_ref[...], w1_ref[pl.ds(256 * n, 256), :], NT)
        for q in range(256 // rows):
            p, i = divmod((256 // rows) * n + q, nz)
            v = d[:, q * rows : (q + 1) * rows]
            dh_ref[:, at(i, p)] = v if first else v + dhin_ref[:, at(i, p)]


def mlp_piece(core, h2, h2t, dy, mine, other, c1, acc):
    rows = mine[0].shape[2]
    t, width = h2.shape
    nz = width // (2 * rows)
    first = acc is None
    ins = [core, h2, h2t, dy, *mine, *other, c1] + ([] if first else list(acc))
    gradient = ((nz, 2, rows, width), BF16)
    return kernel_call(
        functools.partial(
            mlp_piece_kernel, first=first, nz=nz, counts=(len(mine), len(other))
        ),
        "mlp_piece",
        ins,
        [((t, width), F32), ((t, width), F32), gradient, gradient, (c1.shape, F32)],
        scratch=[pltpu.VMEM((t, width), BF16), pltpu.VMEM(h2t.shape, BF16)]
        + [pltpu.VMEM((width, width), BF16)] * 2
        + [pltpu.VMEM((t, width), BF16)] * 2,
        scalars=1,
        aliases={} if first else {len(ins) - 2: 0, len(ins) - 1: 1},
        vmem=24,
    )


def project_kernel(*refs, clips):
    moved, rest = refs[:clips], refs[clips:]
    x_ref, wo_ref, bo_ref, g_ref, b_ref, att_ref, mid_ref, h_ref, ht_ref = rest
    ring, rows, local = moved[0].shape
    for c in range(clips):
        at = pl.ds(c * rows, rows)
        for s in range(ring):
            att_ref[at, pl.ds(s * local, local)] = moved[c][s]
        middle = x_ref[c].astype(F32) + (dot(att_ref[at, :], wo_ref[...]) + bo_ref[...])
        mid_ref[at, :] = middle
        h = (normalize(middle)[0] * g_ref[...] + b_ref[...]).astype(BF16)
        h_ref[at, :] = h
        ht_ref[c] = jnp.transpose(h)


def project_norm(moved, tokens, wo, bo, gain, shift):
    clips, rows, width = tokens.shape
    flat = (clips * rows, width)
    return kernel_call(
        functools.partial(project_kernel, clips=clips),
        "project_norm",
        [*moved, tokens, wo, bo[None], gain[None], shift[None]],
        [(flat, BF16), (flat, F32), (flat, BF16), ((clips, width, rows), BF16)],
        vmem=20,
    )


def project_back_kernel(*refs, clip, first):
    y_ref, dh_ref, mid_ref, dy_ref, wo_ref, g_ref, c2_ref = refs[:7]
    out_ref, gm_ref, da_ref, do_ref, sum_ref = refs[-5:]
    ring, rows, local = do_ref.shape
    middle = mid_ref[...]
    out_ref[0] = (middle + (y_ref[...] + c2_ref[...])).astype(BF16)
    normed, rstd = normalize(middle)
    dh = dh_ref[...]
    dy = dy_ref[...].astype(F32)
    grad = dy + normalize_back(dh, normed, rstd, g_ref[...])
    gm_ref[0] = grad
    da = grad.astype(BF16)
    da_ref[...] = da
    do = dot(da, wo_ref[...], NT).astype(BF16)
    for s in range(ring):
        do_ref[s] = do[:, s * local : (s + 1) * local]
    sum_ref[...] = jnp.zeros_like(sum_ref)
    for i, terms in enumerate((dh * normed, dh, dy, da.astype(F32))):
        sum_ref[pl.ds(i, 1), :] = jnp.sum(terms, axis=0, keepdims=True)


def project_back(c, y, dh, middle, dy, wo, gain, c2, shape, ring, out, grad):
    clips, rows, width = shape
    at = pl.BlockSpec((rows, width), lambda i: (c, 0))
    at_c = pl.BlockSpec((1, rows, width), lambda i: (c, 0, 0))
    one = pl.BlockSpec((1, width), lambda i: (0, 0))
    back = [] if out is None else [out, grad]
    return pl.pallas_call(
        functools.partial(project_back_kernel, clip=c, first=out is None),
        grid=(1,),
        in_specs=[at] * 4
        + [pl.BlockSpec((width, width), lambda i: (0, 0)), one, one]
        + [pl.BlockSpec(memory_space=pl.ANY)] * len(back),
        out_specs=[
            at_c,
            at_c,
            pl.BlockSpec((rows, width), lambda i: (0, 0)),
            pl.BlockSpec((ring, rows, width // ring), lambda i: (0, 0, 0)),
            pl.BlockSpec((8, width), lambda i: (0, 0)),
        ],
        out_shape=[
            jax.ShapeDtypeStruct(shape, BF16),
            jax.ShapeDtypeStruct(shape, F32),
            jax.ShapeDtypeStruct((rows, width), BF16),
            jax.ShapeDtypeStruct((ring, rows, width // ring), BF16),
            jax.ShapeDtypeStruct((8, width), F32),
        ],
        input_output_aliases={7: 0, 8: 1} if back else {},
        compiler_params=pltpu.CompilerParams(vmem_limit_bytes=LARGE),
        cost_estimate=pl.CostEstimate(flops=1 << 20, bytes_accessed=1 << 20, transcendentals=0),
        name="project_back",
    )(y, dh, middle, dy, wo, gain[None], c2[None], *back)


def project_weight_kernel(*refs, clips):
    das, att_ref, sums = refs[:clips], refs[clips], refs[clips + 1 : 2 * clips + 1]
    c1_ref, gw_ref, sum_ref = refs[2 * clips + 1 :]
    rows, width = das[0].shape
    term = dot(att_ref[pl.ds(0, rows), :], das[0][...], TN)
    total = sums[0][...]
    for c in range(1, clips):
        term = term + dot(att_ref[pl.ds(c * rows, rows), :], das[c][...], TN)
        total = total + sums[c][...]
    sum_ref[...] = jnp.zeros_like(sum_ref)
    sum_ref[pl.ds(0, 8), :] = total
    sum_ref[pl.ds(4, c1_ref.shape[0]), :] = c1_ref[...]
    gw_ref[:, pl.ds(0, width)] = term.astype(BF16)
    gw_ref[:, pl.ds(width, 128)] = jnp.transpose(sum_ref[...]).astype(BF16)


def project_weight(das, attended, sums, c1_sum):
    width = attended.shape[1]
    return kernel_call(
        functools.partial(project_weight_kernel, clips=len(das)),
        "project_weight",
        [*das, attended, *sums, c1_sum],
        [((width, width + 128), BF16)],
        scratch=[pltpu.VMEM((128, width), F32)],
        vmem=56,
    )[0]


def qkv_back_kernel(d_ref, w_ref, part_ref):
    part_ref[0] = dot(d_ref[...], w_ref[...], NT).astype(BF16)


def qkv_back(d, weight, ring):
    whole, triple = d.shape
    width, rows = weight.shape[0], whole // ring
    return pl.pallas_call(
        qkv_back_kernel,
        grid=(ring,),
        in_specs=[
            pl.BlockSpec((rows, triple), lambda r: (r, 0)),
            pl.BlockSpec((width, triple), lambda r: (0, 0)),
        ],
        out_specs=pl.BlockSpec((1, rows, width), lambda r: (r, 0, 0)),
        out_shape=jax.ShapeDtypeStruct((ring, rows, width), BF16),
        compiler_params=pltpu.CompilerParams(vmem_limit_bytes=LARGE),
        cost_estimate=pl.CostEstimate(flops=1 << 20, bytes_accessed=1 << 20, transcendentals=0),
        name="qkv_back",
    )(d, weight)


def qkv_weight_kernel(me_ref, d_ref, h_ref, w_ref, *rest, first, last):
    rest = list(rest)
    acc_ref, bias_ref = (None, None) if first else (rest.pop(0), rest.pop(0))
    triple = d_ref.shape[1]
    local = triple // 3
    term = dot(h_ref[...], d_ref[...], TN)
    bias = jnp.sum(d_ref[...].astype(F32), axis=0, keepdims=True)
    if not first:
        term = term + acc_ref[...]
        bias = bias + bias_ref[pl.ds(0, 1), :]
    if not last:
        out_ref, sum_ref = rest
        out_ref[...] = term
        sum_ref[...] = jnp.broadcast_to(bias, sum_ref.shape)
        return
    out_ref, own_ref, one_ref, two_ref, top_ref, low_ref, row_ref = rest
    rows, cut = own_ref.shape[1], top_ref.shape[0]
    for r in (3, 1, 2, 0):
        at = pl.ds(pl.multiple_of((me_ref[0] ^ r) * rows, 8), rows)
        part = dot(d_ref[at, :], w_ref[:, pl.ds(0, triple)], NT).astype(BF16)
        if r == 3:
            top_ref[...] = part[:cut]
            low_ref[...] = part[cut:]
        else:
            (own_ref, one_ref, two_ref)[r][0] = part
    out_ref[:, pl.ds(0, triple)] = term.astype(BF16)
    weight = w_ref[:, pl.ds(0, triple)].astype(F32)
    vectors = w_ref[:, pl.ds(triple, 128)].astype(F32)
    gain, shift = vectors[:, 0:1], vectors[:, 1:2]
    shift_sum = jnp.sum(weight * bias, axis=1, keepdims=True)
    gain_sum = (jnp.sum(weight * term, axis=1, keepdims=True) - shift * shift_sum) / gain
    row_ref[...] = jnp.zeros_like(row_ref)
    at_me = pl.ds(pl.multiple_of(me_ref[0] * local, local), local)
    row_ref[pl.ds(2, 1), at_me] = bias[:, :local]
    row_ref[pl.ds(3, 1), at_me] = bias[:, 2 * local :]
    lane = lax.broadcasted_iota(jnp.int32, (1, 128), 1)
    sums = jnp.transpose(row_ref[...])
    sums = jnp.where(lane == 0, gain_sum, jnp.where(lane == 1, shift_sum, sums))
    out_ref[:, pl.ds(triple, 128)] = sums.astype(BF16)


def qkv_weight(me, d, h, mine, acc, ring, last):
    (whole, triple), width = d.shape, h.shape[1]
    outs = [((width, triple), F32), ((8, triple), F32)]
    if last:
        rows = whole // ring
        cut = rows // 16 * 8
        outs = [((width, triple + 128), BF16)] + [((1, rows, width), BF16)] * 3
        outs += [((cut, width), BF16), ((rows - cut, width), BF16)]
    return kernel_call(
        functools.partial(qkv_weight_kernel, first=acc is None, last=last),
        "qkv_weight",
        [me[None], d, h, mine] + list(acc or ()),
        outs,
        scratch=[pltpu.VMEM((128, width), F32)] if last else (),
        scalars=1,
        vmem=56,
    )


def tokens_back_kernel(*refs, counts):
    term_refs, (x_ref, gm_ref, g_ref) = refs[: len(counts)], refs[len(counts) : len(counts) + 3]
    out_ref = refs[-1]
    grad = None
    for count, ref in zip(counts, term_refs):
        for r in range(count):
            term = ref[r].astype(F32)
            grad = term if grad is None else grad + term
    normed, rstd = normalize(x_ref[0].astype(F32))
    out_ref[0] = gm_ref[0] + normalize_back(grad, normed, rstd, g_ref[...])


def tokens_back(c, terms, tokens, grad_middle, gain, out):
    clips, rows, width = tokens.shape
    steps = max(n for n in (7, 4, 2, 1) if rows % (8 * n) == 0)
    block = rows // steps
    at_c = pl.BlockSpec((1, block, width), lambda i: (c, i, 0))
    counts = [count for _, count in terms]
    specs = [pl.BlockSpec((n, block, width), lambda i: (0, i, 0)) for n in counts] + [at_c, at_c]
    specs.append(pl.BlockSpec((1, width), lambda i: (0, 0)))
    operands = [*[array for array, _ in terms], tokens, grad_middle, gain[None]]
    if out is not None:
        specs.append(pl.BlockSpec(memory_space=pl.ANY))
        operands.append(out)
    return pl.pallas_call(
        functools.partial(tokens_back_kernel, counts=counts),
        grid=(steps,),
        in_specs=specs,
        out_specs=at_c,
        out_shape=jax.ShapeDtypeStruct((clips, rows, width), F32),
        input_output_aliases={} if out is None else {len(operands) - 1: 0},
        compiler_params=pltpu.CompilerParams(vmem_limit_bytes=LARGE),
        cost_estimate=pl.CostEstimate(flops=1 << 20, bytes_accessed=1 << 20, transcendentals=0),
        name="tokens_back",
    )(*operands)


def add_kernel(*refs, ranges):
    out_ref = refs[-1]
    step = pl.program_id(0)
    total = None
    for (start, stop), ref in zip(ranges, refs):
        term = ref[...].astype(F32)
        if start is not None:
            inside = (step >= start) & (step < stop)
            term = jnp.where(inside, term, 0.0)
        total = term if total is None else total + term
    out_ref[...] = total.astype(BF16)


def add_terms(terms):
    shape = terms[0][0].shape
    block = (1,) + shape[1:]
    rest = (0,) * (len(shape) - 1)

    def spec(count, row):
        if row is None:
            return pl.BlockSpec(block, lambda z: (z, *rest))
        return pl.BlockSpec(block, lambda z: (jnp.clip(z - row, 0, count - 1), *rest))

    return pl.pallas_call(
        functools.partial(
            add_kernel,
            ranges=[(r, None if r is None else r + t.shape[0]) for t, r in terms],
        ),
        grid=shape[:1],
        in_specs=[spec(t.shape[0], row) for t, row in terms],
        out_specs=pl.BlockSpec(block, lambda z: (z, *rest)),
        out_shape=jax.ShapeDtypeStruct(shape, BF16),
        compiler_params=pltpu.CompilerParams(vmem_limit_bytes=24 << 20),
        cost_estimate=pl.CostEstimate(flops=1 << 20, bytes_accessed=1 << 20, transcendentals=0),
        name="add_terms",
    )(*[t for t, _ in terms])


def spread_mlp_kernel(me_ref, own_ref, one_ref, two_ref, far1_ref, far2_ref, w1_ref, w2_ref):
    own = own_ref.shape[1]
    ring = w1_ref.shape[1] // own_ref.shape[2]
    firsts = [own_ref.at[0], one_ref.at[0], two_ref.at[0], far1_ref.at[0]]
    seconds = [own_ref.at[1], one_ref.at[1], two_ref.at[1], far2_ref.at[0]]
    for r in range(ring):
        q = me_ref[0] ^ r
        part = firsts[r][...].astype(F32)
        for f in range(part.shape[1] // own):
            at = pl.ds(pl.multiple_of((f * ring + q) * own, own), own)
            w1_ref[:, at] = part[:, f * own : (f + 1) * own]
        w2_ref[pl.ds(pl.multiple_of(q * own, own), own), :] = seconds[r][...].astype(F32)


def spread_mlp(me, parts, ring):
    _, own, width = parts[0].shape
    return kernel_call(
        spread_mlp_kernel,
        "spread_mlp",
        [me[None], *parts],
        [((own, ring * width), F32), ((ring * own, width), F32)],
        scalars=1,
    )


def spread_attn_kernel(me_ref, *refs, ring):
    wo_ref, qkv_refs = refs[0], refs[1 : ring + 1]
    gwo_ref, gqkv_ref, vec_ref, more_ref = refs[ring + 1 :]
    own, width = gwo_ref.shape
    rows = wo_ref.shape[1]
    triple = qkv_refs[0].shape[1] - 128
    local = triple // 3
    last = jnp.zeros((own, 128), F32)
    for r in range(ring):
        q = me_ref[0] ^ r
        gwo_ref[pl.ds(r * rows, rows), :] = wo_ref[r, :, :width].astype(F32)
        more_ref[pl.ds(r * rows, rows), :] = wo_ref[r, :, width:].astype(F32)
        last = last + qkv_refs[r][:, triple:].astype(F32)
        for i in range(3):
            part = qkv_refs[r][:, i * local : (i + 1) * local].astype(F32)
            gqkv_ref[:, pl.ds(pl.multiple_of(i * width + q * local, local), local)] = part
    vec_ref[0] = jnp.transpose(more_ref[...])
    vec_ref[1] = jnp.transpose(last)


def spread_attn(me, wo_parts, qkv_parts):
    ring, own = len(qkv_parts), qkv_parts[0].shape[0]
    width = wo_parts.shape[2] - 128
    return kernel_call(
        functools.partial(spread_attn_kernel, ring=ring),
        "spread_attn",
        [me[None], wo_parts, *qkv_parts],
        [((own, width), F32), ((own, 3 * width), F32), ((2, 128, own), F32)],
        scratch=[pltpu.VMEM((own, 128), F32)],
        scalars=1,
    )


def swap(value, ring, r):
    return lax.ppermute(value, "seq", [(i, i ^ r) for i in range(ring)])


def gather_seq(value, ring, me):
    out = jnp.zeros((ring,) + value.shape, value.dtype)
    out = lax.dynamic_update_index_in_dim(out, value, me, 0)
    for r in range(1, ring):
        out = lax.dynamic_update_index_in_dim(out, swap(value, ring, r), me ^ r, 0)
    return out


def sum_seq(terms, ring, me):
    total = lax.dynamic_index_in_dim(terms, me, 0, keepdims=False).astype(F32)
    for r in range(1, ring):
        term = lax.dynamic_index_in_dim(terms, me ^ r, 0, keepdims=False)
        total = total + swap(term, ring, r).astype(F32)
    return total


def to_owners(grad):
    return lax.psum_scatter(grad, "fsdp", scatter_dimension=0, tiled=True)


def sum_owned(owned, ring, me):
    rows, width = owned.shape
    part = sum_seq(owned.reshape(ring, rows // ring, width), ring, me).astype(BF16)
    return gather_seq(part, ring, me).reshape(rows, width).astype(F32)


def sum_vectors(rows, devices, ring):
    count, width = rows.shape
    sent = rows.reshape(count, devices, width // devices).transpose(1, 0, 2)
    total = jnp.sum(lax.all_to_all(sent, "fsdp", split_axis=0, concat_axis=0, tiled=True), axis=0)
    return total + sum(swap(total, ring, r) for r in range(1, ring))


def normalize(values):
    centered = values - jnp.mean(values, axis=-1, keepdims=True)
    variance = jnp.mean(centered * centered, axis=-1, keepdims=True)
    rstd = lax.rsqrt(variance + EPSILON)
    return centered * rstd, rstd


def normalize_back(grad, normed, rstd, gain):
    e = grad * gain
    mean = jnp.mean(e, axis=-1, keepdims=True)
    along = jnp.mean(e * normed, axis=-1, keepdims=True)
    return rstd * (e - mean - normed * along)


def shards_any(
    ring,
    devices,
    tokens,
    lengths,
    ln1_gain,
    ln1_bias,
    w_qkv,
    q_bias,
    v_bias,
    w_out,
    b_out,
    ln2_gain,
    ln2_bias,
    w_fc1,
    b_fc1,
    w_fc2,
    b_fc2,
    cotangent,
):
    clips, rows, width = tokens.shape
    total_rows = clips * rows
    clip_rows = rows * ring
    local = width // ring
    me = lax.axis_index("seq")

    whole = [gather_seq(tokens[c], ring, me).reshape(clip_rows, width) for c in range(clips)]

    own = ln1_gain.shape[0]
    packed = jnp.concatenate(
        [
            jnp.stack([ln1_gain, ln1_bias, q_bias, v_bias, b_out, ln2_gain, ln2_bias, b_fc2]),
            b_fc1.reshape(-1, own),
        ]
    )
    vectors = lax.all_gather(packed, "fsdp", axis=0, tiled=False)
    c1 = vectors[:, 8:].reshape(-1).astype(F32)
    vectors = vectors[:, :8].transpose(1, 0, 2).reshape(8, width).astype(F32)
    g1, b1, qb, vb, bo, g2, b2, c2 = (vectors[i] for i in range(8))
    qb_mine = lax.dynamic_slice_in_dim(qb, me * local, local)
    vb_mine = lax.dynamic_slice_in_dim(vb, me * local, local)
    bias_mine = jnp.concatenate([qb_mine, jnp.zeros_like(qb_mine), vb_mine])

    mine = lax.dynamic_index_in_dim(w_qkv.reshape(own, 3, ring, local), me, 2, keepdims=False)
    wqkv = lax.all_gather(mine.reshape(own, 3 * local), "fsdp", axis=0, tiled=True)
    wo = lax.all_gather(w_out, "fsdp", axis=0, tiled=True)
    w1 = lax.all_gather(w_fc1, "fsdp", axis=0, tiled=True)
    w2 = lax.all_gather(w_fc2, "fsdp", axis=0, tiled=True)

    normed, qkv, heads_out, logs, attended = [], [], [], [], []
    for c in range(clips):
        n1 = normalize(whole[c].astype(F32))[0]
        h1 = (n1 * g1 + b1).astype(BF16)
        part = (dot(h1, wqkv) + bias_mine).astype(BF16)[None]
        out, log = attend(part, lax.dynamic_slice_in_dim(lengths, c, 1))
        moved = lax.all_to_all(
            out.reshape(ring, rows, local), "seq", split_axis=0, concat_axis=0, tiled=True
        )
        normed.append(h1)
        qkv.append(part)
        heads_out.append(out)
        logs.append(log)
        attended.append(moved.transpose(1, 0, 2).reshape(rows, width))
    attended = jnp.concatenate(attended, axis=0)

    inputs = tokens.astype(F32).reshape(total_rows, width)
    middle = inputs + (dot(attended, wo) + bo)
    n2, r2 = normalize(middle)
    h2 = (n2 * g2 + b2).astype(BF16)
    z = dot(h2, w1) + c1
    phi = 0.5 * (1.0 + lax.erf(z * (2.0 ** -0.5)))
    hidden = (z * phi).astype(BF16)
    slope = phi + z * (jnp.exp(-0.5 * z * z) * 0.3989422804014327)
    layer_out = (middle + (dot(hidden, w2) + c2)).astype(BF16).reshape(clips, rows, width)

    dy = cotangent.reshape(total_rows, width)
    dy_f = dy.astype(F32)
    term_w2 = dot(hidden, dy, TN).astype(BF16)
    dz = (dot(dy, w2, NT) * slope).astype(BF16)
    term_w1 = dot(h2, dz, TN).astype(BF16)
    dh2 = dot(dz, w1, NT)
    grad_middle = dy_f + normalize_back(dh2, n2, r2, g2)
    da = grad_middle.astype(BF16)
    term_wo = dot(attended, da, TN).astype(BF16)
    do = dot(da, wo, NT).astype(BF16)
    do, term_w2, term_w1, term_wo = lax.optimization_barrier((do, term_w2, term_w1, term_wo))
    owned_w2, owned_w1, owned_wo = (to_owners(t) for t in (term_w2, term_w1, term_wo))

    dqkv, own_terms, gain_sum, shift_sum = [], [], 0.0, 0.0
    for c in range(clips):
        sent = do[c * rows : (c + 1) * rows].reshape(rows, ring, local).transpose(1, 0, 2)
        moved = lax.all_to_all(sent, "seq", split_axis=0, concat_axis=0, tiled=True)
        moved = moved.reshape(1, clip_rows, local)
        d = attend_back(
            qkv[c], moved, heads_out[c], logs[c], lax.dynamic_slice_in_dim(lengths, c, 1)
        )[0]
        dh1 = dot(d, wqkv, NT)
        n1 = normalize(whole[c].astype(F32))[0]
        gain_sum = gain_sum + jnp.sum(dh1 * n1, axis=0)
        shift_sum = shift_sum + jnp.sum(dh1, axis=0)
        own_terms.append(sum_seq(dh1.astype(BF16).reshape(ring, rows, width), ring, me))
        dqkv.append(d)
    dqkv = jnp.concatenate(dqkv, axis=0)
    grad_mine = dot(jnp.concatenate(normed, axis=0), dqkv, TN).astype(BF16)
    grad_mine, owned_w2, owned_w1, owned_wo = lax.optimization_barrier(
        (grad_mine, owned_w2, owned_w1, owned_wo)
    )
    owned = to_owners(grad_mine)
    grad_w2, grad_w1, grad_wo = (sum_owned(o, ring, me) for o in (owned_w2, owned_w1, owned_wo))
    grad_qkv = gather_seq(owned, ring, me).astype(F32)
    grad_qkv = jnp.concatenate(
        [grad_qkv[r, :, i * local : (i + 1) * local] for i in range(3) for r in range(ring)], axis=1
    )

    bias_sum = jnp.sum(dqkv.astype(F32), axis=0)
    zeros = jnp.zeros((width,), F32)
    first = jnp.stack(
        [
            gain_sum,
            shift_sum,
            lax.dynamic_update_slice_in_dim(zeros, bias_sum[:local], me * local, 0),
            lax.dynamic_update_slice_in_dim(zeros, bias_sum[2 * local :], me * local, 0),
        ]
    )
    second = jnp.stack(
        [
            jnp.sum(dh2 * n2, axis=0),
            jnp.sum(dh2, axis=0),
            jnp.sum(dy_f, axis=0),
            jnp.sum(da.astype(F32), axis=0),
        ]
    )
    c1_sum = jnp.sum(dz.astype(F32), axis=0).reshape(devices, -1, own).transpose(1, 0, 2)
    second = jnp.concatenate([second, c1_sum.reshape(-1, width)])
    four = sum_vectors(second, devices, ring)
    grad_c1 = four[4:].reshape(-1)
    late = sum_vectors(first, devices, ring)

    terms = jnp.concatenate(own_terms, axis=0)
    n1, r1 = normalize(inputs)
    grad_inputs = (grad_middle + normalize_back(terms, n1, r1, g1)).reshape(clips, rows, width)
    return (
        layer_out,
        grad_inputs,
        late[0],
        late[1],
        grad_qkv,
        late[2],
        late[3],
        grad_wo,
        four[3],
        four[0],
        four[1],
        grad_w1,
        grad_c1,
        grad_w2,
        four[2],
    )


def twin(value, devices):
    return lax.ppermute(value, "fsdp", [(i, i ^ 1) for i in range(devices)])


def columns(vectors):
    vectors = jnp.pad(vectors.astype(BF16), ((0, -vectors.shape[0] % 128), (0, 0)))
    return dot(jnp.eye(vectors.shape[1], dtype=BF16), vectors, NT).astype(BF16)


def as_rows(block, count):
    return dot(block, jnp.eye(block.shape[0], dtype=BF16), TN)[:count]


def plus(a, b):
    return (a.astype(F32) + b.astype(F32)).astype(BF16)


def plus_rows(a, b, more, row):
    total = a.astype(F32) + b.astype(F32)
    pad = [(row, a.shape[0] - row - more.shape[0])] + [(0, 0)] * (a.ndim - 1)
    return (total + jnp.pad(more.astype(F32), pad)).astype(BF16)


def stage(*values):
    return lax.optimization_barrier(values)


def placed(parts, me):
    out = jnp.zeros((len(parts),) + parts[0].shape, parts[0].dtype)
    for r, part in enumerate(parts):
        out = lax.dynamic_update_index_in_dim(out, part, me ^ r, 0)
    return out


def shards(
    ring,
    devices,
    tokens,
    lengths,
    ln1_gain,
    ln1_bias,
    w_qkv,
    q_bias,
    v_bias,
    w_out,
    b_out,
    ln2_gain,
    ln2_bias,
    w_fc1,
    b_fc1,
    w_fc2,
    b_fc2,
    cotangent,
):
    clips, rows, width = tokens.shape
    total_rows, clip_rows, local = clips * rows, rows * ring, width // ring
    own, half, cut = ln1_gain.shape[0], clips // 2, devices // 4
    me, core = lax.axis_index("seq"), lax.axis_index("fsdp") % 2
    same_core = [list(range(p, devices, 2)) for p in range(2)]

    def over(value, r):
        return swap(value, ring, r)

    vectors = jnp.concatenate(
        [
            jnp.stack([ln1_gain, ln1_bias, q_bias, v_bias, b_out, ln2_gain, ln2_bias, b_fc2]),
            b_fc1.reshape(-1, own),
        ]
    )
    count = vectors.shape[0]
    mine = lax.dynamic_index_in_dim(w_qkv.reshape(own, 3, ring, local), me, 2, keepdims=False)
    mine = jnp.concatenate([mine.reshape(own, 3 * local), columns(vectors)], axis=1)
    mine = lax.all_gather(mine, "fsdp", axis=0, tiled=True)
    part1 = lax.dynamic_index_in_dim(w_fc1.reshape(own, devices, ring, own), me, 2)
    part2 = lax.dynamic_index_in_dim(w_fc2.reshape(ring, own, width), me, 0)
    quarter = jnp.concatenate([part1.reshape(1, own, width), part2], axis=0)
    quarter = lax.all_gather(quarter, "fsdp", axis=0, axis_index_groups=same_core)
    wo = lax.all_gather(w_out, "fsdp", axis=0, tiled=True)

    middle_row = rows // 16 * 8
    one, two = stage(over(tokens[0], 1), over(tokens[0], 2))
    far = [over(two[:middle_row], 1), over(one[middle_row:], 2)]
    mine, one, two = stage(mine, one, two)
    vectors = as_rows(mine[:, 3 * local :], count)
    g1, b1, qb, vb, bo, g2, b2, c2 = (vectors[i] for i in range(8))
    c1_rows = vectors[8:]
    qb_mine = lax.dynamic_slice_in_dim(qb, me * local, local)
    vb_mine = lax.dynamic_slice_in_dim(vb, me * local, local)
    bias_mine = jnp.concatenate([qb_mine, jnp.zeros_like(qb_mine), vb_mine])

    normed, qkv, outs, logs = ([None] * clips for _ in range(4))

    def project(c, groups, start=0, made=()):
        made = norm_project(me, groups, g1, b1, mine, bias_mine, ring, start, made)
        normed[c] = made[0].reshape(clip_rows, width)
        qkv[c] = made[1].reshape(1, clip_rows, 3 * local)
        return made

    def to_rows(out):
        return lax.all_to_all(
            out.reshape(ring, rows, local), "seq", split_axis=0, concat_axis=0, tiled=True
        )

    def length(c):
        return lax.dynamic_slice_in_dim(lengths, c, 1)

    made = project(0, [[(tokens, 0)], [one], [two]])
    made, far = lax.optimization_barrier((made, far))
    project(0, [far], 3, made)
    outs[0], logs[0] = attend(qkv[0], length(0))
    rest, *_ = stage(tokens[1:], *far)
    others = [over(rest, r) for r in range(1, ring)]
    outs[0], *others = stage(outs[0], *others)
    moved = []
    for c in range(1, clips):
        moved.append(to_rows(outs[c - 1]))
        project(c, [[(tokens, c)]] + [[(t, c - 1)] for t in others])
        if c == 1:
            qkv[c], quarter, moved[0] = stage(qkv[c], quarter, moved[0])
            ends_of = [quarter[:cut], quarter[cut:]]
            low1, top2 = over(ends_of[1], 1), over(ends_of[0], 2)
            twin0 = twin(quarter, devices)
        outs[c], logs[c] = attend(qkv[c], length(c))
        if c == 1:
            outs[c], low1, top2, twin0 = stage(outs[c], low1, top2, twin0)
    moved.append(to_rows(outs[-1]))
    moved, low1, top2, ends_of = lax.optimization_barrier((moved, low1, top2, ends_of))
    top1, low2 = over(ends_of[0], 1), over(ends_of[1], 2)
    attended, middle, h2, h2t = project_norm(moved, tokens, wo, bo, g2, b2)
    dy = cotangent.reshape(total_rows, width)

    sums = [None] * ring

    def quarter_of(r, mine_r, twin_r, acc):
        shift = lax.dynamic_index_in_dim(c1_rows, me ^ r, 0)
        y, dh2, keep, send, sums[r] = mlp_piece(
            core[None], h2, h2t, dy, mine_r, twin_r, shift, acc
        )
        return (y, dh2), keep, send

    early = [twin(low1, devices), twin(top2, devices)]
    acc, keep0, send0 = quarter_of(0, [quarter], [twin0], None)
    acc, keep0, send0, early, top1, low2 = lax.optimization_barrier(
        (acc, keep0, send0, early, top1, low2)
    )
    far = [over(top2, 1), over(low1, 2)]
    got0, later2 = twin(send0, devices), twin(low2, devices)
    (later1,) = stage(twin(top1, devices))
    acc, keep1, send1 = quarter_of(1, [top1, low1], [later1, early[0]], acc)
    acc, keep1, send1, far, later2, got0 = lax.optimization_barrier(
        (acc, keep1, send1, far, later2, got0)
    )
    twin_far, got1 = [twin(f, devices) for f in far], twin(send1, devices)
    acc, keep2, send2 = quarter_of(2, [top2, low2], [early[1], later2], acc)
    acc, keep2, send2, twin_far, got1 = lax.optimization_barrier(
        (acc, keep2, send2, twin_far, got1)
    )
    got2 = twin(send2, devices)
    acc, keep3, send3 = quarter_of(3, far, twin_far, acc)
    (y, dh2), keep3, send3, got2 = lax.optimization_barrier((acc, keep3, send3, got2))
    (got3,) = stage(twin(send3, devices))
    term3 = plus(keep3, got3)
    ends = [over(term3[:cut], 1), over(term3[cut:], 2)]

    c1_sum = placed([v[0] for v in sums], me)
    def to_heads(part):
        part = lax.all_to_all(part, "seq", split_axis=0, concat_axis=0, tiled=True)
        return part.reshape(1, clip_rows, local)

    layer_out = grad_middle = None
    das, heads, column_sums = ([None] * clips for _ in range(3))
    for c in range(clips):
        layer_out, grad_middle, das[c], heads[c], column_sums[c] = project_back(
            c, y, dh2, middle, dy, wo, g2, c2, tokens.shape, ring, layer_out, grad_middle
        )
        if c == 0:
            moved = to_heads(heads[0])
    term_wo = project_weight(das, attended, column_sums, c1_sum)
    moved, term_wo, end2, end1 = stage(moved, term_wo, *ends)
    owned_wo = to_owners(term_wo)

    second = [
        add_terms([(keep1, None), (got1, None), (end1, cut)]),
        add_terms([(keep2, None), (got2, None), (end2, 0)]),
    ]
    *second, next_moved = stage(*second, to_heads(heads[1]))
    second = [over(second[0], 1), over(second[1], 2)]
    acc, flying, token_terms = None, [], [None] * clips

    def exchange(parts):
        return lax.all_to_all(parts, "seq", 0, 0, tiled=True)

    def to_all(part):
        return exchange(jnp.broadcast_to(part[None], (ring,) + part.shape))

    for c in range(clips):
        later = [to_heads(heads[c + 1])] if 0 < c < clips - 1 else []
        if c == clips - 1:
            owned_wo = owned_wo.reshape(ring, own // ring, width + 128)
            later = [lax.dynamic_index_in_dim(owned_wo, me ^ r, 0, False) for r in range(ring)]
            later = [over(t, r) if r else t for r, t in enumerate(later)]
        d = attend_back(qkv[c], moved, outs[c], logs[c], length(c))
        if c < clips - 1:
            acc = qkv_weight(me, d[0], normed[c], mine, acc, ring, False)
        d, later, flying, second, acc = lax.optimization_barrier((d, later, flying, second, acc))
        moved, wo_terms = (later[0], later) if later else (next_moved, later)
        if c:
            token_terms[c - 1] = flying[0]
        else:
            total = add_terms([(t, None) for t in (keep0, got0, *second)])
            owned_mlp = lax.psum_scatter(
                total,
                "fsdp",
                scatter_dimension=0,
                tiled=True,
                axis_index_groups=same_core,
            )[0]
            second = []
        last = c == clips - 1
        if c < clips - 1:
            flying = [exchange(qkv_back(d[0], mine, ring))]

    d, owned_mlp = stage(d, owned_mlp)
    shared = [over(owned_mlp, 1), over(owned_mlp, 2)]
    grad_mine, kept, one, two, top, low = qkv_weight(
        me, d[0], normed[-1], mine, acc, ring, True
    )
    one, two, top, low, shared, grad_mine = lax.optimization_barrier(
        (one, two, top, low, shared, grad_mine)
    )
    owned = to_owners(grad_mine)

    cross = [over(top, 1), over(low, 2)]
    grad_inputs = None
    for c in range(clips - 1):
        terms = [(token_terms[c], ring)]
        grad_inputs = tokens_back(c, terms, tokens, grad_middle, g1, grad_inputs)
    grad_inputs, cross = lax.optimization_barrier((grad_inputs, cross))
    flying = [
        over(jnp.concatenate([one[:, :middle_row], plus(one[:, middle_row:], cross[1][None])], 1), 1),
        over(jnp.concatenate([plus(two[:, :middle_row], cross[0][None]), two[:, middle_row:]], 1), 2),
    ]
    wo_term = sum(t.astype(F32) for t in wo_terms).astype(BF16)
    wo_parts = to_all(wo_term)
    flying, wo_parts = lax.optimization_barrier((flying, wo_parts))
    owned, flying, shared = lax.optimization_barrier((owned, flying, shared))
    far = [over(shared[1][:1], 1), over(shared[0][1:], 2)]
    grad_w1, grad_w2 = spread_mlp(me, [owned_mlp, *shared, *far], ring)
    owned = [over(owned, r) if r else owned for r in range(ring)]
    terms = [(kept, 1)] + [(f, 1) for f in flying]
    grad_inputs = tokens_back(clips - 1, terms, tokens, grad_middle, g1, grad_inputs)
    grad_wo, grad_qkv, sums = spread_attn(me, wo_parts, owned)
    middle_sums, last_sums = sums[0], sums[1]
    return (
        layer_out,
        grad_inputs,
        last_sums[0],
        last_sums[1],
        grad_qkv,
        last_sums[2],
        last_sums[3],
        grad_wo,
        middle_sums[3],
        middle_sums[0],
        middle_sums[1],
        grad_w1,
        middle_sums[4 : count - 4].reshape(-1),
        grad_w2,
        middle_sums[2],
    )


def solution(mesh):
    act, vec, mat = P("fsdp", "seq", None), P("fsdp"), P("fsdp", None)
    in_specs = (act, vec, vec, vec, mat, vec, vec, mat, vec, vec, vec, mat, vec, mat, vec, act)
    out_specs = (act, act, vec, vec, mat, vec, vec, mat, vec, vec, vec, mat, vec, mat, vec)
    ring, devices = mesh.shape["seq"], mesh.shape["fsdp"]

    def layer(*args):
        clips, rows, width = args[0].shape
        square = ring == 4 and args[11].shape[1] == ring * width and devices % 4 == 0
        square = square and clips % (2 * devices) == 0 and width % (128 * devices) == 0
        return jax.shard_map(
            functools.partial(shards if square else shards_any, ring, devices),
            mesh=mesh,
            in_specs=in_specs,
            out_specs=out_specs,
            check_vma=False,
        )(*args)

    return layer
```
